32 devices in a mesh: fsdp: 8 (over z, y), rep: 4 (over x, core).
Axes of the slice: x: 2, y: 2, z: 4, core: 2. Of those that a mesh axis runs over, the one named last changes fastest.
Arguments:
- latents: float32 [192, 4, 1024], P(('fsdp', 'rep')), may hold values from -6 to 6
- tsteps: int32 [192], P(('fsdp', 'rep')), may hold values from 0 to 999
- labels: int32 [192], P(('fsdp', 'rep')), may hold values from 0 to 1000
- noise: float32 [192, 4, 1024], P(('fsdp', 'rep')), may hold values from -6 to 6
- layer_in: float32 [2, 384, 5376], P(None, 'fsdp'), may hold values from -0.3125 to 0.3125
- layer_out: float32 [2, 1536, 384], P(None, 'fsdp'), may hold values from -0.15625 to 0.15625
- edge_mat: float32 [384, 2457], P('fsdp'), may hold values from -4 to 4
- layer_bias: float32 [2, 5376], replicated, may hold values from -2 to 2
- top_bias: float32 [1952], replicated, may hold values from -2 to 2
- in_rows: float32 [2, 384], P(None, 'fsdp'), may hold values from 0.0005 to 0.2
- in_cols: float32 [2, 5376], replicated, may hold values from 0.005 to 0.05
- out_rows: float32 [2, 1536], P(None, 'fsdp'), may hold values from 0.0005 to 0.2
- out_cols: float32 [2, 384], replicated, may hold values from 0.005 to 0.05
- edge_rows: float32 [384], P('fsdp'), may hold values from 0.0005 to 0.2
- edge_cols: float32 [2457], replicated, may hold values from 0.005 to 0.05
- layer_bias_v: float32 [2, 5376], replicated, may hold values from 0.005 to 0.05
- top_bias_v: float32 [1952], replicated, may hold values from 0.005 to 0.05
Outputs:
- loss: float32 [], replicated
- layer_in_new: float32 [2, 384, 5376], P(None, 'fsdp')
- layer_out_new: float32 [2, 1536, 384], P(None, 'fsdp')
- edge_mat_new: float32 [384, 2457], P('fsdp')
- layer_bias_new: float32 [2, 5376], replicated
- top_bias_new: float32 [1952], replicated
- in_rows_new: float32 [2, 384], P(None, 'fsdp')
- in_cols_new: float32 [2, 5376], replicated
- out_rows_new: float32 [2, 1536], P(None, 'fsdp')
- out_cols_new: float32 [2, 384], replicated
- edge_rows_new: float32 [384], P('fsdp')
- edge_cols_new: float32 [2457], replicated
- layer_bias_v_new: float32 [2, 5376], replicated
- top_bias_v_new: float32 [1952], replicated
- clip_roots: float32 [5], replicated
The draws below stay inside these ranges and needn't reach their ends.
All inputs are finite; a program needn't handle non-finite values.
Results may differ from the reference program's by a relative error of at most 0.0015.
The reference program's roundings to bfloat16 on the way count: a program that leaves them out, or rounds other values in their place, can miss the bound.
Values may be sent and summed in bfloat16 or wider, within the bound.
A program may use at most 256 MiB of HBM per device.

```python
import math
import jax
import jax.numpy as jnp
from jax import lax

D = 384
HEADS = 6
HEAD_DIM = 64
FF = 1536
CHANNELS = 4
PATCH = 2
GRID = 32
TSTEPS = 1000
NCLS = 1001
FREQ = 256
L = 2
TOK = 256
PATCH_IN = 16
HEAD_OUT = 32
WIDE = 5376
E = 2457
IMAGES = 192
NTOK = 49152


def draw_edge_mat(key, part):
    base = jnp.clip(jax.random.normal(key, (D, E), jnp.float32), -4.0, 4.0)
    column = jnp.arange(E)
    start_freq = NCLS + PATCH_IN
    start_tail = start_freq + FREQ
    scales = jnp.where(column < NCLS, 1.0, jnp.where(column < start_freq, PATCH_IN ** (-0.5), jnp.where(column < start_tail, FREQ ** (-0.5), D ** (-0.5))))
    return base * scales.astype(jnp.float32)[None, :]


def rising_rows(key, shape):
    count = shape[-1]
    place = jnp.arange(count, dtype=jnp.float32) / count
    low_end = jnp.log(0.002)
    high_end = jnp.log(0.04)
    rough = jax.random.uniform(key, shape, jnp.float32, 0.7, 1.3)
    return jnp.exp(low_end + (high_end - low_end) * place) * rough


def draw_in_rows(key, part):
    return rising_rows(key, (L, D))


def draw_out_rows(key, part):
    return rising_rows(key, (L, FF))


def draw_edge_rows(key, part):
    return rising_rows(key, (D,))


def place_ends(entries, own_key, least, largest):
    index_at = [jax.random.randint(jax.random.fold_in(own_key, axis), (), 0, length) for axis, length in enumerate(entries.shape)]
    main_axis = entries.shape.index(max(entries.shape))
    neighbour = index_at[:main_axis] + [(index_at[main_axis] + 1) % entries.shape[main_axis]] + index_at[main_axis + 1:]
    return entries.at[tuple(index_at)].set(least).at[tuple(neighbour)].set(largest)


def block_scale(stream_key, extent, pieces, least, top_value):
    def one(position, parts):
        draws = jax.random.uniform(jax.random.fold_in(jax.random.fold_in(stream_key, 6), position), (parts,), jnp.float32, least / len(pieces), top_value / len(pieces))
        return jnp.repeat(jnp.exp(draws), extent[position] // parts).reshape((-1,) + (1,) * (len(extent) - position - 1))

    loudness = one(*pieces[0])
    for cut in pieces[1:]:
        loudness = loudness * one(*cut)
    return loudness


def scatter_about(stream_key, dims, deviation, bound, shards=(), held_as=jnp.bfloat16):
    drawn = jax.random.normal(stream_key, dims, jnp.float32) * deviation
    if len(shards) > 0:
        drawn = block_scale(stream_key, dims, shards, -0.22, 0.18) * drawn
    return jnp.clip(drawn, min=-bound, max=bound).astype(held_as)


def setup_inputs(seed: int = 0) -> dict:
    splits = jax.random.split(jax.random.key(seed), 18)
    return {
        "latents": scatter_about(splits[0], (IMAGES, CHANNELS, GRID * GRID), 1.0, 6.0, ((0, 32),), jnp.float32),
        "tsteps": place_ends(jax.random.randint(splits[1], (IMAGES,), 0, TSTEPS), jax.random.fold_in(splits[1], 1), 0, TSTEPS - 1).astype(jnp.int32),
        "labels": place_ends(jax.random.randint(splits[2], (IMAGES,), 0, NCLS), jax.random.fold_in(splits[2], 1), 0, NCLS - 1).astype(jnp.int32),
        "noise": scatter_about(splits[3], (IMAGES, CHANNELS, GRID * GRID), 1.0, 6.0, ((0, 32),), jnp.float32),
        "layer_in": scatter_about(splits[4], (L, D, WIDE), D ** -0.5, 0.3125, ((1, 8),), jnp.float32),
        "layer_out": scatter_about(splits[5], (L, FF, D), FF ** -0.5, 0.15625, ((1, 8),), jnp.float32),
        "edge_mat": draw_edge_mat(jax.random.fold_in(splits[17], 71), 0),
        "layer_bias": scatter_about(splits[7], (L, WIDE), 0.3, 2.0, (), jnp.float32),
        "top_bias": scatter_about(splits[8], (5 * D + HEAD_OUT,), 0.3, 2.0, (), jnp.float32),
        "in_rows": draw_in_rows(jax.random.fold_in(splits[17], 71), 0),
        "in_cols": jnp.clip(jnp.exp(jax.random.uniform(splits[10], (L, WIDE), jnp.float32, math.log(0.005), math.log(0.05))), 0.005, 0.05),
        "out_rows": draw_out_rows(jax.random.fold_in(splits[17], 71), 0),
        "out_cols": jnp.clip(jnp.exp(jax.random.uniform(splits[12], (L, D), jnp.float32, math.log(0.005), math.log(0.05))), 0.005, 0.05),
        "edge_rows": draw_edge_rows(jax.random.fold_in(splits[17], 71), 0),
        "edge_cols": jnp.clip(jnp.exp(jax.random.uniform(splits[14], (E,), jnp.float32, math.log(0.005), math.log(0.05))), 0.005, 0.05),
        "layer_bias_v": jnp.clip(jnp.exp(jax.random.uniform(splits[15], (L, WIDE), jnp.float32, math.log(0.005), math.log(0.05))), 0.005, 0.05),
        "top_bias_v": jnp.clip(jnp.exp(jax.random.uniform(splits[16], (5 * D + HEAD_OUT,), jnp.float32, math.log(0.005), math.log(0.05))), 0.005, 0.05),
    }


eps_norm = 1e-06
eps_stat = 1e-30
decay = 0.5
rate = 0.01
clip_level = 1.0

@jax.custom_vjp
def low(v):
    return lax.optimization_barrier(v.astype(jnp.bfloat16)).astype(jnp.float32)

@jax.custom_vjp
def low_back(v):
    return v

def low_keep(v):
    return (low(v), None)

def low_pass(kept, grad):
    return (grad,)

def back_keep(v):
    return (v, None)

def back_low(kept, grad):
    return (low(grad),)
low.defvjp(low_keep, low_pass)
low_back.defvjp(back_keep, back_low)

def mult(left, right, form):
    return jnp.einsum(form, left, right, precision=lax.Precision.HIGHEST)

def normalize(values):
    center = values - lax.optimization_barrier(jnp.mean(values, axis=-1, keepdims=True))
    spread = lax.optimization_barrier(jnp.mean(center * center, axis=-1, keepdims=True))
    return center * lax.rsqrt(spread + eps_norm)

def mix_weights(tsteps):
    betas = 0.0001 + (0.02 - 0.0001) * jnp.arange(TSTEPS, dtype=jnp.float32) / (TSTEPS - 1)
    alpha_bar = jnp.exp(jnp.cumsum(jnp.log(1.0 - betas)))
    picked = jnp.arange(TSTEPS)[None, :] == tsteps[:, None]
    return lax.optimization_barrier(jnp.sum(jnp.where(picked, alpha_bar[None, :], 0.0), axis=1))

def patchify(latent_rows):
    images = latent_rows.shape[0]
    grid_side = GRID // PATCH
    shaped = latent_rows.reshape(images, CHANNELS, grid_side, PATCH, grid_side, PATCH)
    shaped = jnp.transpose(shaped, (0, 2, 4, 1, 3, 5))
    return shaped.reshape(images, grid_side * grid_side, CHANNELS * PATCH * PATCH)

def position_table():
    grid_side = GRID // PATCH
    quarter = D // 4
    omegas = 1.0 / 10000.0 ** (jnp.arange(quarter, dtype=jnp.float32) / quarter)
    places = jnp.arange(grid_side * grid_side)
    across = (places % grid_side).astype(jnp.float32)
    downward = (places // grid_side).astype(jnp.float32)

    def one_axis(coords):
        angles = coords[:, None] * omegas[None, :]
        return jnp.concatenate([jnp.sin(angles), jnp.cos(angles)], axis=1)
    return jnp.concatenate([one_axis(across), one_axis(downward)], axis=1)

def time_features(tsteps):
    half_freq = FREQ // 2
    frequencies = jnp.exp(-math.log(10000.0) * jnp.arange(half_freq, dtype=jnp.float32) / half_freq)
    angles = tsteps.astype(jnp.float32)[:, None] * frequencies[None, :]
    return jnp.concatenate([jnp.cos(angles), jnp.sin(angles)], axis=1)

def block(tokens, condition, weights, weights_down, biases):
    images = tokens.shape[0]
    modulation = low_back(mult(condition, weights[:, :6 * D], 'bd,de->be') + biases[:6 * D])
    shift_attn = modulation[:, 0:D][:, None]
    scale_attn = modulation[:, D:2 * D][:, None]
    gate_attn = modulation[:, 2 * D:3 * D][:, None]
    shift_mlp = modulation[:, 3 * D:4 * D][:, None]
    scale_mlp = modulation[:, 4 * D:5 * D][:, None]
    gate_mlp = modulation[:, 5 * D:6 * D][:, None]
    normed = low(normalize(tokens) * (1.0 + scale_attn) + shift_attn)
    bias_qkv = jnp.concatenate([biases[6 * D:7 * D], jnp.zeros_like(biases[:D]), biases[7 * D:8 * D]])
    project = low(low_back(mult(normed, weights[:, 6 * D:9 * D], 'btd,de->bte') + bias_qkv))
    queries = project[..., :D].reshape(images, TOK, HEADS, HEAD_DIM)
    keys_all = project[..., D:2 * D].reshape(images, TOK, HEADS, HEAD_DIM)
    values_all = project[..., 2 * D:].reshape(images, TOK, HEADS, HEAD_DIM)
    scores = low_back(mult(queries, keys_all, 'bqhe,bkhe->bhqk') * HEAD_DIM ** (-0.5))
    weights_soft = low(jax.nn.softmax(scores, axis=-1))
    attended = low(low_back(mult(weights_soft, values_all, 'bhqk,bkhe->bqhe'))).reshape(images, TOK, D)
    branch = low_back(mult(attended, weights[:, 9 * D:10 * D], 'btd,de->bte') + biases[8 * D:9 * D])
    tokens = tokens + gate_attn * branch
    normed_mlp = low(normalize(tokens) * (1.0 + scale_mlp) + shift_mlp)
    inner = low_back(mult(normed_mlp, weights[:, 10 * D:], 'btd,df->btf') + biases[9 * D:9 * D + FF])
    activated = low(jax.nn.gelu(inner, approximate=True))
    outward = low_back(mult(activated, weights_down, 'btf,fd->btd') + biases[9 * D + FF:])
    return tokens + gate_mlp * outward

def image_loss(params, latents, tsteps, labels, noise):
    layer_in, layer_out, edge_mat, layer_bias, top_bias = params
    alphas = mix_weights(tsteps)
    noisy = jnp.sqrt(alphas)[:, None, None] * latents + jnp.sqrt(1.0 - alphas)[:, None, None] * noise
    patches = low(patchify(noisy))
    target = patchify(noise)
    edge_low = low(edge_mat)
    start_freq = NCLS + PATCH_IN
    start_tail = start_freq + FREQ
    class_cols = edge_low[:, :NCLS]
    patch_cols = edge_low[:, NCLS:start_freq]
    freq_cols = edge_low[:, start_freq:start_tail]
    time_second = edge_low[:, start_tail:start_tail + D]
    final_cols = edge_low[:, start_tail + D:start_tail + 3 * D]
    head_cols = edge_low[:, start_tail + 3 * D:]
    tokens = low_back(mult(patches, patch_cols, 'btp,dp->btd') + top_bias[:D]) + position_table()[None]
    features = low(time_features(tsteps))
    time_first = low_back(mult(features, freq_cols, 'bf,df->bd') + top_bias[D:2 * D])
    time_out = low_back(mult(low(jax.nn.silu(time_first)), time_second, 'bd,de->be') + top_bias[2 * D:3 * D])
    class_emb = jnp.take(class_cols, labels, axis=1).T
    condition = low(jax.nn.silu(time_out + class_emb))
    for layer_index in range(L):
        tokens = block(tokens, condition, low(layer_in[layer_index]), low(layer_out[layer_index]), layer_bias[layer_index])
    closing = low_back(mult(condition, final_cols, 'bd,de->be') + top_bias[3 * D:5 * D])
    normed = low(normalize(tokens) * (1.0 + closing[:, None, D:]) + closing[:, None, :D])
    predicted = low_back(mult(normed, head_cols, 'btd,dp->btp') + top_bias[5 * D:])
    misfit = predicted[..., :PATCH_IN] - target
    return jnp.sum(misfit * misfit)

def factored(weight, grad, rows_old, cols_old):
    squared = grad * grad + eps_stat
    rows_new = decay * rows_old + (1.0 - decay) * lax.optimization_barrier(jnp.mean(squared, axis=1))
    cols_new = decay * cols_old + (1.0 - decay) * lax.optimization_barrier(jnp.mean(squared, axis=0))
    second = rows_new[:, None] * cols_new[None, :] / jnp.mean(rows_new)
    update = grad * lax.rsqrt(second)
    root = jnp.sqrt(jnp.mean(update * update))
    return (weight - rate * update / jnp.maximum(1.0, root / clip_level), rows_new, cols_new, root)

def plain(weight, grad, moment):
    moment_new = decay * moment + (1.0 - decay) * (grad * grad + eps_stat)
    update = grad * lax.rsqrt(moment_new)
    root = jnp.sqrt(jnp.mean(update * update))
    return (weight - rate * update / jnp.maximum(1.0, root / clip_level), moment_new)

def reference(latents, tsteps, labels, noise, layer_in, layer_out, edge_mat, layer_bias, top_bias, in_rows, in_cols, out_rows, out_cols, edge_rows, edge_cols, layer_bias_v, top_bias_v):
    params = (layer_in, layer_out, edge_mat, layer_bias, top_bias)
    groups = IMAGES // 16

    def regroup(array):
        return array.reshape((groups, 16) + array.shape[1:])

    def one_group(carried, group_data):
        loss_sum, gradients = carried

        def local_loss(params_now):
            return image_loss(params_now, *group_data)
        loss_part, pullback = jax.vjp(local_loss, params)
        grads_now, = pullback(jnp.ones_like(loss_part))
        return ((loss_sum + loss_part, jax.tree.map(jnp.add, gradients, grads_now)), None)
    zeroed = jax.tree.map(jnp.zeros_like, params)
    (loss_sum, gradients), unused = lax.scan(one_group, (jnp.zeros((), jnp.float32), zeroed), (regroup(latents), regroup(tsteps), regroup(labels), regroup(noise)))
    scale_grad = 1.0 / (PATCH_IN * math.sqrt(NTOK))
    grad_in, grad_out, grad_edge, grad_lbias, grad_tbias = [item * scale_grad for item in gradients]
    loss = loss_sum / (NTOK * PATCH_IN)
    in_new, in_rows_new, in_cols_new, roots_in = jax.vmap(factored)(layer_in, grad_in, in_rows, in_cols)
    out_new, out_rows_new, out_cols_new, roots_out = jax.vmap(factored)(layer_out, grad_out, out_rows, out_cols)
    edge_new, edge_rows_new, edge_cols_new, root_edge = factored(edge_mat, grad_edge, edge_rows, edge_cols)
    lbias_new, lbias_v_new = jax.vmap(plain)(layer_bias, grad_lbias, layer_bias_v)
    tbias_new, tbias_v_new = plain(top_bias, grad_tbias, top_bias_v)
    clip_roots = jnp.concatenate([roots_in, roots_out, root_edge[None]])
    return (loss, in_new, out_new, edge_new, lbias_new, tbias_new, in_rows_new, in_cols_new, out_rows_new, out_cols_new, edge_rows_new, edge_cols_new, lbias_v_new, tbias_v_new, clip_roots)
```

```python
import math

import jax
import jax.numpy as jnp
from jax import lax
from jax.sharding import PartitionSpec as P

D = 384
HEADS = 6
HEAD_DIM = 64
FF = 1536
CHANNELS = 4
PATCH = 2
GRID = 32
TSTEPS = 1000
NCLS = 1001
FREQ = 256
MICRO = 1
PATCH_IN = 16


eps_norm = 1e-06
eps_stat = 1e-30
decay = 0.5
rate = 0.01
clip_level = 1.0


def round_value(values):
    return lax.optimization_barrier(values.astype(jnp.bfloat16)).astype(jnp.float32)


def rounders():
    rounding = jax.custom_vjp(round_value)

    def keep_forward(values):
        return (round_value(values), None)

    def pass_backward(kept, grad):
        return (grad,)

    rounding.defvjp(keep_forward, pass_backward)

    def unchanged(values):
        return values

    backing = jax.custom_vjp(unchanged)

    def back_forward(values):
        return (values, None)

    def back_backward(kept, grad):
        return (round_value(grad),)

    backing.defvjp(back_forward, back_backward)
    return (rounding, backing)


def low(values):
    return rounders()[0](values)


def low_back(values):
    return rounders()[1](values)


def mult(left, right, form):
    return jnp.einsum(form, left, right, preferred_element_type=jnp.float32)


def normalize(values):
    center = values - jnp.mean(values, axis=-1, keepdims=True)
    spread = jnp.mean(center * center, axis=-1, keepdims=True)
    return center * lax.rsqrt(spread + eps_norm)


def mix_weights(tsteps):
    betas = 0.0001 + (0.02 - 0.0001) * jnp.arange(TSTEPS, dtype=jnp.float32) / (TSTEPS - 1)
    alpha_bar = jnp.exp(jnp.cumsum(jnp.log(1.0 - betas)))
    picked = jnp.arange(TSTEPS)[None, :] == tsteps[:, None]
    return jnp.sum(jnp.where(picked, alpha_bar[None, :], 0.0), axis=1)


def patchify(latent_rows):
    images = latent_rows.shape[0]
    grid_side = GRID // PATCH
    shaped = latent_rows.reshape(images, CHANNELS, grid_side, PATCH, grid_side, PATCH)
    shaped = jnp.transpose(shaped, (0, 2, 4, 1, 3, 5))
    return shaped.reshape(images, grid_side * grid_side, CHANNELS * PATCH * PATCH)


def position_table():
    grid_side = GRID // PATCH
    quarter = D // 4
    omegas = 1.0 / 10000.0 ** (jnp.arange(quarter, dtype=jnp.float32) / quarter)
    places = jnp.arange(grid_side * grid_side)
    across = (places % grid_side).astype(jnp.float32)
    downward = (places // grid_side).astype(jnp.float32)

    def one_axis(coords):
        angles = coords[:, None] * omegas[None, :]
        return jnp.concatenate([jnp.sin(angles), jnp.cos(angles)], axis=1)

    return jnp.concatenate([one_axis(across), one_axis(downward)], axis=1)


def time_features(tsteps):
    half_freq = FREQ // 2
    frequencies = jnp.exp(-math.log(10000.0) * jnp.arange(half_freq, dtype=jnp.float32) / half_freq)
    angles = tsteps.astype(jnp.float32)[:, None] * frequencies[None, :]
    return jnp.concatenate([jnp.cos(angles), jnp.sin(angles)], axis=1)


def block(tokens, condition, weights, weights_down, biases):
    images = tokens.shape[0]
    tok_count = tokens.shape[1]
    modulation = low_back(mult(condition, weights[:, : 6 * D], "bd,de->be") + biases[: 6 * D])
    shift_attn = modulation[:, 0:D][:, None]
    scale_attn = modulation[:, D : 2 * D][:, None]
    gate_attn = modulation[:, 2 * D : 3 * D][:, None]
    shift_mlp = modulation[:, 3 * D : 4 * D][:, None]
    scale_mlp = modulation[:, 4 * D : 5 * D][:, None]
    gate_mlp = modulation[:, 5 * D : 6 * D][:, None]
    normed = low(normalize(tokens) * (1.0 + scale_attn) + shift_attn)
    bias_qkv = jnp.concatenate(
        [biases[6 * D : 7 * D], jnp.zeros_like(biases[:D]), biases[7 * D : 8 * D]]
    )
    project = low(low_back(mult(normed, weights[:, 6 * D : 9 * D], "btd,de->bte") + bias_qkv))
    queries = project[..., :D].reshape(images, tok_count, HEADS, HEAD_DIM)
    keys_all = project[..., D : 2 * D].reshape(images, tok_count, HEADS, HEAD_DIM)
    values_all = project[..., 2 * D :].reshape(images, tok_count, HEADS, HEAD_DIM)
    scores = low_back(mult(queries, keys_all, "bqhe,bkhe->bhqk") * HEAD_DIM ** (-0.5))
    weights_soft = low(jax.nn.softmax(scores, axis=-1))
    attended = low(low_back(mult(weights_soft, values_all, "bhqk,bkhe->bqhe"))).reshape(
        images, tok_count, D
    )
    branch = low_back(
        mult(attended, weights[:, 9 * D : 10 * D], "btd,de->bte") + biases[8 * D : 9 * D]
    )
    tokens = tokens + gate_attn * branch
    normed_mlp = low(normalize(tokens) * (1.0 + scale_mlp) + shift_mlp)
    inner = low_back(
        mult(normed_mlp, weights[:, 10 * D :], "btd,df->btf") + biases[9 * D : 9 * D + FF]
    )
    activated = low(jax.nn.gelu(inner, approximate=True))
    outward = low_back(mult(activated, weights_down, "btf,fd->btd") + biases[9 * D + FF :])
    return tokens + gate_mlp * outward


def image_loss(params, latents, tsteps, labels, noise):
    layer_in, layer_out, edge_mat, layer_bias, top_bias = params
    depth = layer_in.shape[0]
    alphas = mix_weights(tsteps)
    noisy = (
        jnp.sqrt(alphas)[:, None, None] * latents + jnp.sqrt(1.0 - alphas)[:, None, None] * noise
    )
    patches = low(patchify(noisy))
    target = patchify(noise)
    edge_low = low(edge_mat)
    start_freq = NCLS + PATCH_IN
    start_tail = start_freq + FREQ
    class_cols = edge_low[:, :NCLS]
    patch_cols = edge_low[:, NCLS:start_freq]
    freq_cols = edge_low[:, start_freq:start_tail]
    time_second = edge_low[:, start_tail : start_tail + D]
    final_cols = edge_low[:, start_tail + D : start_tail + 3 * D]
    head_cols = edge_low[:, start_tail + 3 * D :]
    tokens = (
        low_back(mult(patches, patch_cols, "btp,dp->btd") + top_bias[:D]) + position_table()[None]
    )
    features = low(time_features(tsteps))
    time_first = low_back(mult(features, freq_cols, "bf,df->bd") + top_bias[D : 2 * D])
    time_out = low_back(
        mult(low(jax.nn.silu(time_first)), time_second, "bd,de->be") + top_bias[2 * D : 3 * D]
    )
    class_emb = jnp.take(class_cols, labels, axis=1).T
    condition = low(jax.nn.silu(time_out + class_emb))
    for layer_index in range(depth):
        tokens = block(
            tokens,
            condition,
            low(layer_in[layer_index]),
            low(layer_out[layer_index]),
            layer_bias[layer_index],
        )
    closing = low_back(mult(condition, final_cols, "bd,de->be") + top_bias[3 * D : 5 * D])
    normed = low(normalize(tokens) * (1.0 + closing[:, None, D:]) + closing[:, None, :D])
    predicted = low_back(mult(normed, head_cols, "btd,dp->btp") + top_bias[5 * D :])
    misfit = predicted[..., :PATCH_IN] - target
    return jnp.sum(misfit * misfit)


def fetch_weights(layer_in, layer_out, edge_mat, again):
    gathered_in = []
    gathered_out = []
    for layer_index in range(layer_in.shape[0]):
        own_in = layer_in[layer_index].astype(jnp.bfloat16)
        own_out = layer_out[layer_index].astype(jnp.bfloat16)
        if again:
            full_in, full_out = (
                lax.all_gather(own_in, "fsdp", axis=0, tiled=True),
                lax.all_gather(own_out, "fsdp", axis=0, tiled=True),
            )
        else:
            full_in, full_out = (
                lax.all_gather(own_in, "fsdp", axis=0, tiled=True),
                lax.all_gather(own_out, "fsdp", axis=0, tiled=True),
            )
        gathered_in.append(full_in)
        gathered_out.append(full_out)
    if again:
        full_edge = lax.all_gather(edge_mat.astype(jnp.bfloat16), "fsdp", axis=0, tiled=True)
    else:
        full_edge = lax.all_gather(edge_mat.astype(jnp.bfloat16), "fsdp", axis=0, tiled=True)
    return (
        jnp.stack(gathered_in).astype(jnp.float32),
        jnp.stack(gathered_out).astype(jnp.float32),
        full_edge.astype(jnp.float32),
    )


def step_of(grad, rows_new, cols_new, rows_mean):
    second = rows_new[:, :, None] * cols_new[:, None, :] / rows_mean[:, None, None]
    return grad * lax.rsqrt(second)


def plain(weight, grad, moment):
    moment_new = decay * moment + (1.0 - decay) * (grad * grad + eps_stat)
    update = grad * lax.rsqrt(moment_new)
    root = jnp.sqrt(jnp.mean(update * update, axis=-1, keepdims=True))
    return (weight - rate * update / jnp.maximum(1.0, root / clip_level), moment_new)


def shards(
    latents,
    tsteps,
    labels,
    noise,
    layer_in,
    layer_out,
    edge_mat,
    layer_bias,
    top_bias,
    in_rows,
    in_cols,
    out_rows,
    out_cols,
    edge_rows,
    edge_cols,
    layer_bias_v,
    top_bias_v,
):
    per_micro = latents.shape[0] // MICRO
    loss_sum = jnp.zeros((), jnp.float32)
    gradients = None

    def add_grads(total_grads, grads_now):
        if total_grads is None:
            return grads_now
        return jax.tree.map(jnp.add, total_grads, grads_now)

    for micro_index in range(MICRO):
        start = micro_index * per_micro
        data_now = (
            latents[start : start + per_micro],
            tsteps[start : start + per_micro],
            labels[start : start + per_micro],
            noise[start : start + per_micro],
        )
        again_in, again_out, again_edge = fetch_weights(layer_in, layer_out, edge_mat, True)
        params = (again_in, again_out, again_edge, layer_bias, top_bias)
        recomputed, pullback = jax.vjp(lambda params_now: image_loss(params_now, *data_now), params)
        (grads_now,) = pullback(jnp.ones_like(recomputed))
        loss_sum = loss_sum + recomputed
        gradients = add_grads(gradients, grads_now)
    grad_in_full, grad_out_full, grad_edge_full, grad_lbias, grad_tbias = gradients
    shard_in, shard_out, shard_edge = (
        lax.psum_scatter(grad_in_full, "fsdp", scatter_dimension=1, tiled=True),
        lax.psum_scatter(grad_out_full, "fsdp", scatter_dimension=1, tiled=True),
        lax.psum_scatter(grad_edge_full[None], "fsdp", scatter_dimension=1, tiled=True),
    )
    shard_in, shard_out, shard_edge = lax.psum((shard_in, shard_out, shard_edge), "rep")
    bias_in_sum, bias_top_sum, loss_total = lax.psum(
        (grad_lbias, grad_tbias, loss_sum), ("fsdp", "rep")
    )
    fsdp_count = lax.axis_size("fsdp")
    tok_total = latents.shape[0] * fsdp_count * lax.axis_size("rep") * (GRID // PATCH) ** 2
    scale_grad = 1.0 / (PATCH_IN * math.sqrt(tok_total))
    loss = loss_total / (tok_total * PATCH_IN)
    grad_in = shard_in * scale_grad
    grad_out = shard_out * scale_grad
    grad_edge = shard_edge * scale_grad
    full_rows_in = layer_in.shape[1] * fsdp_count
    full_rows_out = layer_out.shape[1] * fsdp_count
    full_rows_edge = edge_mat.shape[0] * fsdp_count
    square_in = grad_in * grad_in + eps_stat
    square_out = grad_out * grad_out + eps_stat
    square_edge = grad_edge * grad_edge + eps_stat
    rows_in_new = decay * in_rows + (1.0 - decay) * jnp.mean(square_in, axis=2)
    rows_out_new = decay * out_rows + (1.0 - decay) * jnp.mean(square_out, axis=2)
    rows_edge_new = decay * edge_rows[None] + (1.0 - decay) * jnp.mean(square_edge, axis=2)
    col_in, total_in, col_out, total_out, col_edge, total_edge = lax.psum(
        (
            jnp.sum(square_in, axis=1),
            jnp.sum(rows_in_new, axis=1),
            jnp.sum(square_out, axis=1),
            jnp.sum(rows_out_new, axis=1),
            jnp.sum(square_edge, axis=1),
            jnp.sum(rows_edge_new, axis=1),
        ),
        "fsdp",
    )
    cols_in_new = decay * in_cols + (1.0 - decay) * col_in / full_rows_in
    cols_out_new = decay * out_cols + (1.0 - decay) * col_out / full_rows_out
    cols_edge_new = decay * edge_cols[None] + (1.0 - decay) * col_edge / full_rows_edge
    update_in = step_of(grad_in, rows_in_new, cols_in_new, total_in / full_rows_in)
    update_out = step_of(grad_out, rows_out_new, cols_out_new, total_out / full_rows_out)
    update_edge = step_of(grad_edge, rows_edge_new, cols_edge_new, total_edge / full_rows_edge)
    sum_in, sum_out, sum_edge = lax.psum(
        (
            jnp.sum(update_in * update_in, axis=(1, 2)),
            jnp.sum(update_out * update_out, axis=(1, 2)),
            jnp.sum(update_edge * update_edge, axis=(1, 2)),
        ),
        "fsdp",
    )
    mean_sq_in = sum_in / (full_rows_in * grad_in.shape[2])
    mean_sq_out = sum_out / (full_rows_out * grad_out.shape[2])
    mean_sq_edge = sum_edge / (full_rows_edge * grad_edge.shape[2])
    roots_in = jnp.sqrt(mean_sq_in)
    roots_out = jnp.sqrt(mean_sq_out)
    roots_edge = jnp.sqrt(mean_sq_edge)
    factor_in = jnp.maximum(1.0, roots_in / clip_level)[:, None, None]
    factor_out = jnp.maximum(1.0, roots_out / clip_level)[:, None, None]
    factor_edge = jnp.maximum(1.0, roots_edge / clip_level)[:, None, None]
    in_new = layer_in - rate * update_in / factor_in
    out_new = layer_out - rate * update_out / factor_out
    edge_new = (edge_mat[None] - rate * update_edge / factor_edge)[0]
    clip_roots = jnp.concatenate([roots_in, roots_out, roots_edge])
    lbias_new, lbias_v_new = plain(layer_bias, bias_in_sum * scale_grad, layer_bias_v)
    tbias_new, tbias_v_new = plain(top_bias, bias_top_sum * scale_grad, top_bias_v)
    return (
        loss,
        in_new,
        out_new,
        edge_new,
        lbias_new,
        tbias_new,
        rows_in_new,
        cols_in_new,
        rows_out_new,
        cols_out_new,
        rows_edge_new[0],
        cols_edge_new[0],
        lbias_v_new,
        tbias_v_new,
        clip_roots,
    )


def solution(mesh):
    placed = (
        P(("fsdp", "rep"), None, None),
        P(("fsdp", "rep")),
        P(("fsdp", "rep")),
        P(("fsdp", "rep"), None, None),
        P(None, "fsdp", None),
        P(None, "fsdp", None),
        P("fsdp", None),
        P(),
        P(),
        P(None, "fsdp"),
        P(),
        P(None, "fsdp"),
        P(),
        P("fsdp"),
        P(),
        P(),
        P(),
    )
    return jax.shard_map(
        shards,
        mesh=mesh,
        in_specs=placed,
        out_specs=(
            P(),
            P(None, "fsdp", None),
            P(None, "fsdp", None),
            P("fsdp", None),
            P(),
            P(),
            P(None, "fsdp"),
            P(),
            P(None, "fsdp"),
            P(),
            P("fsdp"),
            P(),
            P(),
            P(),
            P(),
        ),
        check_vma=False,
    )
```

```python
import functools
import math

import jax
import jax.numpy as jnp
from jax import lax
from jax.experimental import pallas as pl
from jax.experimental.pallas import tpu as pltpu
from jax.sharding import PartitionSpec as P

NCLS = 1001
FREQ = 256
CHANNELS = 4
PATCH = 2
GRID = 32
TSTEPS = 1000
eps_stat = 1e-30
decay = 0.5
rate = 0.01
clip_level = 1.0
D = 384
HEADS = 6
HEAD_DIM = 64
FF = 1536
TOK = 256
PATCH_IN = 16
eps_norm = 1e-06
F32 = jnp.float32
BF16 = jnp.bfloat16
GELU_A = 0.7978845608028654
GELU_B = 0.044715
NT = (((1,), (1,)), ((), ()))
TN = (((0,), (0,)), ((), ()))
FFC = 512
OWN = 48


def dot(a, b, dims=(((1,), (0,)), ((), ()))):
    return lax.dot_general(a, b, dims, preferred_element_type=F32)


def norm_rows(t):
    center = t - jnp.mean(t, axis=-1, keepdims=True)
    spread = jnp.mean(center * center, axis=-1, keepdims=True)
    scale = lax.rsqrt(spread + eps_norm)
    return center * scale, scale


def norm_back(dn, n, scale):
    mean_d = jnp.mean(dn, axis=-1, keepdims=True)
    mean_dn = jnp.mean(dn * n, axis=-1, keepdims=True)
    return scale * (dn - mean_d - n * mean_dn)


def rows_sum(v):
    return jnp.sum(v, axis=0, keepdims=True)


def soft_rows(s):
    e = jnp.exp(s - jnp.max(s, axis=-1, keepdims=True))
    return e / jnp.sum(e, axis=-1, keepdims=True)


def gelu_parts(x):
    t = jnp.tanh(GELU_A * (x + GELU_B * (x * x * x)))
    return t


QKV = 0
WO = 3 * D
WF1 = 4 * D
BQ, BV, BO, BF1, BF2 = 0, D, 2 * D, 3 * D, 3 * D + FF
BW = 4 * D + FF


def compute_kernel(
    images,
    group,
    blocked,
    patches_ref,
    target_ref,
    pos_ref,
    mods_ref,
    w_in_ref,
    w_out_ref,
    w_patch_ref,
    w_head_ref,
    bias_ref,
    bpatch_ref,
    bhead_ref,
    g_in_ref,
    g_out_ref,
    g_patch_ref,
    g_head_ref,
    g_bias_ref,
    g_bpatch_ref,
    g_bhead_ref,
    g_mods_ref,
    sse_ref,
    tok,
    mid,
    qkv,
    att,
    branch,
    outb,
    normed,
    act,
    dinner,
    dsmall,
    dqkv,
    stage,
    sems,
):
    steps = images // group
    crow = group * TOK
    lane = lax.broadcasted_iota(jnp.int32, (TOK, 128), 1)
    first_half = lane < HEAD_DIM

    def rows_of(i):
        return pl.ds(pl.multiple_of(i * TOK, TOK), TOK)

    def chunk_of(i):
        return pl.ds(pl.multiple_of(i * crow, crow), crow)

    def mod_row(b, k):
        return mods_ref[b, pl.ds(k, 1), :]

    g_bias_ref[...] = jnp.zeros_like(g_bias_ref)
    g_patch_ref[...] = jnp.zeros_like(g_patch_ref)
    g_head_ref[...] = jnp.zeros_like(g_head_ref)
    g_bpatch_ref[...] = jnp.zeros_like(g_bpatch_ref)
    g_bhead_ref[...] = jnp.zeros_like(g_bhead_ref)
    sse_ref[...] = jnp.zeros_like(sse_ref)
    depth = w_in_ref.shape[0]

    @pl.loop(0, images)
    def _(b):
        r = rows_of(b)
        tok[0, r, :] = dot(patches_ref[r, :], w_patch_ref[...], NT) + bpatch_ref[...] + pos_ref[...]

    def half(v, which):
        zero = jnp.zeros_like(v)
        return jnp.where(first_half, v, zero) if which == 0 else jnp.where(first_half, zero, v)

    def attention(layer, r):
        for pair in range(HEADS // 2):
            c = pair * 128
            q = qkv[layer, r, c : c + 128]
            k = qkv[layer, r, D + c : D + c + 128]
            v = qkv[layer, r, 2 * D + c : 2 * D + c + 128]
            got = []
            for which in range(2):
                s = dot(half(q, which), k, NT) * HEAD_DIM ** (-0.5)
                got.append(dot(soft_rows(s).astype(BF16), v))
            att[layer, r, c : c + 128] = jnp.where(first_half, got[0], got[1]).astype(BF16)

    def modulated(t, b, k):
        n, scale = norm_rows(t)
        return n, scale, (n * (1.0 + mod_row(b, k + 1)) + mod_row(b, k)).astype(BF16)

    for layer in range(depth):
        mo = layer * 6

        @pl.loop(0, steps)
        def _(i):
            cr = chunk_of(i)
            for j in range(group):
                b = i * group + j
                r = rows_of(b)
                normed[r, :] = modulated(tok[layer, r, :], b, mo)[2]
            hc = normed[cr, :]
            for part in range(3):
                p = dot(hc, w_in_ref[layer, :, QKV + part * D : QKV + (part + 1) * D])
                if part == 0:
                    p = p + bias_ref[layer : layer + 1, BQ : BQ + D]
                if part == 2:
                    p = p + bias_ref[layer : layer + 1, BV : BV + D]
                qkv[layer, cr, part * D : (part + 1) * D] = p.astype(BF16)
            for j in range(group):
                attention(layer, rows_of(i * group + j))
            br = dot(att[layer, cr, :], w_in_ref[layer, :, WO : WO + D]) + bias_ref[layer : layer + 1, BO : BO + D]
            branch[layer, cr, :] = br.astype(BF16)
            for j in range(group):
                b = i * group + j
                r = rows_of(b)
                t2 = tok[layer, r, :] + mod_row(b, mo + 2) * br[j * TOK : (j + 1) * TOK]
                mid[layer, r, :] = t2
                normed[r, :] = modulated(t2, b, mo + 3)[2]
            mc = normed[cr, :]
            out = jnp.zeros((crow, D), F32) + bias_ref[layer : layer + 1, BF2 : BF2 + D]
            for c in range(0, FF, FFC):
                x = dot(mc, w_in_ref[layer, :, WF1 + c : WF1 + c + FFC]) + bias_ref[layer : layer + 1, BF1 + c : BF1 + c + FFC]
                a = (x * (0.5 * (1.0 + gelu_parts(x)))).astype(BF16)
                out = out + dot(a, w_out_ref[layer, c : c + FFC, :])
            outb[layer, cr, :] = out.astype(BF16)
            for j in range(group):
                b = i * group + j
                r = rows_of(b)
                tok[layer + 1, r, :] = mid[layer, r, :] + mod_row(b, mo + 5) * out[j * TOK : (j + 1) * TOK]

    dtok = tok.at[depth]

    @pl.loop(0, images)
    def _(b):
        r = rows_of(b)
        k = 6 * depth
        n, scale, n3 = modulated(dtok[r, :], b, k)
        miss = dot(n3, w_head_ref[...], NT) + bhead_ref[...] - target_ref[r, :]
        sse_ref[...] += jnp.sum(rows_sum(miss * miss), axis=1, keepdims=True)
        dp = (2.0 * miss).astype(BF16)
        g_head_ref[...] += dot(dp, n3, TN)
        g_bhead_ref[...] += rows_sum(dp.astype(F32))
        dn3 = dot(dp, w_head_ref[...])
        g_mods_ref[b, pl.ds(k, 1), :] = rows_sum(dn3)
        g_mods_ref[b, pl.ds(k + 1, 1), :] = rows_sum(dn3 * n)
        dtok[r, :] = norm_back(dn3 * (1.0 + mod_row(b, k + 1)), n, scale)

    pending = {}

    def free(slot):
        for copy in pending.pop(slot, ()):
            copy.wait()

    def send_in(layer, first):
        slot = 0
        moves = []
        for q in range(4):
            source = stage.at[slot, :, q * D : (q + 1) * D]
            if blocked:
                target = (g_in_ref if first == QKV else g_out_ref).at[layer, q, :, 0:D]
            else:
                target = g_in_ref.at[layer, :, first + q * D : first + (q + 1) * D]
            moves.append(pltpu.make_async_copy(source, target, sems.at[slot, q]))
        for move in moves:
            move.start()
        pending[slot] = moves

    def send_down(layer):
        slot = 1
        moves = []
        for c in range(4):
            if not blocked:
                source = stage.at[slot, :, c * D : (c + 1) * D]
                target = g_out_ref.at[layer, c * D : (c + 1) * D, :]
                moves.append(pltpu.make_async_copy(source, target, sems.at[slot, c]))
                continue
            for owner in range(2):
                for q in range(4):
                    start = owner * (D // 2) + q * OWN
                    source = stage.at[slot, start : start + OWN, c * D : (c + 1) * D]
                    begin = (2 * c + owner) * OWN
                    target = g_out_ref.at[layer, q, begin : begin + OWN, D : 2 * D]
                    moves.append(pltpu.make_async_copy(source, target, sems.at[slot, len(moves)]))
        for move in moves:
            move.start()
        pending[slot] = moves

    for layer in reversed(range(depth)):
        mo = layer * 6
        lb = slice(layer, layer + 1)

        @pl.loop(0, steps)
        def _(i):
            cr = chunk_of(i)
            for j in range(group):
                b = i * group + j
                r = rows_of(b)
                normed[r, :] = modulated(mid[layer, r, :], b, mo + 3)[2]
                d = dtok[r, :]
                g_mods_ref[b, pl.ds(mo + 5, 1), :] = rows_sum(d * outb[layer, r, :].astype(F32))
                do = (d * mod_row(b, mo + 5)).astype(BF16)
                dsmall[r, :] = do
                g_bias_ref[lb, BF2 : BF2 + D] += rows_sum(do.astype(F32))
            mc = normed[cr, :]
            do = dsmall[cr, :]
            dm = jnp.zeros((crow, D), F32)
            for c in range(0, FF, FFC):
                x = dot(mc, w_in_ref[layer, :, WF1 + c : WF1 + c + FFC]) + bias_ref[lb, BF1 + c : BF1 + c + FFC]
                x2 = x * x
                t = jnp.tanh(GELU_A * (x + GELU_B * (x2 * x)))
                cdf = 0.5 * (1.0 + t)
                act[cr, c : c + FFC] = (x * cdf).astype(BF16)
                slope = cdf + (0.5 * GELU_A) * x * (1.0 - t * t) * (1.0 + (3.0 * GELU_B) * x2)
                di = (dot(do, w_out_ref[layer, c : c + FFC, :], NT) * slope).astype(BF16)
                dinner[cr, c : c + FFC] = di
                g_bias_ref[lb, BF1 + c : BF1 + c + FFC] += rows_sum(di.astype(F32))
                dm = dm + dot(di, w_in_ref[layer, :, WF1 + c : WF1 + c + FFC], NT)
            for j in range(group):
                b = i * group + j
                r = rows_of(b)
                n, scale = norm_rows(mid[layer, r, :])
                dmj = dm[j * TOK : (j + 1) * TOK]
                g_mods_ref[b, pl.ds(mo + 3, 1), :] = rows_sum(dmj)
                g_mods_ref[b, pl.ds(mo + 4, 1), :] = rows_sum(dmj * n)
                dtok[r, :] = dtok[r, :] + norm_back(dmj * (1.0 + mod_row(b, mo + 4)), n, scale)

        free(0)

        @pl.loop(0, FF // D)
        def _(c):
            cs = pl.ds(pl.multiple_of(c * D, D), D)
            stage[0, :, cs] = dot(normed[...], dinner[:, cs], TN)

        send_in(layer, WF1)
        free(1)

        @pl.loop(0, FF // D)
        def _(c):
            cs = pl.ds(pl.multiple_of(c * D, D), D)
            stage[1, :, cs] = dot(dsmall[...], act[:, cs], TN).T

        send_down(layer)

        @pl.loop(0, steps)
        def _(i):
            cr = chunk_of(i)
            for j in range(group):
                b = i * group + j
                r = rows_of(b)
                d = dtok[r, :]
                g_mods_ref[b, pl.ds(mo + 2, 1), :] = rows_sum(d * branch[layer, r, :].astype(F32))
                db = (d * mod_row(b, mo + 2)).astype(BF16)
                dsmall[r, :] = db
                g_bias_ref[lb, BO : BO + D] += rows_sum(db.astype(F32))
            branch[layer, cr, :] = dot(dsmall[cr, :], w_in_ref[layer, :, WO : WO + D], NT).astype(BF16)
            for j in range(group):
                r = rows_of(i * group + j)
                for pair in range(HEADS // 2):
                    c = pair * 128
                    q = qkv[layer, r, c : c + 128]
                    k = qkv[layer, r, D + c : D + c + 128]
                    v = qkv[layer, r, 2 * D + c : 2 * D + c + 128]
                    da = branch[layer, r, c : c + 128]
                    got = []
                    for which in range(2):
                        s = dot(half(q, which), k, NT) * HEAD_DIM ** (-0.5)
                        p = soft_rows(s)
                        dv = dot(p.astype(BF16), da, TN)
                        dpr = dot(half(da, which), v, NT)
                        ds = p * (dpr - jnp.sum(dpr * p, axis=-1, keepdims=True))
                        ds = ds.astype(BF16)
                        dq = dot(ds, k)
                        dk = dot(ds, q, TN)
                        got.append((dq, dk, dv))
                    dq = (jnp.where(first_half, got[0][0], got[1][0]) * HEAD_DIM ** (-0.5)).astype(BF16)
                    dk = (jnp.where(first_half, got[0][1], got[1][1]) * HEAD_DIM ** (-0.5)).astype(BF16)
                    dv = jnp.where(first_half, got[0][2], got[1][2]).astype(BF16)
                    dqkv[r, c : c + 128] = dq
                    dqkv[r, D + c : D + c + 128] = dk
                    dqkv[r, 2 * D + c : 2 * D + c + 128] = dv
                    g_bias_ref[lb, BQ + c : BQ + c + 128] += rows_sum(dq.astype(F32))
                    g_bias_ref[lb, BV + c : BV + c + 128] += rows_sum(dv.astype(F32))
            dh = dot(dqkv[cr, :], w_in_ref[layer, :, QKV : QKV + 3 * D], NT)
            for j in range(group):
                b = i * group + j
                r = rows_of(b)
                n, scale, h = modulated(tok[layer, r, :], b, mo)
                normed[r, :] = h
                dhj = dh[j * TOK : (j + 1) * TOK]
                g_mods_ref[b, pl.ds(mo, 1), :] = rows_sum(dhj)
                g_mods_ref[b, pl.ds(mo + 1, 1), :] = rows_sum(dhj * n)
                dtok[r, :] = dtok[r, :] + norm_back(dhj * (1.0 + mod_row(b, mo + 1)), n, scale)

        free(0)

        @pl.loop(0, 3)
        def _(c):
            cs = pl.ds(pl.multiple_of(c * D, D), D)
            stage[0, :, cs] = dot(normed[...], dqkv[:, cs], TN)

        stage[0, :, 3 * D : 4 * D] = dot(att[layer], dsmall[...], TN)
        send_in(layer, QKV)
        free(1)

    @pl.loop(0, images)
    def _(b):
        r = rows_of(b)
        d = dtok[r, :].astype(BF16)
        g_bpatch_ref[...] += rows_sum(d.astype(F32))
        g_patch_ref[...] += dot(patches_ref[r, :], d, TN)

    free(0)


def compute(patches, target, pos, mods, w_in, w_out, w_patch, w_head_t, bias, bpatch, bhead, group=3, blocked=False):
    depth = w_in.shape[0]
    rows = patches.shape[0]
    images = rows // TOK
    kinds = mods.shape[1]
    vm = pl.BlockSpec(memory_space=pltpu.VMEM)
    anyspace = pl.BlockSpec(memory_space=pl.ANY)
    shape = jax.ShapeDtypeStruct
    return pl.pallas_call(
        functools.partial(compute_kernel, images, group, blocked),
        out_shape=(
            shape((depth, 4, D, D) if blocked else (depth, D, 4 * D + FF), F32),
            shape((depth, 4, D, 2 * D) if blocked else (depth, FF, D), F32),
            shape((PATCH_IN, D), F32),
            shape((PATCH_IN, D), F32),
            shape((depth, BW), F32),
            shape((1, D), F32),
            shape((1, PATCH_IN), F32),
            shape((images, kinds, D), F32),
            shape((1, 1), F32),
        ),
        in_specs=[vm] * 11,
        out_specs=(anyspace, anyspace, vm, vm, vm, vm, vm, vm, vm),
        scratch_shapes=[
            pltpu.VMEM((depth + 1, rows, D), F32),
            pltpu.VMEM((depth, rows, D), F32),
            pltpu.VMEM((depth, rows, 3 * D), BF16),
            pltpu.VMEM((depth, rows, D), BF16),
            pltpu.VMEM((depth, rows, D), BF16),
            pltpu.VMEM((depth, rows, D), BF16),
            pltpu.VMEM((rows, D), BF16),
            pltpu.VMEM((rows, FF), BF16),
            pltpu.VMEM((rows, FF), BF16),
            pltpu.VMEM((rows, D), BF16),
            pltpu.VMEM((rows, 3 * D), BF16),
            pltpu.VMEM((2, D, FF), F32),
            pltpu.SemaphoreType.DMA((2, 32)),
        ],
        compiler_params=pltpu.CompilerParams(vmem_limit_bytes=60 * 1024 * 1024),
        name="step_compute",
    )(patches, target, pos, mods, w_in, w_out, w_patch, w_head_t, bias, bpatch, bhead)


def place():
    f = lax.axis_index("fsdp")
    r = lax.axis_index("rep")
    z = f // 2
    y = f - 2 * z
    x = r // 2
    c = r - 2 * x
    return z, y, x, c


def device(z, y, x, c):
    return {"fsdp": 2 * z + y, "rep": 2 * x + c}


def greet(peers):
    barrier = pltpu.get_barrier_semaphore()
    for peer in peers:
        pl.semaphore_signal(barrier, inc=1, device_id=peer, device_id_type=pl.DeviceIdType.MESH)
    pl.semaphore_wait(barrier, len(peers))


def remote(source, target, send, recv, peer):
    return pltpu.make_async_remote_copy(
        src_ref=source, dst_ref=target, send_sem=send, recv_sem=recv, device_id=peer, device_id_type=pl.DeviceIdType.MESH
    )


class Reducer:
    def __init__(self, source, bufs, out, sends, recvs, loads):
        self.source = source
        self.keep, self.got0, self.sx, self.gotx, self.sy, self.goty, self.sz, self.gotz, self.sw, self.gotw = bufs
        self.out = out
        self.sends, self.recvs, self.loads = sends, recvs, loads
        self.link = self.sx.dtype
        self.z, self.y, self.x, self.c = place()
        z, y, x, c = self.z, self.y, self.x, self.c
        self.to_c = device(z, y, x, 1 - c)
        self.to_x = device(z, y, 1 - x, c)
        self.to_y = device(z, 1 - y, x, c)
        self.z1 = z + 1 - 2 * lax.rem(z, 2)
        self.z2 = lax.rem(z + 2, 4)
        self.to_z1 = device(self.z1, y, x, c)
        self.to_z2 = device(self.z2, y, x, c)
        self.moves = {}

    def send(self, slot, source, target, peer):
        copy = remote(source, target, self.sends.at[slot], self.recvs.at[slot], peer)
        copy.start()
        self.moves[slot] = copy

    def step(self, k):
        z, y, x, c = self.z, self.y, self.x, self.c
        if k == 0:
            for half in range(2):
                load = pltpu.make_async_copy(self.source.at[2 * half + c], self.keep.at[half], self.loads.at[half])
                load.start()
                self.moves["load", half] = load
                self.send(half, self.source.at[2 * half + 1 - c], self.got0.at[half], self.to_c)
        if k == 1:
            for half in range(2):
                self.moves["load", half].wait()
                self.moves[half].wait()

            @pl.loop(0, 4)
            def _(i):
                for j in range(2):
                    self.sx[i, j] = (self.keep[1 - x, i, j] + self.got0[1 - x, i, j]).astype(self.link)

            self.send(2, self.sx, self.gotx, self.to_x)

            @pl.loop(0, 4)
            def _(i):
                for j in range(2):
                    self.keep[x, i, j] = self.keep[x, i, j] + self.got0[x, i, j]
        if k == 2:
            self.moves[2].wait()

            @pl.loop(0, 4)
            def _(i):
                self.sy[i] = (self.keep[x, i, 1 - y] + self.gotx[i, 1 - y].astype(F32)).astype(self.link)

            self.send(3, self.sy, self.goty, self.to_y)

            @pl.loop(0, 4)
            def _(i):
                self.keep[x, i, y] = self.keep[x, i, y] + self.gotx[i, y].astype(F32)
        if k == 3:
            self.moves[3].wait()
            for s in range(2):
                at = lax.rem(self.z1 + 2 * s, 4)
                self.sz[s] = (self.keep[x, at, y] + self.goty[at].astype(F32)).astype(self.link)
            self.send(4, self.sz, self.gotz, self.to_z1)
            for s in range(2):
                at = lax.rem(z + 2 * s, 4)
                self.keep[x, at, y] = self.keep[x, at, y] + self.goty[at].astype(F32)
        if k == 4:
            self.moves[4].wait()
            self.sw[...] = (self.keep[x, self.z2, y] + self.gotz[1].astype(F32)).astype(self.link)
            self.send(5, self.sw, self.gotw, self.to_z2)
        if k == 5:
            self.moves[5].wait()
            mine = 2 * x + c
            self.out[mine] = self.keep[x, z, y] + self.gotz[0].astype(F32) + self.gotw[...].astype(F32)
            self.send(6, self.out.at[mine], self.out.at[mine], self.to_x)
            self.send(7, self.out.at[mine], self.out.at[mine], self.to_c)
        if k == 6:
            self.moves[6].wait()
            other = 2 * (1 - x) + c
            self.send(8, self.out.at[other], self.out.at[other], self.to_c)
        if k == 7:
            self.moves[7].wait()
            self.moves[8].wait()

    def peers(self):
        return [self.to_c, self.to_x, self.to_y, self.to_z1, self.to_z2]


REDUCER_STEPS = 8


def reducer_scratch(width, own=OWN, link=BF16):
    return [
        pltpu.VMEM((2, 4, 2, own, width), F32),
        pltpu.VMEM((2, 4, 2, own, width), F32),
        pltpu.VMEM((4, 2, own, width), link),
        pltpu.VMEM((4, 2, own, width), link),
        pltpu.VMEM((4, own, width), link),
        pltpu.VMEM((4, own, width), link),
        pltpu.VMEM((2, own, width), link),
        pltpu.VMEM((2, own, width), link),
        pltpu.VMEM((own, width), link),
        pltpu.VMEM((own, width), link),
    ]


def reduce_kernel(depth, t_ref, m_ref, s_ref, out_t_ref, out_m_ref, out_s_ref, *scratch):
    sends, recvs, loads = scratch[-3:]
    pieces = []

    def piece(source, out):
        n = len(pieces)
        pieces.append(Reducer(source, scratch[10 * n : 10 * n + 10], out, sends.at[n], recvs.at[n], loads.at[n]))

    for layer in reversed(range(depth)):
        piece(m_ref.at[layer], out_m_ref.at[layer])
        piece(t_ref.at[layer], out_t_ref.at[layer])
    piece(s_ref, out_s_ref)
    greet(pieces[0].peers())
    for t in range(REDUCER_STEPS + len(pieces) - 1):
        for n, one in enumerate(pieces):
            if 0 <= t - n < REDUCER_STEPS:
                one.step(t - n)


def reduce_grads(g_t, g_m, small):
    depth = g_t.shape[0]
    shape = jax.ShapeDtypeStruct
    scratch = []
    for _ in range(depth):
        scratch += reducer_scratch(2 * D) + reducer_scratch(D)
    scratch += reducer_scratch(128, 8, F32)
    count = 2 * depth + 1
    scratch += [pltpu.SemaphoreType.DMA((count, 9)), pltpu.SemaphoreType.DMA((count, 9)), pltpu.SemaphoreType.DMA((count, 2))]
    anyspace = pl.BlockSpec(memory_space=pl.ANY)
    vm = pl.BlockSpec(memory_space=pltpu.VMEM)
    return pl.pallas_call(
        functools.partial(reduce_kernel, depth),
        out_shape=(shape((depth, 4, OWN, D), F32), shape((depth, 4, OWN, 2 * D), F32), shape((4, 8, 128), F32)),
        in_specs=[anyspace] * 3,
        out_specs=(vm, vm, vm),
        scratch_shapes=scratch,
        compiler_params=pltpu.CompilerParams(collective_id=1, has_side_effects=True, vmem_limit_bytes=60 * 1024 * 1024),
        name="step_reduce",
    )(g_t.reshape(depth, 4, 4, 2, OWN, D), g_m.reshape(depth, 4, 4, 2, OWN, 2 * D), small)


class Gatherer:
    def __init__(self, source, target, whole, sends, recvs, local):
        self.source, self.target, self.whole = source, target, whole
        self.sends, self.recvs, self.local = sends, recvs, local
        self.z, self.y, self.x, self.c = place()
        self.q = 2 * self.x + self.c
        self.moves = {}

    def send(self, slot, source, target, peer):
        copy = remote(source, target, self.sends.at[slot], self.recvs.at[slot], peer)
        copy.start()
        self.moves[slot] = copy

    def step(self, k):
        z, y, x, c, q = self.z, self.y, self.x, self.c, self.q
        f = 2 * z + y
        if k == 0:
            for d in range(1, 4):
                peer = lax.rem(z + d, 4)
                self.send(d - 1, self.source(q), self.target(f, q), device(peer, y, x, c))
            self.send(3, self.source(q), self.target(f, q), device(z, 1 - y, x, c))
            own = pltpu.make_async_copy(self.source(q), self.target(f, q), self.local)
            own.start()
            self.moves["own"] = own
        if k == 1:
            for d in range(1, 4):
                self.moves[d - 1].wait()
                at = 2 * lax.rem(z + 4 - d, 4) + y
                self.send(3 + d, self.target(at, q), self.target(at, q), device(z, 1 - y, x, c))
        if k == 2:
            self.moves["own"].wait()
            for slot in range(3, 7):
                self.moves[slot].wait()
            self.send(7, self.whole(q), self.whole(q), device(z, y, 1 - x, c))
            self.send(8, self.whole(q), self.whole(q), device(z, y, x, 1 - c))
        if k == 3:
            self.moves[7].wait()
            other = 2 * (1 - x) + c
            self.send(9, self.whole(other), self.whole(other), device(z, y, x, 1 - c))
        if k == 4:
            self.moves[8].wait()
            self.moves[9].wait()

    def peers(self):
        z, y, x, c = self.z, self.y, self.x, self.c
        return [device(lax.rem(z + d, 4), y, x, c) for d in range(1, 4)] + [
            device(z, 1 - y, x, c),
            device(z, y, 1 - x, c),
            device(z, y, x, 1 - c),
        ]


GATHER_STEPS = 5


def by_columns(source, target, sends, recvs, local):
    rows, width = source.shape
    part = width // 4

    def cols(q):
        return pl.ds(pl.multiple_of(q * part, 128), part)

    def rows_of(f):
        return pl.ds(pl.multiple_of(f * rows, 16), rows)

    return Gatherer(
        lambda q: source.at[:, cols(q)],
        lambda f, q: target.at[rows_of(f), cols(q)],
        lambda q: target.at[:, cols(q)],
        sends,
        recvs,
        local,
    )


def by_rows(source, target, sends, recvs, local):
    return Gatherer(
        lambda q: source.at[q],
        lambda f, q: target.at[f, q],
        lambda q: target.at[:, q],
        sends,
        recvs,
        local,
    )


def gather_kernel(kinds, *refs):
    n = len(kinds)
    sends, recvs, local = refs[-3:]
    pieces = []
    for i, kind in enumerate(kinds):
        make = by_columns if kind == "columns" else by_rows
        pieces.append(make(refs[i], refs[n + i], sends.at[i], recvs.at[i], local.at[i]))
    greet(pieces[0].peers())
    for t in range(GATHER_STEPS + n - 1):
        for i, piece in enumerate(pieces):
            if 0 <= t - i < GATHER_STEPS:
                piece.step(t - i)


def gather(items, ident, space=pltpu.VMEM):
    kinds = tuple(kind for kind, _ in items)
    n = len(items)
    outs = tuple(
        jax.ShapeDtypeStruct((8 * v.shape[0],) + v.shape[1:] if kind == "columns" else (8,) + v.shape, v.dtype)
        for kind, v in items
    )
    return pl.pallas_call(
        functools.partial(gather_kernel, kinds),
        out_shape=outs,
        in_specs=[pl.BlockSpec(memory_space=pl.ANY)] * n,
        out_specs=tuple(pl.BlockSpec(memory_space=space) for _ in items),
        scratch_shapes=[
            pltpu.SemaphoreType.DMA((n, 10)),
            pltpu.SemaphoreType.DMA((n, 10)),
            pltpu.SemaphoreType.DMA((n,)),
        ],
        compiler_params=pltpu.CompilerParams(collective_id=ident, has_side_effects=True, vmem_limit_bytes=60 * 1024 * 1024),
        name="step_gather",
    )(*[v for _, v in items])


def exchange_kernel(axes, count, x_ref, out_ref, sends, recvs, local):
    sizes = [lax.axis_size(a) for a in axes]
    me = lax.axis_index(axes[0])
    for a in axes[1:]:
        me = me * lax.axis_size(a) + lax.axis_index(a)

    def peer_of(k):
        other = lax.rem(me + k, count)
        if len(axes) == 1:
            return {axes[0]: other}
        return {axes[0]: other // sizes[1], axes[1]: lax.rem(other, sizes[1])}

    greet([peer_of(k) for k in range(1, count)])
    own = pltpu.make_async_copy(x_ref, out_ref.at[me], local)
    own.start()
    copies = []
    for k in range(1, count):
        copies.append(remote(x_ref, out_ref.at[me], sends.at[k - 1], recvs.at[k - 1], peer_of(k)))
        copies[-1].start()
    own.wait()
    for copy in copies:
        copy.wait()


def exchange(x, axes, count, ident):
    vm = pl.BlockSpec(memory_space=pltpu.VMEM)
    return pl.pallas_call(
        functools.partial(exchange_kernel, axes, count),
        out_shape=jax.ShapeDtypeStruct((count,) + x.shape, x.dtype),
        in_specs=[vm],
        out_specs=vm,
        scratch_shapes=[
            pltpu.SemaphoreType.DMA((count - 1,)),
            pltpu.SemaphoreType.DMA((count - 1,)),
            pltpu.SemaphoreType.DMA,
        ],
        compiler_params=pltpu.CompilerParams(collective_id=ident, has_side_effects=True),
        name="step_exchange",
    )(x)


def swap_kernel(count, x_ref, out_ref, got, sends, recvs, local):
    me = lax.axis_index("fsdp")
    peers = [{"fsdp": lax.rem(me + k, count)} for k in range(1, count)]
    greet(peers)
    own = pltpu.make_async_copy(x_ref.at[me], got.at[me], local)
    own.start()
    copies = []
    for k in range(1, count):
        copies.append(remote(x_ref.at[lax.rem(me + k, count)], got.at[me], sends.at[k - 1], recvs.at[k - 1], peers[k - 1]))
        copies[-1].start()
    own.wait()
    for copy in copies:
        copy.wait()
    total = got[0]
    for k in range(1, count):
        total = total + got[k]
    out_ref[...] = total


def swap_sum(x, ident):
    count = x.shape[0]
    vm = pl.BlockSpec(memory_space=pltpu.VMEM)
    return pl.pallas_call(
        functools.partial(swap_kernel, count),
        out_shape=jax.ShapeDtypeStruct(x.shape[1:], x.dtype),
        in_specs=[vm],
        out_specs=vm,
        scratch_shapes=[
            pltpu.VMEM(x.shape, x.dtype),
            pltpu.SemaphoreType.DMA((count - 1,)),
            pltpu.SemaphoreType.DMA((count - 1,)),
            pltpu.SemaphoreType.DMA,
        ],
        compiler_params=pltpu.CompilerParams(collective_id=ident, has_side_effects=True),
        name="step_swap",
    )(x)


def mix_weights(tsteps):
    betas = 0.0001 + (0.02 - 0.0001) * jnp.arange(TSTEPS, dtype=jnp.float32) / (TSTEPS - 1)
    alpha_bar = jnp.exp(jnp.cumsum(jnp.log(1.0 - betas)))
    picked = jnp.arange(TSTEPS)[None, :] == tsteps[:, None]
    return jnp.sum(jnp.where(picked, alpha_bar[None, :], 0.0), axis=1)


def patchify(latent_rows):
    images = latent_rows.shape[0]
    grid_side = GRID // PATCH
    shaped = latent_rows.reshape(images, CHANNELS, grid_side, PATCH, grid_side, PATCH)
    shaped = jnp.transpose(shaped, (0, 2, 4, 1, 3, 5))
    return shaped.reshape(images, grid_side * grid_side, CHANNELS * PATCH * PATCH)


def position_table():
    grid_side = GRID // PATCH
    quarter = D // 4
    omegas = 1.0 / 10000.0 ** (jnp.arange(quarter, dtype=jnp.float32) / quarter)
    places = jnp.arange(grid_side * grid_side)
    across = (places % grid_side).astype(jnp.float32)
    downward = (places // grid_side).astype(jnp.float32)

    def one_axis(coords):
        angles = coords[:, None] * omegas[None, :]
        return jnp.concatenate([jnp.sin(angles), jnp.cos(angles)], axis=1)

    return jnp.concatenate([one_axis(across), one_axis(downward)], axis=1)


def time_features(tsteps):
    half_freq = FREQ // 2
    frequencies = jnp.exp(-math.log(10000.0) * jnp.arange(half_freq, dtype=jnp.float32) / half_freq)
    angles = tsteps.astype(jnp.float32)[:, None] * frequencies[None, :]
    return jnp.concatenate([jnp.cos(angles), jnp.sin(angles)], axis=1)


def fetch(layer_in, layer_out, direct):
    own_in = layer_in[:, :, 6 * D :].astype(BF16)
    own_out = layer_out.astype(BF16)
    depth = layer_in.shape[0]
    if direct:
        items = []
        for layer in range(depth):
            items.append(("columns", own_in[layer]))
            items.append(("rows", own_out[layer].reshape(4, OWN, D)))
        got = gather(items, 2)
        return jnp.stack(got[0::2]), jnp.stack([v.reshape(FF, D) for v in got[1::2]])
    w_in = lax.all_gather(own_in, "fsdp", axis=1, tiled=True)
    w_out = lax.all_gather(own_out, "fsdp", axis=1, tiled=True)
    return w_in, w_out


def silu_slope(x):
    gate = jax.nn.sigmoid(x)
    return gate * (1.0 + x * (1.0 - gate))


def matmul(a, b, form):
    return jnp.einsum(form, a, b, preferred_element_type=F32)


def step_of(grad, rows_new, cols_new, rows_mean):
    second = rows_new[:, :, None] * cols_new[:, None, :] / rows_mean[:, None, None]
    return grad * lax.rsqrt(second)


def plain(weight, grad, moment):
    moment_new = decay * moment + (1.0 - decay) * (grad * grad + eps_stat)
    update = grad * lax.rsqrt(moment_new)
    root = jnp.sqrt(jnp.mean(update * update, axis=-1, keepdims=True))
    return (weight - rate * update / jnp.maximum(1.0, root / clip_level), moment_new)


def shards(
    latents,
    tsteps,
    labels,
    noise,
    layer_in,
    layer_out,
    edge_mat,
    layer_bias,
    top_bias,
    in_rows,
    in_cols,
    out_rows,
    out_cols,
    edge_rows,
    edge_cols,
    layer_bias_v,
    top_bias_v,
):
    images = latents.shape[0]
    depth, own, wide = layer_in.shape
    fsdp = lax.axis_size("fsdp")
    rep = lax.axis_size("rep")
    at_f = lax.axis_index("fsdp")
    at_r = lax.axis_index("rep")
    every = images * fsdp * rep
    direct = (fsdp, rep, own) == (8, 4, OWN)
    width = own * fsdp
    MOD = 6 * D
    start_freq = NCLS + PATCH_IN
    start_tail = start_freq + FREQ

    edge_low = edge_mat.astype(BF16)
    small = jnp.concatenate([edge_low[:, : start_tail + D], edge_low[:, start_tail + 3 * D :]], axis=1)
    if direct:
        small = jnp.pad(small, ((0, 0), (0, -small.shape[1] % 512)))
        full = gather([("columns", small)], 3)[0]
    else:
        full = lax.all_gather(small, "fsdp", axis=0, tiled=True)
    class_cols = full[:, :NCLS]
    patch_cols = full[:, NCLS:start_freq]
    freq_cols = full[:, start_freq:start_tail]
    time_second = full[:, start_tail : start_tail + D]
    head_cols = full[:, start_tail + D : start_tail + D + PATCH_IN]
    if direct:
        both = jnp.pad(jnp.stack([tsteps, labels]), ((0, 6), (0, 128 - images)))
        both = exchange(both, ("fsdp", "rep"), fsdp * rep, 4)
        all_tsteps = both[:, 0, :images].reshape(every)
        all_labels = both[:, 1, :images].reshape(every)
    else:
        all_tsteps = lax.all_gather(tsteps, ("fsdp", "rep"), axis=0, tiled=True)
        all_labels = lax.all_gather(labels, ("fsdp", "rep"), axis=0, tiled=True)
    features = time_features(all_tsteps).astype(BF16)
    time1 = matmul(features, freq_cols, "bf,df->bd") + top_bias[D : 2 * D]
    s1 = jax.nn.silu(time1).astype(BF16)
    picked = (all_labels[:, None] == jnp.arange(NCLS)[None, :]).astype(BF16)
    before = matmul(s1, time_second, "bd,de->be") + top_bias[2 * D : 3 * D] + matmul(picked, class_cols, "bc,dc->bd")
    cond = jax.nn.silu(before).astype(BF16)

    def own_part(values):
        return lax.dynamic_slice_in_dim(values, at_f * own, own, axis=1)

    low_in = layer_in.astype(BF16)
    w_mods = jnp.concatenate(
        [low_in[layer, :, :MOD] for layer in range(depth)] + [edge_low[:, start_tail + D : start_tail + 3 * D]], axis=1
    )
    cond_own = own_part(cond)
    group_own = lax.dynamic_index_in_dim(cond_own.reshape(fsdp, rep, images, own), at_r, axis=1, keepdims=False)
    part = matmul(group_own.reshape(fsdp * images, own), w_mods, "bd,de->be")
    bias_mods = jnp.concatenate([layer_bias[layer, :MOD] for layer in range(depth)] + [top_bias[3 * D : 5 * D]])
    kinds = 6 * depth + 2
    if direct:
        mods = swap_sum(jnp.pad(part.reshape(fsdp, images, kinds * D), ((0, 0), (0, 8 - images), (0, 0))), 5)[:images]
    else:
        mods = lax.psum_scatter(part, "fsdp", scatter_dimension=0, tiled=True)
    mods = (mods + bias_mods).reshape(images, kinds, D)

    alphas = mix_weights(tsteps)
    noisy = jnp.sqrt(alphas)[:, None, None] * latents + jnp.sqrt(1.0 - alphas)[:, None, None] * noise
    patches = patchify(noisy).astype(BF16).reshape(images * TOK, PATCH_IN)
    target = patchify(noise).reshape(images * TOK, PATCH_IN)

    w_in, w_out = fetch(layer_in, layer_out, direct)
    bias_rows = jnp.concatenate([layer_bias[:, MOD : MOD + D], layer_bias[:, MOD + D :]], axis=1)
    g_in, g_out, g_patch, g_head, g_bias, g_bpatch, g_bhead, g_mods, sse = compute(
        patches,
        target,
        position_table(),
        jnp.pad(mods, ((0, 0), (0, 16 - kinds), (0, 0))),
        w_in,
        w_out,
        patch_cols,
        head_cols.T,
        bias_rows,
        top_bias[None, :D],
        top_bias[None, 5 * D : 5 * D + PATCH_IN],
        blocked=direct,
    )

    d_mods = g_mods[:, :kinds].astype(BF16).reshape(images, kinds * D)
    if direct:
        d_mods = exchange(jnp.pad(d_mods.reshape(-1, 128), ((0, 4), (0, 0))), ("fsdp", "rep"), fsdp * rep, 6)
        d_mods = d_mods[:, : images * kinds * D // 128].reshape(every, kinds * D)
    else:
        d_mods = lax.all_gather(d_mods, ("fsdp", "rep"), axis=0, tiled=True)
    g_rows = matmul(cond_own, d_mods, "bd,be->de")
    g_bmods = jnp.sum(d_mods.astype(F32), axis=0)
    d_before = matmul(d_mods, w_mods, "be,de->bd") * silu_slope(own_part(before))
    g_class = jnp.einsum("bd,bc->dc", d_before, picked.astype(F32), precision=lax.Precision.HIGHEST)
    d_time2 = d_before.astype(BF16)
    if direct:
        d_time2 = exchange(jnp.pad(d_time2, ((0, 0), (0, 128 - own))), ("fsdp",), fsdp, 7)
        d_time2 = jnp.transpose(d_time2[:, :, :own], (1, 0, 2)).reshape(every, width)
    else:
        d_time2 = lax.all_gather(d_time2, "fsdp", axis=1, tiled=True)
    g_time2 = matmul(own_part(s1), d_time2, "bd,be->de")
    d_time1 = (matmul(d_time2, time_second, "be,de->bd") * silu_slope(time1)).astype(BF16)
    g_time1 = matmul(own_part(d_time1), features, "bd,bf->df")

    if direct:
        parts = (g_patch, g_head, g_bias, g_bpatch, g_bhead, sse)
        flat = jnp.concatenate([v.reshape(-1) for v in parts])
        flat = jnp.pad(flat, (0, 32 * 1024 - flat.shape[0])).reshape(4, 4, 2, 8, 128)
        out_t, out_m, out_s = reduce_grads(g_in, g_out, flat)

        def joined(v):
            return jnp.transpose(v, (0, 2, 1, 3)).reshape(depth, own, 4 * D)

        shard_in = jnp.concatenate([joined(out_t), joined(out_m[..., :D])], axis=2)
        shard_out = out_m[..., D:].reshape(depth, 4 * own, D)
        flat = jnp.transpose(exchange(out_s, ("fsdp",), fsdp, 8), (1, 0, 2, 3)).reshape(-1)
        sums = []
        at = 0
        for v in parts:
            sums.append(flat[at : at + v.size].reshape(v.shape))
            at += v.size
        g_patch, g_head, g_bias, g_bpatch, g_bhead, sse = sums
    else:
        shard_in = lax.psum(lax.psum_scatter(g_in, "fsdp", scatter_dimension=1, tiled=True), "rep")
        shard_out = lax.psum(lax.psum_scatter(g_out, "fsdp", scatter_dimension=1, tiled=True), "rep")
        g_patch, g_head, g_bias, g_bpatch, g_bhead, sse = lax.psum(
            (g_patch, g_head, g_bias, g_bpatch, g_bhead, sse), ("fsdp", "rep")
        )

    def over_fsdp(values, ident):
        if not direct:
            return lax.psum(values, "fsdp")
        flat = jnp.concatenate([v.reshape(-1) for v in values])
        flat = jnp.pad(flat, (0, -flat.shape[0] % 1024)).reshape(-1, 128)
        flat = jnp.sum(exchange(flat, ("fsdp",), fsdp, ident), axis=0).reshape(-1)
        sums = []
        at = 0
        for v in values:
            sums.append(flat[at : at + v.size].reshape(v.shape))
            at += v.size
        return sums

    tok_total = every * TOK
    scale_grad = 1.0 / (PATCH_IN * math.sqrt(tok_total))
    loss = sse[0, 0] / (tok_total * PATCH_IN)
    fin = depth * MOD
    grad_edge = jnp.concatenate(
        [
            g_class,
            own_part(g_patch).T,
            g_time1,
            g_time2,
            g_rows[:, fin:],
            own_part(g_head).T,
            jnp.zeros((own, PATCH_IN), F32),
        ],
        axis=1,
    )[None] * scale_grad
    grad_in = jnp.concatenate([jnp.stack([g_rows[:, layer * MOD : (layer + 1) * MOD] for layer in range(depth)]), shard_in], axis=2) * scale_grad
    grad_out = shard_out * scale_grad
    grad_lbias = jnp.concatenate([g_bmods[:fin].reshape(depth, MOD), g_bias], axis=1) * scale_grad
    grad_tbias = jnp.concatenate(
        [
            g_bpatch[0],
            jnp.sum(d_time1.astype(F32), axis=0),
            jnp.sum(d_time2.astype(F32), axis=0),
            g_bmods[fin:],
            g_bhead[0],
            jnp.zeros((PATCH_IN,), F32),
        ]
    ) * scale_grad

    full_rows_in = width
    full_rows_out = layer_out.shape[1] * fsdp
    full_rows_edge = edge_mat.shape[0] * fsdp
    square_in = grad_in * grad_in + eps_stat
    square_out = grad_out * grad_out + eps_stat
    square_edge = grad_edge * grad_edge + eps_stat
    rows_in_new = decay * in_rows + (1.0 - decay) * jnp.mean(square_in, axis=2)
    rows_out_new = decay * out_rows + (1.0 - decay) * jnp.mean(square_out, axis=2)
    rows_edge_new = decay * edge_rows[None] + (1.0 - decay) * jnp.mean(square_edge, axis=2)
    col_in, total_in, col_out, total_out, col_edge, total_edge = over_fsdp(
        (
            jnp.sum(square_in, axis=1),
            jnp.sum(rows_in_new, axis=1),
            jnp.sum(square_out, axis=1),
            jnp.sum(rows_out_new, axis=1),
            jnp.sum(square_edge, axis=1),
            jnp.sum(rows_edge_new, axis=1),
        ),
        9,
    )
    cols_in_new = decay * in_cols + (1.0 - decay) * col_in / full_rows_in
    cols_out_new = decay * out_cols + (1.0 - decay) * col_out / full_rows_out
    cols_edge_new = decay * edge_cols[None] + (1.0 - decay) * col_edge / full_rows_edge
    update_in = step_of(grad_in, rows_in_new, cols_in_new, total_in / full_rows_in)
    update_out = step_of(grad_out, rows_out_new, cols_out_new, total_out / full_rows_out)
    update_edge = step_of(grad_edge, rows_edge_new, cols_edge_new, total_edge / full_rows_edge)
    sum_in, sum_out, sum_edge = over_fsdp(
        (
            jnp.sum(update_in * update_in, axis=(1, 2)),
            jnp.sum(update_out * update_out, axis=(1, 2)),
            jnp.sum(update_edge * update_edge, axis=(1, 2)),
        ),
        10,
    )
    roots_in = jnp.sqrt(sum_in / (full_rows_in * grad_in.shape[2]))
    roots_out = jnp.sqrt(sum_out / (full_rows_out * grad_out.shape[2]))
    roots_edge = jnp.sqrt(sum_edge / (full_rows_edge * grad_edge.shape[2]))
    factor_in = jnp.maximum(1.0, roots_in / clip_level)[:, None, None]
    factor_out = jnp.maximum(1.0, roots_out / clip_level)[:, None, None]
    factor_edge = jnp.maximum(1.0, roots_edge / clip_level)[:, None, None]
    in_new = layer_in - rate * update_in / factor_in
    out_new = layer_out - rate * update_out / factor_out
    edge_new = (edge_mat[None] - rate * update_edge / factor_edge)[0]
    clip_roots = jnp.concatenate([roots_in, roots_out, roots_edge])
    lbias_new, lbias_v_new = plain(layer_bias, grad_lbias, layer_bias_v)
    tbias_new, tbias_v_new = plain(top_bias, grad_tbias, top_bias_v)
    return (
        loss,
        in_new,
        out_new,
        edge_new,
        lbias_new,
        tbias_new,
        rows_in_new,
        cols_in_new,
        rows_out_new,
        cols_out_new,
        rows_edge_new[0],
        cols_edge_new[0],
        lbias_v_new,
        tbias_v_new,
        clip_roots,
    )


def solution(mesh):
    placed = (
        P(("fsdp", "rep"), None, None),
        P(("fsdp", "rep")),
        P(("fsdp", "rep")),
        P(("fsdp", "rep"), None, None),
        P(None, "fsdp", None),
        P(None, "fsdp", None),
        P("fsdp", None),
        P(),
        P(),
        P(None, "fsdp"),
        P(),
        P(None, "fsdp"),
        P(),
        P("fsdp"),
        P(),
        P(),
        P(),
    )
    return jax.shard_map(
        shards,
        mesh=mesh,
        in_specs=placed,
        out_specs=(
            P(),
            P(None, "fsdp", None),
            P(None, "fsdp", None),
            P("fsdp", None),
            P(),
            P(),
            P(None, "fsdp"),
            P(),
            P(None, "fsdp"),
            P(),
            P("fsdp"),
            P(),
            P(),
            P(),
            P(),
        ),
        check_vma=False,
    )
```

```python
import functools
import math

import jax
import jax.numpy as jnp
from jax import lax
from jax.experimental import pallas as pl
from jax.experimental.pallas import tpu as pltpu
from jax.sharding import PartitionSpec as P

NCLS = 1001
FREQ = 256
CHANNELS = 4
PATCH = 2
GRID = 32
TSTEPS = 1000
eps_stat = 1e-30
decay = 0.5
rate = 0.01
clip_level = 1.0
D = 384
HEADS = 6
HEAD_DIM = 64
FF = 1536
TOK = 256
PATCH_IN = 16
eps_norm = 1e-06
F32 = jnp.float32
BF16 = jnp.bfloat16
GELU_A = 0.7978845608028654
GELU_B = 0.044715
NT = (((1,), (1,)), ((), ()))
TN = (((0,), (0,)), ((), ()))
FFC = 768
OWN = 48


def dot(a, b, dims=(((1,), (0,)), ((), ()))):
    return lax.dot_general(a, b, dims, preferred_element_type=F32)


def norm_rows(t):
    center = t - jnp.mean(t, axis=-1, keepdims=True)
    spread = jnp.mean(center * center, axis=-1, keepdims=True)
    scale = lax.rsqrt(spread + eps_norm)
    return center * scale, scale


def norm_back(dn, n, scale):
    mean_d = jnp.mean(dn, axis=-1, keepdims=True)
    mean_dn = jnp.mean(dn * n, axis=-1, keepdims=True)
    return scale * (dn - mean_d - n * mean_dn)


def rows_sum(v):
    return jnp.sum(v, axis=0, keepdims=True)


def soft_rows(s):
    e = jnp.exp(s - jnp.max(s, axis=-1, keepdims=True))
    return e / jnp.sum(e, axis=-1, keepdims=True)


def gelu_parts(x):
    t = jnp.tanh(GELU_A * (x + GELU_B * (x * x * x)))
    return t


QKV = 0
WO = 3 * D
WF1 = 4 * D
BQ, BV, BO, BF1, BF2 = 0, D, 2 * D, 3 * D, 3 * D + FF
BW = 4 * D + FF
S_HEAD, S_BIAS, S_BPATCH, S_BHEAD, S_SSE, S_ROWS = 16, 32, 48, 49, 50, 56


def compute_kernel(
    images,
    group,
    blocked,
    patches_ref,
    target_ref,
    pos_ref,
    mods_ref,
    w_in_ref,
    w_out_ref,
    w_patch_ref,
    w_head_ref,
    bias_ref,
    bpatch_ref,
    bhead_ref,
    g_in_ref,
    g_out_ref,
    sums_ref,
    g_mods_ref,
    tok,
    mid,
    qkv,
    att,
    branch,
    outb,
    normed,
    act,
    dinner,
    dsmall,
    dqkv,
    stage,
    mod_sums,
    sems,
):
    steps = images // group
    crow = group * TOK
    lane = lax.broadcasted_iota(jnp.int32, (TOK, 128), 1)
    first_half = lane < HEAD_DIM

    def rows_of(i):
        return pl.ds(pl.multiple_of(i * TOK, TOK), TOK)

    def chunk_of(i):
        return pl.ds(pl.multiple_of(i * crow, crow), crow)

    def mod_row(b, k):
        return mods_ref[k, pl.ds(b, 1), :]

    sums_ref[...] = jnp.zeros_like(sums_ref)
    mod_sums[...] = jnp.zeros_like(mod_sums)

    def add_bias(layer, first, value):
        for at in range(0, value.shape[1], D):
            row = S_BIAS + 8 * layer + (first + at) // D
            sums_ref[row : row + 1, :] += value[:, at : at + D]

    def put_mod(b, k, value):
        mod_sums[k, pl.ds(b, 1), :] = value

    depth = w_in_ref.shape[0]

    @pl.loop(0, images)
    def _(b):
        r = rows_of(b)
        tok[0, r, :] = dot(patches_ref[r, :], w_patch_ref[...], NT) + bpatch_ref[...] + pos_ref[...]

    def half(v, which):
        zero = jnp.zeros_like(v)
        return jnp.where(first_half, v, zero) if which == 0 else jnp.where(first_half, zero, v)

    def attention(layer, r):
        for pair in range(HEADS // 2):
            c = pair * 128
            q = qkv[layer, r, c : c + 128]
            k = qkv[layer, r, D + c : D + c + 128]
            v = qkv[layer, r, 2 * D + c : 2 * D + c + 128]
            got = []
            for which in range(2):
                s = dot(half(q, which), k, NT) * HEAD_DIM ** (-0.5)
                got.append(dot(soft_rows(s).astype(BF16), v))
            att[layer, r, c : c + 128] = jnp.where(first_half, got[0], got[1]).astype(BF16)

    def modulated(t, b, k):
        n, scale = norm_rows(t)
        return n, scale, (n * (1.0 + mod_row(b, k + 1)) + mod_row(b, k)).astype(BF16)

    for layer in range(depth):
        mo = layer * 6

        @pl.loop(0, steps)
        def _(i):
            cr = chunk_of(i)
            for j in range(group):
                b = i * group + j
                r = rows_of(b)
                normed[r, :] = modulated(tok[layer, r, :], b, mo)[2]
            hc = normed[cr, :]
            p = dot(hc, w_in_ref[layer, :, QKV : QKV + 2 * D])
            qkv[layer, cr, 0:D] = (p[:, 0:D] + bias_ref[layer : layer + 1, BQ : BQ + D]).astype(BF16)
            qkv[layer, cr, D : 2 * D] = p[:, D : 2 * D].astype(BF16)
            p = dot(hc, w_in_ref[layer, :, QKV + 2 * D : QKV + 3 * D])
            qkv[layer, cr, 2 * D : 3 * D] = (p + bias_ref[layer : layer + 1, BV : BV + D]).astype(BF16)
            for j in range(group):
                attention(layer, rows_of(i * group + j))
            br = dot(att[layer, cr, :], w_in_ref[layer, :, WO : WO + D]) + bias_ref[layer : layer + 1, BO : BO + D]
            branch[layer, cr, :] = br.astype(BF16)
            for j in range(group):
                b = i * group + j
                r = rows_of(b)
                t2 = tok[layer, r, :] + mod_row(b, mo + 2) * br[j * TOK : (j + 1) * TOK]
                mid[layer, r, :] = t2
                normed[r, :] = modulated(t2, b, mo + 3)[2]
            mc = normed[cr, :]
            out = jnp.zeros((crow, D), F32) + bias_ref[layer : layer + 1, BF2 : BF2 + D]
            for c in range(0, FF, FFC):
                x = dot(mc, w_in_ref[layer, :, WF1 + c : WF1 + c + FFC]) + bias_ref[layer : layer + 1, BF1 + c : BF1 + c + FFC]
                a = (x * (0.5 * (1.0 + gelu_parts(x)))).astype(BF16)
                out = out + dot(a, w_out_ref[layer, c : c + FFC, :])
            outb[layer, cr, :] = out.astype(BF16)
            for j in range(group):
                b = i * group + j
                r = rows_of(b)
                tok[layer + 1, r, :] = mid[layer, r, :] + mod_row(b, mo + 5) * out[j * TOK : (j + 1) * TOK]

    dtok = tok.at[depth]

    @pl.loop(0, images)
    def _(b):
        r = rows_of(b)
        k = 6 * depth
        n, scale, n3 = modulated(dtok[r, :], b, k)
        miss = dot(n3, w_head_ref[...], NT) + bhead_ref[...] - target_ref[r, :]
        sums_ref[S_SSE : S_SSE + 1, 0:PATCH_IN] += rows_sum(miss * miss)
        dp = (2.0 * miss).astype(BF16)
        sums_ref[S_HEAD : S_HEAD + PATCH_IN, :] += dot(dp, n3, TN)
        sums_ref[S_BHEAD : S_BHEAD + 1, 0:PATCH_IN] += rows_sum(dp.astype(F32))
        dn3 = dot(dp, w_head_ref[...])
        put_mod(b, k, rows_sum(dn3))
        put_mod(b, k + 1, rows_sum(dn3 * n))
        dtok[r, :] = norm_back(dn3 * (1.0 + mod_row(b, k + 1)), n, scale)

    pending = {}

    def free(slot):
        for copy in pending.pop(slot, ()):
            copy.wait()

    def send_in(layer, first):
        slot = 0
        moves = []
        for q in range(4):
            source = stage.at[slot, :, q * D : (q + 1) * D]
            if blocked:
                target = (g_in_ref if first == QKV else g_out_ref).at[layer, q, :, 0:D]
            else:
                target = g_in_ref.at[layer, :, first + q * D : first + (q + 1) * D]
            moves.append(pltpu.make_async_copy(source, target, sems.at[slot, q]))
        for move in moves:
            move.start()
        pending[slot] = moves

    def send_down(layer):
        slot = 1
        moves = []
        for c in range(4):
            if not blocked:
                source = stage.at[slot, :, c * D : (c + 1) * D]
                target = g_out_ref.at[layer, c * D : (c + 1) * D, :]
                moves.append(pltpu.make_async_copy(source, target, sems.at[slot, c]))
                continue
            for owner in range(2):
                for q in range(4):
                    start = owner * (D // 2) + q * OWN
                    source = stage.at[slot, start : start + OWN, c * D : (c + 1) * D]
                    begin = (2 * c + owner) * OWN
                    target = g_out_ref.at[layer, q, begin : begin + OWN, D : 2 * D]
                    moves.append(pltpu.make_async_copy(source, target, sems.at[slot, len(moves)]))
        for move in moves:
            move.start()
        pending[slot] = moves

    for layer in reversed(range(depth)):
        mo = layer * 6
        lb = slice(layer, layer + 1)

        @pl.loop(0, steps)
        def _(i):
            cr = chunk_of(i)
            for j in range(group):
                b = i * group + j
                r = rows_of(b)
                normed[r, :] = modulated(mid[layer, r, :], b, mo + 3)[2]
                d = dtok[r, :]
                put_mod(b, mo + 5, rows_sum(d * outb[layer, r, :].astype(F32)))
                do = (d * mod_row(b, mo + 5)).astype(BF16)
                dsmall[r, :] = do
                add_bias(layer, BF2, rows_sum(do.astype(F32)))
            mc = normed[cr, :]
            do = dsmall[cr, :]
            dm = jnp.zeros((crow, D), F32)
            for c in range(0, FF, FFC):
                x = dot(mc, w_in_ref[layer, :, WF1 + c : WF1 + c + FFC]) + bias_ref[lb, BF1 + c : BF1 + c + FFC]
                x2 = x * x
                t = jnp.tanh(GELU_A * (x + GELU_B * (x2 * x)))
                cdf = 0.5 * (1.0 + t)
                act[cr, c : c + FFC] = (x * cdf).astype(BF16)
                slope = cdf + (0.5 * GELU_A) * x * (1.0 - t * t) * (1.0 + (3.0 * GELU_B) * x2)
                di = (dot(do, w_out_ref[layer, c : c + FFC, :], NT) * slope).astype(BF16)
                dinner[cr, c : c + FFC] = di
                add_bias(layer, BF1 + c, rows_sum(di.astype(F32)))
                dm = dm + dot(di, w_in_ref[layer, :, WF1 + c : WF1 + c + FFC], NT)
            for j in range(group):
                b = i * group + j
                r = rows_of(b)
                n, scale = norm_rows(mid[layer, r, :])
                dmj = dm[j * TOK : (j + 1) * TOK]
                put_mod(b, mo + 3, rows_sum(dmj))
                put_mod(b, mo + 4, rows_sum(dmj * n))
                dtok[r, :] = dtok[r, :] + norm_back(dmj * (1.0 + mod_row(b, mo + 4)), n, scale)

        free(0)

        @pl.loop(0, FF // D)
        def _(c):
            cs = pl.ds(pl.multiple_of(c * D, D), D)
            stage[0, :, cs] = dot(normed[...], dinner[:, cs], TN)

        send_in(layer, WF1)
        free(1)

        @pl.loop(0, FF // D)
        def _(c):
            cs = pl.ds(pl.multiple_of(c * D, D), D)
            stage[1, :, cs] = dot(dsmall[...], act[:, cs], TN).T

        send_down(layer)

        @pl.loop(0, steps)
        def _(i):
            cr = chunk_of(i)
            for j in range(group):
                b = i * group + j
                r = rows_of(b)
                d = dtok[r, :]
                put_mod(b, mo + 2, rows_sum(d * branch[layer, r, :].astype(F32)))
                db = (d * mod_row(b, mo + 2)).astype(BF16)
                dsmall[r, :] = db
                add_bias(layer, BO, rows_sum(db.astype(F32)))
            branch[layer, cr, :] = dot(dsmall[cr, :], w_in_ref[layer, :, WO : WO + D], NT).astype(BF16)
            for j in range(group):
                r = rows_of(i * group + j)
                for pair in range(HEADS // 2):
                    c = pair * 128
                    q = qkv[layer, r, c : c + 128]
                    k = qkv[layer, r, D + c : D + c + 128]
                    v = qkv[layer, r, 2 * D + c : 2 * D + c + 128]
                    da = branch[layer, r, c : c + 128]
                    got = []
                    for which in range(2):
                        s = dot(half(q, which), k, NT) * HEAD_DIM ** (-0.5)
                        p = soft_rows(s)
                        dv = dot(p.astype(BF16), da, TN)
                        dpr = dot(half(da, which), v, NT)
                        ds = p * (dpr - jnp.sum(dpr * p, axis=-1, keepdims=True))
                        ds = ds.astype(BF16)
                        dq = dot(ds, k)
                        dk = dot(ds, q, TN)
                        got.append((dq, dk, dv))
                    dq = (jnp.where(first_half, got[0][0], got[1][0]) * HEAD_DIM ** (-0.5)).astype(BF16)
                    dk = (jnp.where(first_half, got[0][1], got[1][1]) * HEAD_DIM ** (-0.5)).astype(BF16)
                    dv = jnp.where(first_half, got[0][2], got[1][2]).astype(BF16)
                    dqkv[r, c : c + 128] = dq
                    dqkv[r, D + c : D + c + 128] = dk
                    dqkv[r, 2 * D + c : 2 * D + c + 128] = dv
                    row = S_BIAS + 8 * layer
                    sums_ref[row : row + 1, c : c + 128] += rows_sum(dq.astype(F32))
                    sums_ref[row + 1 : row + 2, c : c + 128] += rows_sum(dv.astype(F32))
            dh = dot(dqkv[cr, :], w_in_ref[layer, :, QKV : QKV + 3 * D], NT)
            for j in range(group):
                b = i * group + j
                r = rows_of(b)
                n, scale, h = modulated(tok[layer, r, :], b, mo)
                normed[r, :] = h
                dhj = dh[j * TOK : (j + 1) * TOK]
                put_mod(b, mo, rows_sum(dhj))
                put_mod(b, mo + 1, rows_sum(dhj * n))
                dtok[r, :] = dtok[r, :] + norm_back(dhj * (1.0 + mod_row(b, mo + 1)), n, scale)

        free(0)

        @pl.loop(0, 3)
        def _(c):
            cs = pl.ds(pl.multiple_of(c * D, D), D)
            stage[0, :, cs] = dot(normed[...], dqkv[:, cs], TN)

        stage[0, :, 3 * D : 4 * D] = dot(att[layer], dsmall[...], TN)
        send_in(layer, QKV)
        free(1)

    @pl.loop(0, images)
    def _(b):
        r = rows_of(b)
        d = dtok[r, :].astype(BF16)
        sums_ref[S_BPATCH : S_BPATCH + 1, :] += rows_sum(d.astype(F32))
        sums_ref[0:PATCH_IN, :] += dot(patches_ref[r, :], d, TN)

    g_mods_ref[...] = mod_sums[...].astype(BF16)
    free(0)


def compute(patches, target, pos, mods, w_in, w_out, w_patch, w_head_t, bias, bpatch, bhead, group=3, blocked=False):
    depth = w_in.shape[0]
    rows = patches.shape[0]
    images = rows // TOK
    kinds = mods.shape[0]
    vm = pl.BlockSpec(memory_space=pltpu.VMEM)
    anyspace = pl.BlockSpec(memory_space=pl.ANY)
    shape = jax.ShapeDtypeStruct
    return pl.pallas_call(
        functools.partial(compute_kernel, images, group, blocked),
        out_shape=(
            shape((depth, 4, D, D) if blocked else (depth, D, 4 * D + FF), F32),
            shape((depth, 4, D, 2 * D) if blocked else (depth, FF, D), F32),
            shape((S_ROWS, D), F32),
            shape((kinds, 8, D), BF16),
        ),
        in_specs=[vm] * 11,
        out_specs=(anyspace, anyspace, vm, vm),
        scratch_shapes=[
            pltpu.VMEM((depth + 1, rows, D), F32),
            pltpu.VMEM((depth, rows, D), F32),
            pltpu.VMEM((depth, rows, 3 * D), BF16),
            pltpu.VMEM((depth, rows, D), BF16),
            pltpu.VMEM((depth, rows, D), BF16),
            pltpu.VMEM((depth, rows, D), BF16),
            pltpu.VMEM((rows, D), BF16),
            pltpu.VMEM((rows, FF), BF16),
            pltpu.VMEM((rows, FF), BF16),
            pltpu.VMEM((rows, D), BF16),
            pltpu.VMEM((rows, 3 * D), BF16),
            pltpu.VMEM((2, D, FF), F32),
            pltpu.VMEM((mods.shape[0], 8, D), F32),
            pltpu.SemaphoreType.DMA((2, 32)),
        ],
        compiler_params=pltpu.CompilerParams(vmem_limit_bytes=60 * 1024 * 1024),
        name="step_compute",
    )(patches, target, pos, mods, w_in, w_out, w_patch, w_head_t, bias, bpatch, bhead)


def place():
    f = lax.axis_index("fsdp")
    r = lax.axis_index("rep")
    z = f // 2
    y = f - 2 * z
    x = r // 2
    c = r - 2 * x
    return z, y, x, c


def device(z, y, x, c):
    return {"fsdp": 2 * z + y, "rep": 2 * x + c}


def greet(peers):
    barrier = pltpu.get_barrier_semaphore()
    for peer in peers:
        pl.semaphore_signal(barrier, inc=1, device_id=peer, device_id_type=pl.DeviceIdType.MESH)
    pl.semaphore_wait(barrier, len(peers))


def remote(source, target, send, recv, peer):
    return pltpu.make_async_remote_copy(
        src_ref=source, dst_ref=target, send_sem=send, recv_sem=recv, device_id=peer, device_id_type=pl.DeviceIdType.MESH
    )


class Reducer:
    def __init__(self, source, bufs, out, sends, recvs, loads):
        self.source = source
        self.keep, self.got0, self.sx, self.gotx, self.sy, self.goty, self.sz, self.gotz, self.sw, self.gotw = bufs
        self.out = out
        self.sends, self.recvs, self.loads = sends, recvs, loads
        self.link = self.sx.dtype
        self.z, self.y, self.x, self.c = place()
        z, y, x, c = self.z, self.y, self.x, self.c
        self.to_c = device(z, y, x, 1 - c)
        self.to_x = device(z, y, 1 - x, c)
        self.to_y = device(z, 1 - y, x, c)
        self.z1 = z + 1 - 2 * lax.rem(z, 2)
        self.z2 = lax.rem(z + 2, 4)
        self.to_z1 = device(self.z1, y, x, c)
        self.to_z2 = device(self.z2, y, x, c)
        self.moves = {}

    def send(self, slot, source, target, peer):
        copy = remote(source, target, self.sends.at[slot], self.recvs.at[slot], peer)
        copy.start()
        self.moves[slot] = copy

    def step(self, k):
        z, y, x, c = self.z, self.y, self.x, self.c
        if k == 0:
            for half in range(2):
                load = pltpu.make_async_copy(self.source.at[2 * half + c], self.keep.at[half], self.loads.at[half])
                load.start()
                self.moves["load", half] = load
                self.send(half, self.source.at[2 * half + 1 - c], self.got0.at[half], self.to_c)
        if k == 1:
            for half in range(2):
                self.moves["load", half].wait()
                self.moves[half].wait()

            @pl.loop(0, 4)
            def _(i):
                for j in range(2):
                    self.sx[i, j] = (self.keep[1 - x, i, j] + self.got0[1 - x, i, j]).astype(self.link)

            self.send(2, self.sx, self.gotx, self.to_x)

            @pl.loop(0, 4)
            def _(i):
                for j in range(2):
                    self.keep[x, i, j] = self.keep[x, i, j] + self.got0[x, i, j]
        if k == 2:
            self.moves[2].wait()

            @pl.loop(0, 4)
            def _(i):
                self.sy[i] = (self.keep[x, i, 1 - y] + self.gotx[i, 1 - y].astype(F32)).astype(self.link)

            self.send(3, self.sy, self.goty, self.to_y)

            @pl.loop(0, 4)
            def _(i):
                self.keep[x, i, y] = self.keep[x, i, y] + self.gotx[i, y].astype(F32)
        if k == 3:
            self.moves[3].wait()
            for s in range(2):
                at = lax.rem(self.z1 + 2 * s, 4)
                self.sz[s] = (self.keep[x, at, y] + self.goty[at].astype(F32)).astype(self.link)
            self.send(4, self.sz, self.gotz, self.to_z1)
            for s in range(2):
                at = lax.rem(z + 2 * s, 4)
                self.keep[x, at, y] = self.keep[x, at, y] + self.goty[at].astype(F32)
        if k == 4:
            self.moves[4].wait()
            self.sw[...] = (self.keep[x, self.z2, y] + self.gotz[1].astype(F32)).astype(self.link)
            self.send(5, self.sw, self.gotw, self.to_z2)
        if k == 5:
            self.moves[5].wait()
            mine = 2 * x + c
            self.out[mine] = self.keep[x, z, y] + self.gotz[0].astype(F32) + self.gotw[...].astype(F32)
            self.send(6, self.out.at[mine], self.out.at[mine], self.to_x)
            self.send(7, self.out.at[mine], self.out.at[mine], self.to_c)
        if k == 6:
            self.moves[6].wait()
            other = 2 * (1 - x) + c
            self.send(8, self.out.at[other], self.out.at[other], self.to_c)
        if k == 7:
            self.moves[7].wait()
            self.moves[8].wait()

    def peers(self):
        return [self.to_c, self.to_x, self.to_y, self.to_z1, self.to_z2]


REDUCER_STEPS = 8


def reducer_scratch(width, own=OWN, link=BF16):
    return [
        pltpu.VMEM((2, 4, 2, own, width), F32),
        pltpu.VMEM((2, 4, 2, own, width), F32),
        pltpu.VMEM((4, 2, own, width), link),
        pltpu.VMEM((4, 2, own, width), link),
        pltpu.VMEM((4, own, width), link),
        pltpu.VMEM((4, own, width), link),
        pltpu.VMEM((2, own, width), link),
        pltpu.VMEM((2, own, width), link),
        pltpu.VMEM((own, width), link),
        pltpu.VMEM((own, width), link),
    ]


class Gatherer:
    def __init__(self, source, target, whole, sends, recvs, local):
        self.source, self.target, self.whole = source, target, whole
        self.sends, self.recvs, self.local = sends, recvs, local
        self.z, self.y, self.x, self.c = place()
        self.q = 2 * self.x + self.c
        self.moves = {}

    def send(self, slot, source, target, peer):
        copy = remote(source, target, self.sends.at[slot], self.recvs.at[slot], peer)
        copy.start()
        self.moves[slot] = copy

    def step(self, k):
        z, y, x, c, q = self.z, self.y, self.x, self.c, self.q
        f = 2 * z + y
        if k == 0:
            for d in range(1, 4):
                peer = lax.rem(z + d, 4)
                self.send(d - 1, self.source(q), self.target(f, q), device(peer, y, x, c))
            self.send(3, self.source(q), self.target(f, q), device(z, 1 - y, x, c))
            own = pltpu.make_async_copy(self.source(q), self.target(f, q), self.local)
            own.start()
            self.moves["own"] = own
        if k == 1:
            for d in range(1, 4):
                self.moves[d - 1].wait()
                at = 2 * lax.rem(z + 4 - d, 4) + y
                self.send(3 + d, self.target(at, q), self.target(at, q), device(z, 1 - y, x, c))
        if k == 2:
            self.moves["own"].wait()
            for slot in range(3, 7):
                self.moves[slot].wait()
            self.send(7, self.whole(q), self.whole(q), device(z, y, 1 - x, c))
            self.send(8, self.whole(q), self.whole(q), device(z, y, x, 1 - c))
        if k == 3:
            self.moves[7].wait()
            other = 2 * (1 - x) + c
            self.send(9, self.whole(other), self.whole(other), device(z, y, x, 1 - c))
        if k == 4:
            self.moves[8].wait()
            self.moves[9].wait()

    def peers(self):
        z, y, x, c = self.z, self.y, self.x, self.c
        return [device(lax.rem(z + d, 4), y, x, c) for d in range(1, 4)] + [
            device(z, 1 - y, x, c),
            device(z, y, 1 - x, c),
            device(z, y, x, 1 - c),
        ]


GATHER_STEPS = 5


def by_columns(source, target, sends, recvs, local):
    rows, width = source.shape
    part = width // 4

    def cols(q):
        return pl.ds(pl.multiple_of(q * part, 128), part)

    def rows_of(f):
        return pl.ds(pl.multiple_of(f * rows, 16), rows)

    return Gatherer(
        lambda q: source.at[:, cols(q)],
        lambda f, q: target.at[rows_of(f), cols(q)],
        lambda q: target.at[:, cols(q)],
        sends,
        recvs,
        local,
    )


def by_rows(source, target, sends, recvs, local):
    return Gatherer(
        lambda q: source.at[q],
        lambda f, q: target.at[f, q],
        lambda q: target.at[:, q],
        sends,
        recvs,
        local,
    )


def slab(source, target, sends, recvs, local):
    return Gatherer(lambda q: source, lambda f, q: target.at[q, f], lambda q: target.at[q], sends, recvs, local)


class Butterfly:
    def __init__(self, total, got, sends, recvs, like):
        self.total, self.got, self.sends, self.recvs = total, got, sends, recvs
        self.order = [like.to_c, like.to_x, like.to_y, like.to_z1, like.to_z2]
        self.move = None

    def step(self, k):
        if k > 0:
            self.move.wait()
            self.total[...] = self.total[...] + self.got[k - 1]
        if k < 5:
            self.move = remote(self.total, self.got.at[k], self.sends.at[k], self.recvs.at[k], self.order[k])
            self.move.start()


BUTTERFLY_STEPS = 6


def run_steps(plans):
    last = max(first + count for first, count, _ in plans)
    for tick in range(last):
        for first, count, piece in plans:
            if 0 <= tick - first < count:
                piece.step(tick - first)


def reduce_kernel(depth, t_ref, m_ref, s_ref, d_ref, out_t_ref, out_m_ref, out_s_ref, out_d_ref, *scratch):
    scratch = list(scratch)
    sends, recvs, loads, g_sends, g_recvs, g_local, b_sends, b_recvs, got = scratch[-9:]
    plans = []

    def piece(source, out):
        n = len(plans)
        one = Reducer(source, scratch[10 * n : 10 * n + 10], out, sends.at[n], recvs.at[n], loads.at[n])
        plans.append((n, REDUCER_STEPS, one))

    for layer in reversed(range(depth)):
        piece(m_ref.at[layer], out_m_ref.at[layer])
        piece(t_ref.at[layer], out_t_ref.at[layer])
    first = plans[0][2]
    mods = slab(d_ref, out_d_ref, g_sends, g_recvs, g_local)
    out_s_ref[...] = s_ref[...]
    sums = Butterfly(out_s_ref, got, b_sends, b_recvs, first)
    z, y, x, c = place()
    z3 = 3 - z
    greet(first.peers() + [device(z3, y, x, c)])
    run_steps([(0, GATHER_STEPS, mods), (0, BUTTERFLY_STEPS, sums)] + plans)


def reduce_grads(g_t, g_m, sums, mods):
    depth = g_t.shape[0]
    shape = jax.ShapeDtypeStruct
    scratch = []
    for _ in range(depth):
        scratch += reducer_scratch(2 * D) + reducer_scratch(D)
    count = 2 * depth
    dma = pltpu.SemaphoreType.DMA
    scratch += [dma((count, 9)), dma((count, 9)), dma((count, 2)), dma((10,)), dma((10,)), dma, dma((5,)), dma((5,))]
    scratch += [pltpu.VMEM((5,) + sums.shape, F32)]
    anyspace = pl.BlockSpec(memory_space=pl.ANY)
    vm = pl.BlockSpec(memory_space=pltpu.VMEM)
    return pl.pallas_call(
        functools.partial(reduce_kernel, depth),
        out_shape=(
            shape((depth, 4, OWN, D), F32),
            shape((depth, 4, OWN, 2 * D), F32),
            shape(sums.shape, F32),
            shape((4, 8) + mods.shape, mods.dtype),
        ),
        in_specs=[anyspace, anyspace, vm, vm],
        out_specs=(vm, vm, vm, vm),
        scratch_shapes=scratch,
        compiler_params=pltpu.CompilerParams(collective_id=1, has_side_effects=True, vmem_limit_bytes=60 * 1024 * 1024),
        name="step_reduce",
    )(g_t.reshape(depth, 4, 4, 2, OWN, D), g_m.reshape(depth, 4, 4, 2, OWN, 2 * D), sums, mods)


C_T1, C_T2, C_PATCH, C_HEAD, C_ALL = 1024, 1280, 1664, 1680, 2048
SLOTS = 256


def silu_slope(x):
    gate = 1.0 / (1.0 + jnp.exp(-x))
    return gate * (1.0 + x * (1.0 - gate))


def silu(x):
    return x / (1.0 + jnp.exp(-x))


def prologue_kernel(
    depth,
    kinds,
    small_ref,
    feat_ref,
    w_mods_ref,
    top_ref,
    bias_ref,
    own_in_ref,
    own_out_ref,
    full_ref,
    w_in_ref,
    w_out_ref,
    mods_ref,
    time1_ref,
    s1_ref,
    before_ref,
    cond_ref,
    feats_ref,
    part,
    got,
    cond_rows,
    wide,
    sends,
    recvs,
    local,
    p_sends,
    p_recvs,
    p_local,
):
    z, y, x, c = place()
    f = 2 * z + y
    r = 2 * x + c
    feats = slab(feat_ref, feats_ref, sends.at[0], recvs.at[0], local.at[0])
    small = by_columns(small_ref, full_ref, sends.at[1], recvs.at[1], local.at[1])
    plans = [(0, GATHER_STEPS, feats), (0, GATHER_STEPS, small)]
    for layer in range(depth):
        n = 2 + 2 * layer
        plans.append(
            (1 + 2 * layer, GATHER_STEPS, by_columns(own_in_ref.at[layer], w_in_ref.at[layer], sends.at[n], recvs.at[n], local.at[n]))
        )
        plans.append(
            (
                2 + 2 * layer,
                GATHER_STEPS,
                by_rows(own_out_ref.at[layer], w_out_ref.at[layer], sends.at[n + 1], recvs.at[n + 1], local.at[n + 1]),
            )
        )
    others = [{"fsdp": lax.rem(f + k, 8)} for k in range(1, 8)]
    greet(others + [device(z, y, 1 - x, c), device(z, y, x, 1 - c)])
    last = max(first + count for first, count, _ in plans)
    copies = []
    for tick in range(last):
        for first, count, piece in plans:
            if 0 <= tick - first < count:
                piece.step(tick - first)
        if tick != GATHER_STEPS - 1:
            continue
        rows = feats_ref[...].reshape(SLOTS, feats_ref.shape[-1])
        feat = rows[:, :FREQ].astype(BF16)
        label = rows[:, FREQ : FREQ + 1]
        place_of = lax.broadcasted_iota(jnp.int32, (SLOTS, C_T1), 1).astype(F32)
        picked = jnp.where(label == place_of, 1.0, 0.0).astype(BF16)
        time1 = dot(feat, full_ref[:, C_T1:C_T2], NT) + top_ref[0:1, :]
        s1 = silu(time1).astype(BF16)
        before = dot(s1, full_ref[:, C_T2 : C_T2 + D]) + top_ref[1:2, :] + dot(picked, full_ref[:, :C_T1], NT)
        cond = silu(before)
        cond_rows[...] = cond
        mine = pl.ds(pl.multiple_of(f * OWN, OWN), OWN)
        time1_ref[...] = time1.T
        wide[...] = s1.astype(F32).T
        s1_ref[...] = wide[mine, :].astype(BF16)
        wide[...] = before.T
        before_ref[...] = wide[mine, :]
        wide[...] = cond.T
        cond_ref[...] = wide[mine, :].astype(BF16)
        pick = lax.broadcasted_iota(jnp.int32, (D, OWN), 0) == f * OWN + lax.broadcasted_iota(jnp.int32, (D, OWN), 1)
        group = cond_rows[pl.ds(pl.multiple_of(r * 64, 64), 64), :].astype(BF16)
        group = dot(group, jnp.where(pick, 1.0, 0.0).astype(BF16)).astype(BF16)
        for k in range(kinds):
            part[:, k] = dot(group, w_mods_ref[:, k * D : (k + 1) * D]).reshape(8, 8, D)
        for k in range(1, 8):
            copies.append(remote(part.at[lax.rem(f + k, 8)], got.at[f], p_sends.at[k - 1], p_recvs.at[k - 1], others[k - 1]))
            copies[-1].start()
        own = pltpu.make_async_copy(part.at[f], got.at[f], p_local)
        own.start()
    own.wait()
    for copy in copies:
        copy.wait()
    total = got[0]
    for k in range(1, 8):
        total = total + got[k]
    for k in range(kinds):
        mods_ref[k] = total[k] + bias_ref[:, k * D : (k + 1) * D]
    mods_ref[kinds:] = jnp.zeros_like(mods_ref[kinds:])


def prologue(small, feat, w_mods, top, bias, own_in, own_out):
    depth = own_in.shape[0]
    kinds = w_mods.shape[1] // D
    shape = jax.ShapeDtypeStruct
    anyspace = pl.BlockSpec(memory_space=pl.ANY)
    vm = pl.BlockSpec(memory_space=pltpu.VMEM)
    dma = pltpu.SemaphoreType.DMA
    n = 2 + 2 * depth
    return pl.pallas_call(
        functools.partial(prologue_kernel, depth, kinds),
        out_shape=(
            shape((D, C_ALL), BF16),
            shape((depth, D, own_in.shape[2]), BF16),
            shape((depth, 8, 4, OWN, D), BF16),
            shape((16, 8, D), F32),
            shape((D, SLOTS), F32),
            shape((OWN, SLOTS), BF16),
            shape((OWN, SLOTS), F32),
            shape((OWN, SLOTS), BF16),
            shape((4, 8) + feat.shape, F32),
        ),
        in_specs=[anyspace, vm, vm, vm, vm, anyspace, anyspace],
        out_specs=(vm,) * 9,
        scratch_shapes=[
            pltpu.VMEM((8, kinds, 8, D), F32),
            pltpu.VMEM((8, kinds, 8, D), F32),
            pltpu.VMEM((SLOTS, D), F32),
            pltpu.VMEM((D, SLOTS), F32),
            dma((n, 10)),
            dma((n, 10)),
            dma((n,)),
            dma((7,)),
            dma((7,)),
            dma,
        ],
        compiler_params=pltpu.CompilerParams(collective_id=2, has_side_effects=True, vmem_limit_bytes=60 * 1024 * 1024),
        name="step_prologue",
    )(small, feat, w_mods, top, bias, own_in, own_out)


E_PATCH, E_T1, E_T2, E_FIN, E_HEAD, E_ALL = 1024, 1152, 1408, 1792, 2560, 2688
STAT = 1792


def column_of(row):
    n = row.shape[1]
    same = lax.broadcasted_iota(jnp.int32, (n, n), 0) == lax.broadcasted_iota(jnp.int32, (n, n), 1)
    return jnp.sum(jnp.where(same, row, 0.0), axis=1, keepdims=True)


def row_of(column):
    n = column.shape[0]
    same = lax.broadcasted_iota(jnp.int32, (n, n), 0) == lax.broadcasted_iota(jnp.int32, (n, n), 1)
    return jnp.sum(jnp.where(same, column, 0.0), axis=0, keepdims=True)


def total_of(v):
    return jnp.sum(rows_sum(v), axis=1, keepdims=True)


def update_kernel(
    sizes,
    out_t_ref,
    out_m_ref,
    sums_ref,
    d_mods_ref,
    cond_ref,
    before_ref,
    time1_ref,
    s1_ref,
    feats_ref,
    time2_ref,
    w_mods_ref,
    in_ref,
    down_ref,
    edge_ref,
    lbias_ref,
    tbias_ref,
    in_rows_ref,
    in_cols_ref,
    down_rows_ref,
    down_cols_ref,
    edge_rows_ref,
    edge_cols_ref,
    lbias_v_ref,
    tbias_v_ref,
    in_new,
    down_new,
    edge_new,
    lbias_new,
    tbias_new,
    in_rows_new,
    in_cols_new,
    down_rows_new,
    down_cols_new,
    edge_rows_new,
    edge_cols_new,
    lbias_v_new,
    tbias_v_new,
    tail_ref,
    g_in,
    g_down,
    g_edge,
    d_time2,
    d_time1,
    small_t,
    stats,
    squares,
    sends,
    recvs,
):
    classes, tokens = sizes
    depth = in_ref.shape[0]
    kinds = w_mods_ref.shape[1] // D
    fin = 6 * depth
    f = lax.axis_index("fsdp")
    others = [{"fsdp": lax.rem(f + k, 8)} for k in range(1, 8)]
    scale = 1.0 / (PATCH_IN * math.sqrt(tokens))
    mine = pl.ds(pl.multiple_of(f * OWN, OWN), OWN)
    greet(others)

    def share(n, buffer):
        copies = []
        for k in range(1, 8):
            copies.append(remote(buffer.at[f], buffer.at[f], sends.at[n, k - 1], recvs.at[n, k - 1], others[k - 1]))
            copies[-1].start()
        return copies

    d_cond = jnp.zeros((OWN, SLOTS), F32)
    ones = jnp.ones((8, SLOTS), BF16)
    for k in range(kinds):
        rows = d_mods_ref[:, :, k].astype(F32).reshape(SLOTS, D).astype(BF16)
        g = dot(cond_ref[...], rows) * scale
        b = dot(ones, rows)[0:1] * scale
        if k < fin:
            layer, at = k // 6, (k % 6) * D
            g_in[layer, :, at : at + D] = g
            lbias_new[layer : layer + 1, at : at + D] = b
        else:
            at = (k - fin) * D
            g_edge[:, E_FIN + at : E_FIN + at + D] = g
            tbias_new[:, 3 * D + at : 3 * D + at + D] = b
        d_cond = d_cond + dot(w_mods_ref[:, k * D : (k + 1) * D], rows, NT)
    d_before = d_cond * silu_slope(before_ref[...])
    d_time2[f] = d_before.astype(BF16)
    copies = share(0, d_time2)
    rows = feats_ref[...].reshape(SLOTS, feats_ref.shape[-1])
    feat = rows[:, :FREQ].astype(BF16)
    label = rows[:, FREQ : FREQ + 1]
    picked = jnp.where(label == lax.broadcasted_iota(jnp.int32, (SLOTS, E_PATCH), 1).astype(F32), 1.0, 0.0).astype(BF16)
    top = d_before.astype(BF16)
    left = d_before - top.astype(F32)
    middle = left.astype(BF16)
    low = (left - middle.astype(F32)).astype(BF16)
    g_edge[:, 0:E_PATCH] = (dot(top, picked) + dot(middle, picked) + dot(low, picked)) * scale
    small_t[:, 0 : 2 * PATCH_IN] = sums_ref[0 : 2 * PATCH_IN, :].T * scale
    own_small = small_t[mine, :]
    lane = lax.broadcasted_iota(jnp.int32, (OWN, 128), 1)
    g_edge[:, E_PATCH:E_T1] = jnp.where(lane < PATCH_IN, own_small, 0.0)
    g_edge[:, E_HEAD:E_ALL] = jnp.where(lane < PATCH_IN, pltpu.roll(own_small, 128 - PATCH_IN, 1), 0.0)
    for layer in range(depth):
        for q in range(4):
            g_in[layer, :, 6 * D + q * D : 7 * D + q * D] = out_t_ref[layer, q] * scale
            g_in[layer, :, 10 * D + q * D : 11 * D + q * D] = out_m_ref[layer, q, :, 0:D] * scale
            g_down[layer, q * OWN : (q + 1) * OWN, :] = out_m_ref[layer, q, :, D : 2 * D] * scale
    for copy in copies:
        copy.wait()
    d2 = d_time2[...].reshape(D, SLOTS)
    g_edge[:, E_T2:E_FIN] = dot(s1_ref[...], d2, NT) * scale
    d1 = (dot(time2_ref[...], d2) * silu_slope(time1_ref[...])).astype(BF16)
    d_time1[...] = d1
    g_edge[:, E_T1:E_T2] = dot(d_time1[mine, :], feat) * scale
    tbias_new[:, D : 2 * D] = dot(ones, d1, NT)[0:1] * scale
    tbias_new[:, 2 * D : 3 * D] = dot(ones, d2, NT)[0:1] * scale
    tbias_new[:, 0:D] = sums_ref[S_BPATCH : S_BPATCH + 1, :] * scale
    tail = tbias_new.shape[1]
    tbias_new[:, 5 * D : tail] = jnp.zeros((1, tail - 5 * D), F32)
    tbias_new[:, 5 * D : 5 * D + PATCH_IN] = sums_ref[S_BHEAD : S_BHEAD + 1, 0:PATCH_IN] * scale
    for layer in range(depth):
        for j in range(8):
            row = S_BIAS + 8 * layer + j
            lbias_new[layer : layer + 1, 6 * D + j * D : 7 * D + j * D] = sums_ref[row : row + 1, :] * scale

    wide = in_ref.shape[2]
    rows_in, rows_down = [], []
    for layer in range(depth):
        s = jnp.zeros((OWN, 1), F32)
        for t in range(wide // STAT):
            g = g_in[layer, :, t * STAT : (t + 1) * STAT]
            g2 = g * g
            s = s + jnp.sum(g2, axis=1, keepdims=True)
            stats[f, wide // STAT * layer + t : wide // STAT * layer + t + 1, :] = rows_sum(g2)
        new = decay * column_of(in_rows_ref[layer : layer + 1, :]) + (1.0 - decay) * (s / wide + eps_stat)
        rows_in.append(new)
        in_rows_new[layer : layer + 1, :] = row_of(new)
        g = g_down[layer]
        g2 = g * g
        new = decay * column_of(down_rows_ref[layer : layer + 1, :]) + (1.0 - decay) * (
            jnp.sum(g2, axis=1, keepdims=True) / D + eps_stat
        )
        rows_down.append(new)
        down_rows_new[layer : layer + 1, :] = row_of(new)
        stats[f, 7:8, E_ALL - STAT + layer * D : E_ALL - STAT + (layer + 1) * D] = rows_sum(g2)
    g = g_edge[...]
    g2 = g * g
    rows_edge = decay * column_of(edge_rows_ref[...]) + (1.0 - decay) * (
        jnp.sum(g2, axis=1, keepdims=True) / classes + eps_stat
    )
    edge_rows_new[...] = row_of(rows_edge)
    g2 = rows_sum(g2)
    stats[f, 6:7, :] = g2[:, 0:STAT]
    stats[f, 7:8, 0 : E_ALL - STAT] = g2[:, STAT:E_ALL]
    lane = lax.broadcasted_iota(jnp.int32, (1, 128), 1)
    totals = jnp.zeros((1, 128), F32)
    every = rows_in + rows_down + [rows_edge]
    for n, v in enumerate(every):
        totals = jnp.where(lane == n, rows_sum(v), totals)
    spot = E_ALL - STAT + depth * D
    stats[f, 7:8, spot : spot + 128] = totals
    copies = share(1, stats)

    def plain_rows(weight, new, old_v, new_v, columns):
        g = new[...]
        moment = decay * old_v[...] + (1.0 - decay) * (g * g + eps_stat)
        u = g * lax.rsqrt(moment)
        root = jnp.sqrt(jnp.sum(u * u, axis=1, keepdims=True) / columns)
        new_v[...] = moment
        new[...] = weight[...] - rate * u / jnp.maximum(1.0, root / clip_level)

    plain_rows(lbias_ref, lbias_new, lbias_v_ref, lbias_v_new, wide)
    plain_rows(tbias_ref, tbias_new, tbias_v_ref, tbias_v_new, 5 * D + 2 * PATCH_IN)
    loss = jnp.sum(sums_ref[S_SSE : S_SSE + 1, 0:PATCH_IN], axis=1, keepdims=True) / (tokens * PATCH_IN)

    for copy in copies:
        copy.wait()
    full = stats[0]
    for k in range(1, 8):
        full = full + stats[k]
    height = 8.0 * OWN
    tall = 4.0 * height

    def factors(rows_col, total, count, cols):
        return lax.rsqrt(rows_col / (total / count)), lax.rsqrt(cols)

    squared = jnp.zeros((1, 128), F32)
    used = []
    for layer in range(depth):
        total = full[7:8, spot + layer : spot + layer + 1]
        s = jnp.zeros((1, 1), F32)
        for t in range(wide // STAT):
            at = slice(t * STAT, (t + 1) * STAT)
            line = wide // STAT * layer + t
            cols = decay * in_cols_ref[layer : layer + 1, at] + (1.0 - decay) * (full[line : line + 1, :] / height + eps_stat)
            in_cols_new[layer : layer + 1, at] = cols
            a, b = factors(rows_in[layer], total, height, cols)
            u = g_in[layer, :, at] * a * b
            g_in[layer, :, at] = u
            s = s + total_of(u * u)
        squared = jnp.where(lane == layer, s, squared)
        at = E_ALL - STAT + layer * D
        cols = decay * down_cols_ref[layer : layer + 1, :] + (1.0 - decay) * (full[7:8, at : at + D] / tall + eps_stat)
        down_cols_new[layer : layer + 1, :] = cols
        total = full[7:8, spot + depth + layer : spot + depth + layer + 1]
        a, b = factors(rows_down[layer], total, tall, cols)
        u = g_down[layer] * a * b
        g_down[layer] = u
        squared = jnp.where(lane == depth + layer, total_of(u * u), squared)
    cols = jnp.concatenate([full[6:7, :], full[7:8, 0 : E_ALL - STAT]], axis=1)
    cols = decay * edge_cols_ref[...] + (1.0 - decay) * (cols / height + eps_stat)
    edge_cols_new[...] = cols
    a, b = factors(rows_edge, full[7:8, spot + 2 * depth : spot + 2 * depth + 1], height, cols)
    u = g_edge[...] * a * b
    g_edge[...] = u
    squared = jnp.where(lane == 2 * depth, total_of(u * u), squared)
    squares[f] = jnp.broadcast_to(squared, (8, 128))
    for copy in share(2, squares):
        copy.wait()
    full = squares[0]
    for k in range(1, 8):
        full = full + squares[k]
    full = full[0:1, :]
    counts = jnp.where(lane < depth, height * wide, jnp.where(lane < 2 * depth, tall * D, height * classes))
    roots = jnp.sqrt(full / counts)
    step = rate / jnp.maximum(1.0, roots / clip_level)
    tail_ref[...] = jnp.where(lane == 2 * depth + 1, loss, roots)
    for layer in range(depth):
        in_new[layer] = in_ref[layer] - step[:, layer : layer + 1] * g_in[layer]
        down_new[layer] = down_ref[layer] - step[:, depth + layer : depth + layer + 1] * g_down[layer]
    edge_new[...] = edge_ref[...] - step[:, 2 * depth : 2 * depth + 1] * g_edge[...]


def update(sizes, out_t, out_m, sums, d_mods, cond, before, time1, s1, feats, time2, w_mods, weights, stats):
    shape = jax.ShapeDtypeStruct
    vm = pl.BlockSpec(memory_space=pltpu.VMEM)
    dma = pltpu.SemaphoreType.DMA
    inputs = (out_t, out_m, sums, d_mods, cond, before, time1, s1, feats, time2, w_mods) + weights + stats
    outs = tuple(shape(v.shape, F32) for v in weights + stats) + (shape((1, 128), F32),)
    return pl.pallas_call(
        functools.partial(update_kernel, sizes),
        out_shape=outs,
        in_specs=[vm] * len(inputs),
        out_specs=(vm,) * len(outs),
        scratch_shapes=[
            pltpu.VMEM(weights[0].shape, F32),
            pltpu.VMEM(weights[1].shape, F32),
            pltpu.VMEM(weights[2].shape, F32),
            pltpu.VMEM((8, OWN, SLOTS), BF16),
            pltpu.VMEM((D, SLOTS), BF16),
            pltpu.VMEM((D, 128), F32),
            pltpu.VMEM((8, 8, STAT), F32),
            pltpu.VMEM((8, 8, 128), F32),
            dma((3, 7)),
            dma((3, 7)),
        ],
        compiler_params=pltpu.CompilerParams(collective_id=3, has_side_effects=True, vmem_limit_bytes=60 * 1024 * 1024),
        name="step_update",
    )(*inputs)


def mix_weights(tsteps):
    betas = 0.0001 + (0.02 - 0.0001) * jnp.arange(TSTEPS, dtype=jnp.float32) / (TSTEPS - 1)
    alpha_bar = jnp.exp(jnp.cumsum(jnp.log(1.0 - betas)))
    picked = jnp.arange(TSTEPS)[None, :] == tsteps[:, None]
    return jnp.sum(jnp.where(picked, alpha_bar[None, :], 0.0), axis=1)


def patchify(latent_rows):
    images = latent_rows.shape[0]
    grid_side = GRID // PATCH
    shaped = latent_rows.reshape(images, CHANNELS, grid_side, PATCH, grid_side, PATCH)
    shaped = jnp.transpose(shaped, (0, 2, 4, 1, 3, 5))
    return shaped.reshape(images, grid_side * grid_side, CHANNELS * PATCH * PATCH)


def position_table():
    grid_side = GRID // PATCH
    quarter = D // 4
    omegas = 1.0 / 10000.0 ** (jnp.arange(quarter, dtype=jnp.float32) / quarter)
    places = jnp.arange(grid_side * grid_side)
    across = (places % grid_side).astype(jnp.float32)
    downward = (places // grid_side).astype(jnp.float32)

    def one_axis(coords):
        angles = coords[:, None] * omegas[None, :]
        return jnp.concatenate([jnp.sin(angles), jnp.cos(angles)], axis=1)

    return jnp.concatenate([one_axis(across), one_axis(downward)], axis=1)


def time_features(tsteps):
    half_freq = FREQ // 2
    frequencies = jnp.exp(-math.log(10000.0) * jnp.arange(half_freq, dtype=jnp.float32) / half_freq)
    angles = tsteps.astype(jnp.float32)[:, None] * frequencies[None, :]
    return jnp.concatenate([jnp.cos(angles), jnp.sin(angles)], axis=1)


def fetch(layer_in, layer_out):
    own_in = layer_in[:, :, 6 * D :].astype(BF16)
    own_out = layer_out.astype(BF16)
    w_in = lax.all_gather(own_in, "fsdp", axis=1, tiled=True)
    w_out = lax.all_gather(own_out, "fsdp", axis=1, tiled=True)
    return w_in, w_out


def matmul(a, b, form):
    return jnp.einsum(form, a, b, preferred_element_type=F32)


def step_of(grad, rows_new, cols_new, rows_mean):
    second = rows_new[:, :, None] * cols_new[:, None, :] / rows_mean[:, None, None]
    return grad * lax.rsqrt(second)


def plain(weight, grad, moment):
    moment_new = decay * moment + (1.0 - decay) * (grad * grad + eps_stat)
    update = grad * lax.rsqrt(moment_new)
    root = jnp.sqrt(jnp.mean(update * update, axis=-1, keepdims=True))
    return (weight - rate * update / jnp.maximum(1.0, root / clip_level), moment_new)


def library_step(
    latents,
    tsteps,
    labels,
    noise,
    layer_in,
    layer_out,
    edge_mat,
    layer_bias,
    top_bias,
    in_rows,
    in_cols,
    out_rows,
    out_cols,
    edge_rows,
    edge_cols,
    layer_bias_v,
    top_bias_v,
):
    images = latents.shape[0]
    depth, own, wide = layer_in.shape
    fsdp = lax.axis_size("fsdp")
    rep = lax.axis_size("rep")
    at_f = lax.axis_index("fsdp")
    at_r = lax.axis_index("rep")
    every = images * fsdp * rep
    width = own * fsdp
    MOD = 6 * D
    start_freq = NCLS + PATCH_IN
    start_tail = start_freq + FREQ

    edge_low = edge_mat.astype(BF16)
    small = jnp.concatenate([edge_low[:, : start_tail + D], edge_low[:, start_tail + 3 * D :]], axis=1)
    full = lax.all_gather(small, "fsdp", axis=0, tiled=True)
    class_cols = full[:, :NCLS]
    patch_cols = full[:, NCLS:start_freq]
    freq_cols = full[:, start_freq:start_tail]
    time_second = full[:, start_tail : start_tail + D]
    head_cols = full[:, start_tail + D : start_tail + D + PATCH_IN]
    all_tsteps, all_labels = (
        lax.all_gather(tsteps, ("fsdp", "rep"), axis=0, tiled=True),
        lax.all_gather(labels, ("fsdp", "rep"), axis=0, tiled=True),
    )
    features = time_features(all_tsteps).astype(BF16)
    time1 = matmul(features, freq_cols, "bf,df->bd") + top_bias[D : 2 * D]
    s1 = jax.nn.silu(time1).astype(BF16)
    picked = (all_labels[:, None] == jnp.arange(NCLS)[None, :]).astype(BF16)
    before = matmul(s1, time_second, "bd,de->be") + top_bias[2 * D : 3 * D] + matmul(picked, class_cols, "bc,dc->bd")
    cond = jax.nn.silu(before).astype(BF16)

    def own_part(values):
        return lax.dynamic_slice_in_dim(values, at_f * own, own, axis=1)

    low_in = layer_in.astype(BF16)
    w_mods = jnp.concatenate(
        [low_in[layer, :, :MOD] for layer in range(depth)] + [edge_low[:, start_tail + D : start_tail + 3 * D]], axis=1
    )
    cond_own = own_part(cond)
    group_own = lax.dynamic_index_in_dim(cond_own.reshape(fsdp, rep, images, own), at_r, axis=1, keepdims=False)
    part = matmul(group_own.reshape(fsdp * images, own), w_mods, "bd,de->be")
    bias_mods = jnp.concatenate([layer_bias[layer, :MOD] for layer in range(depth)] + [top_bias[3 * D : 5 * D]])
    mods = lax.psum_scatter(part, "fsdp", scatter_dimension=0, tiled=True) + bias_mods
    kinds = 6 * depth + 2
    mods = mods.reshape(images, kinds, D)

    alphas = mix_weights(tsteps)
    noisy = jnp.sqrt(alphas)[:, None, None] * latents + jnp.sqrt(1.0 - alphas)[:, None, None] * noise
    patches = patchify(noisy).astype(BF16).reshape(images * TOK, PATCH_IN)
    target = patchify(noise).reshape(images * TOK, PATCH_IN)

    w_in, w_out = fetch(layer_in, layer_out)
    bias_rows = jnp.concatenate([layer_bias[:, MOD : MOD + D], layer_bias[:, MOD + D :]], axis=1)
    g_in, g_out, sums, d_mods = compute(
        patches,
        target,
        position_table(),
        jnp.transpose(jnp.pad(mods, ((0, 8 - images), (0, 16 - kinds), (0, 0))), (1, 0, 2)),
        w_in,
        w_out,
        patch_cols,
        head_cols.T,
        bias_rows,
        top_bias[None, :D],
        top_bias[None, 5 * D : 5 * D + PATCH_IN],
    )

    d_mods = jnp.transpose(d_mods, (1, 0, 2))[:images, :kinds].reshape(images, kinds * D)
    d_mods = lax.all_gather(d_mods, ("fsdp", "rep"), axis=0, tiled=True)
    g_rows = matmul(cond_own, d_mods, "bd,be->de")
    g_bmods = jnp.sum(d_mods.astype(F32), axis=0)
    d_before = matmul(d_mods, w_mods, "be,de->bd") * silu_slope(own_part(before))
    g_class = jnp.einsum("bd,bc->dc", d_before, picked.astype(F32), precision=lax.Precision.HIGHEST)
    d_time2 = lax.all_gather(d_before.astype(BF16), "fsdp", axis=1, tiled=True)
    g_time2 = matmul(own_part(s1), d_time2, "bd,be->de")
    d_time1 = (matmul(d_time2, time_second, "be,de->bd") * silu_slope(time1)).astype(BF16)
    g_time1 = matmul(own_part(d_time1), features, "bd,bf->df")

    shard_in = lax.psum(lax.psum_scatter(g_in, "fsdp", scatter_dimension=1, tiled=True), "rep")
    shard_out = lax.psum(lax.psum_scatter(g_out, "fsdp", scatter_dimension=1, tiled=True), "rep")
    sums = lax.psum(sums, ("fsdp", "rep"))
    g_patch, g_head = sums[:S_HEAD], sums[S_HEAD:S_BIAS]
    g_bias = sums[S_BIAS:S_BPATCH].reshape(depth, BW)
    g_bpatch, g_bhead = sums[S_BPATCH : S_BPATCH + 1], sums[S_BHEAD : S_BHEAD + 1, :PATCH_IN]
    sse = jnp.sum(sums[S_SSE, :PATCH_IN])

    tok_total = every * TOK
    scale_grad = 1.0 / (PATCH_IN * math.sqrt(tok_total))
    loss = sse / (tok_total * PATCH_IN)
    fin = depth * MOD
    grad_edge = jnp.concatenate(
        [
            g_class,
            own_part(g_patch).T,
            g_time1,
            g_time2,
            g_rows[:, fin:],
            own_part(g_head).T,
            jnp.zeros((own, PATCH_IN), F32),
        ],
        axis=1,
    )[None] * scale_grad
    grad_in = jnp.concatenate([jnp.stack([g_rows[:, layer * MOD : (layer + 1) * MOD] for layer in range(depth)]), shard_in], axis=2) * scale_grad
    grad_out = shard_out * scale_grad
    grad_lbias = jnp.concatenate([g_bmods[:fin].reshape(depth, MOD), g_bias], axis=1) * scale_grad
    grad_tbias = jnp.concatenate(
        [
            g_bpatch[0],
            jnp.sum(d_time1.astype(F32), axis=0),
            jnp.sum(d_time2.astype(F32), axis=0),
            g_bmods[fin:],
            g_bhead[0],
            jnp.zeros((PATCH_IN,), F32),
        ]
    ) * scale_grad

    full_rows_in = width
    full_rows_out = layer_out.shape[1] * fsdp
    full_rows_edge = edge_mat.shape[0] * fsdp
    square_in = grad_in * grad_in + eps_stat
    square_out = grad_out * grad_out + eps_stat
    square_edge = grad_edge * grad_edge + eps_stat
    rows_in_new = decay * in_rows + (1.0 - decay) * jnp.mean(square_in, axis=2)
    rows_out_new = decay * out_rows + (1.0 - decay) * jnp.mean(square_out, axis=2)
    rows_edge_new = decay * edge_rows[None] + (1.0 - decay) * jnp.mean(square_edge, axis=2)
    col_in, total_in, col_out, total_out, col_edge, total_edge = lax.psum(
        (
            jnp.sum(square_in, axis=1),
            jnp.sum(rows_in_new, axis=1),
            jnp.sum(square_out, axis=1),
            jnp.sum(rows_out_new, axis=1),
            jnp.sum(square_edge, axis=1),
            jnp.sum(rows_edge_new, axis=1),
        ),
        "fsdp",
    )
    cols_in_new = decay * in_cols + (1.0 - decay) * col_in / full_rows_in
    cols_out_new = decay * out_cols + (1.0 - decay) * col_out / full_rows_out
    cols_edge_new = decay * edge_cols[None] + (1.0 - decay) * col_edge / full_rows_edge
    update_in = step_of(grad_in, rows_in_new, cols_in_new, total_in / full_rows_in)
    update_out = step_of(grad_out, rows_out_new, cols_out_new, total_out / full_rows_out)
    update_edge = step_of(grad_edge, rows_edge_new, cols_edge_new, total_edge / full_rows_edge)
    sum_in, sum_out, sum_edge = lax.psum(
        (
            jnp.sum(update_in * update_in, axis=(1, 2)),
            jnp.sum(update_out * update_out, axis=(1, 2)),
            jnp.sum(update_edge * update_edge, axis=(1, 2)),
        ),
        "fsdp",
    )
    roots_in = jnp.sqrt(sum_in / (full_rows_in * grad_in.shape[2]))
    roots_out = jnp.sqrt(sum_out / (full_rows_out * grad_out.shape[2]))
    roots_edge = jnp.sqrt(sum_edge / (full_rows_edge * grad_edge.shape[2]))
    factor_in = jnp.maximum(1.0, roots_in / clip_level)[:, None, None]
    factor_out = jnp.maximum(1.0, roots_out / clip_level)[:, None, None]
    factor_edge = jnp.maximum(1.0, roots_edge / clip_level)[:, None, None]
    in_new = layer_in - rate * update_in / factor_in
    out_new = layer_out - rate * update_out / factor_out
    edge_new = (edge_mat[None] - rate * update_edge / factor_edge)[0]
    clip_roots = jnp.concatenate([roots_in, roots_out, roots_edge])
    lbias_new, lbias_v_new = plain(layer_bias, grad_lbias, layer_bias_v)
    tbias_new, tbias_v_new = plain(top_bias, grad_tbias, top_bias_v)
    return (
        loss,
        in_new,
        out_new,
        edge_new,
        lbias_new,
        tbias_new,
        rows_in_new,
        cols_in_new,
        rows_out_new,
        cols_out_new,
        rows_edge_new[0],
        cols_edge_new[0],
        lbias_v_new,
        tbias_v_new,
        clip_roots,
    )


def direct_step(
    latents,
    tsteps,
    labels,
    noise,
    layer_in,
    layer_out,
    edge_mat,
    layer_bias,
    top_bias,
    in_rows,
    in_cols,
    out_rows,
    out_cols,
    edge_rows,
    edge_cols,
    layer_bias_v,
    top_bias_v,
):
    images = latents.shape[0]
    depth = layer_in.shape[0]
    MOD = 6 * D
    tokens = images * 32 * TOK
    classes = edge_mat.shape[1]
    start_freq = NCLS + PATCH_IN
    start_tail = start_freq + FREQ

    def wide_to(v, width, fill=0.0):
        return jnp.pad(v, ((0, 0), (0, width - v.shape[1])), constant_values=fill)

    def aligned(v, fill):
        return jnp.concatenate(
            [
                wide_to(v[:, :NCLS], E_PATCH, fill),
                wide_to(v[:, NCLS:start_freq], E_T1 - E_PATCH, fill),
                v[:, start_freq : start_tail + 3 * D],
                wide_to(v[:, start_tail + 3 * D :], E_ALL - E_HEAD, fill),
            ],
            axis=1,
        )

    edge_a = aligned(edge_mat, 0.0)
    edge_low = edge_a.astype(BF16)
    small = jnp.concatenate(
        [
            edge_low[:, :E_PATCH],
            edge_low[:, E_T1:E_FIN],
            edge_low[:, E_PATCH : E_PATCH + PATCH_IN],
            edge_low[:, E_HEAD : E_HEAD + PATCH_IN],
            jnp.zeros((OWN, C_ALL - C_HEAD - PATCH_IN), BF16),
        ],
        axis=1,
    )
    w_mods = jnp.concatenate([layer_in[layer, :, :MOD].astype(BF16) for layer in range(depth)] + [edge_low[:, E_FIN:E_HEAD]], axis=1)
    feat = jnp.concatenate(
        [time_features(tsteps), jnp.broadcast_to(labels.astype(F32)[:, None], (images, 128))], axis=1
    )
    feat = jnp.pad(feat, ((0, 8 - images), (0, 0)))
    bias_mods = jnp.concatenate([layer_bias[layer, :MOD] for layer in range(depth)] + [top_bias[3 * D : 5 * D]])[None]
    full, w_in, w_out, mods, time1, s1, before, cond, feats = prologue(
        small,
        feat,
        w_mods,
        top_bias[D : 3 * D].reshape(2, D),
        bias_mods,
        layer_in[:, :, MOD:].astype(BF16),
        layer_out.astype(BF16).reshape(depth, 4, OWN, D),
    )

    alphas = mix_weights(tsteps)
    noisy = jnp.sqrt(alphas)[:, None, None] * latents + jnp.sqrt(1.0 - alphas)[:, None, None] * noise
    patches = patchify(noisy).astype(BF16).reshape(images * TOK, PATCH_IN)
    target = patchify(noise).reshape(images * TOK, PATCH_IN)
    bias_rows = jnp.concatenate([layer_bias[:, MOD : MOD + D], layer_bias[:, MOD + D :]], axis=1)
    g_t, g_m, sums, d_mods = compute(
        patches,
        target,
        position_table(),
        mods,
        w_in,
        w_out.reshape(depth, FF, D),
        full[:, C_PATCH : C_PATCH + PATCH_IN],
        full[:, C_HEAD : C_HEAD + PATCH_IN].T,
        bias_rows,
        top_bias[None, :D],
        top_bias[None, 5 * D : 5 * D + PATCH_IN],
        blocked=True,
    )
    out_t, out_m, sums, d_mods = reduce_grads(g_t, g_m, sums, d_mods)
    weights = (layer_in, layer_out, edge_a, layer_bias, wide_to(top_bias[None], 16 * 128))
    stats = (
        in_rows,
        in_cols,
        out_rows,
        out_cols,
        edge_rows[None],
        aligned(edge_cols[None], 1.0),
        layer_bias_v,
        wide_to(top_bias_v[None], 16 * 128, 1.0),
    )
    (
        in_new,
        out_new,
        edge_new,
        lbias_new,
        tbias_new,
        in_rows_new,
        in_cols_new,
        out_rows_new,
        out_cols_new,
        edge_rows_new,
        edge_cols_new,
        lbias_v_new,
        tbias_v_new,
        tail,
    ) = update(
        (classes, tokens), out_t, out_m, sums, d_mods, cond, before, time1, s1, feats, full[:, C_T2 : C_T2 + D], w_mods, weights, stats
    )

    def natural(v):
        return jnp.concatenate(
            [v[:, :NCLS], v[:, E_PATCH : E_PATCH + PATCH_IN], v[:, E_T1 : E_HEAD + 2 * PATCH_IN]], axis=1
        )

    count = top_bias.shape[0]
    return (
        tail[0, 2 * depth + 1],
        in_new,
        out_new,
        natural(edge_new),
        lbias_new,
        tbias_new[0, :count],
        in_rows_new,
        in_cols_new,
        out_rows_new,
        out_cols_new,
        edge_rows_new[0],
        natural(edge_cols_new)[0],
        lbias_v_new,
        tbias_v_new[0, :count],
        tail[0, : 2 * depth + 1],
    )


def shards(*arrays):
    layer_in = arrays[4]
    mesh = (lax.axis_size("fsdp"), lax.axis_size("rep"), layer_in.shape[0], layer_in.shape[1])
    return (direct_step if mesh == (8, 4, 2, OWN) else library_step)(*arrays)


def solution(mesh):
    placed = (
        P(("fsdp", "rep"), None, None),
        P(("fsdp", "rep")),
        P(("fsdp", "rep")),
        P(("fsdp", "rep"), None, None),
        P(None, "fsdp", None),
        P(None, "fsdp", None),
        P("fsdp", None),
        P(),
        P(),
        P(None, "fsdp"),
        P(),
        P(None, "fsdp"),
        P(),
        P("fsdp"),
        P(),
        P(),
        P(),
    )
    return jax.shard_map(
        shards,
        mesh=mesh,
        in_specs=placed,
        out_specs=(
            P(),
            P(None, "fsdp", None),
            P(None, "fsdp", None),
            P("fsdp", None),
            P(),
            P(),
            P(None, "fsdp"),
            P(),
            P(None, "fsdp"),
            P(),
            P("fsdp"),
            P(),
            P(),
            P(),
            P(),
        ),
        check_vma=False,
    )
```

```python
import functools
import math

import jax
import jax.numpy as jnp
import numpy as np
from jax import lax
from jax.experimental import pallas as pl
from jax.experimental.pallas import tpu as pltpu
from jax.sharding import PartitionSpec as P

NCLS = 1001
FREQ = 256
CHANNELS = 4
PATCH = 2
GRID = 32
TSTEPS = 1000
eps_stat = 1e-30
decay = 0.5
rate = 0.01
clip_level = 1.0
D = 384
HEADS = 6
HEAD_DIM = 64
FF = 1536
TOK = 256
PATCH_IN = 16
eps_norm = 1e-06
F32 = jnp.float32
BF16 = jnp.bfloat16
GELU_A = 0.7978845608028654
GELU_B = 0.044715
NT = (((1,), (1,)), ((), ()))
TN = (((0,), (0,)), ((), ()))
FFC = 768
OWN = 48


def dot(a, b, dims=(((1,), (0,)), ((), ()))):
    return lax.dot_general(a, b, dims, preferred_element_type=F32)


def norm_rows(t):
    center = t - jnp.mean(t, axis=-1, keepdims=True)
    spread = jnp.mean(center * center, axis=-1, keepdims=True)
    scale = lax.rsqrt(spread + eps_norm)
    return center * scale, scale


def norm_back(dn, n, scale):
    mean_d = jnp.mean(dn, axis=-1, keepdims=True)
    mean_dn = jnp.mean(dn * n, axis=-1, keepdims=True)
    return scale * (dn - mean_d - n * mean_dn)


def rows_sum(v):
    return jnp.sum(v, axis=0, keepdims=True)


def soft_rows(s):
    e = jnp.exp(s - jnp.max(s, axis=-1, keepdims=True))
    return e / jnp.sum(e, axis=-1, keepdims=True)


def gelu_parts(x):
    t = jnp.tanh(GELU_A * (x + GELU_B * (x * x * x)))
    return t


QKV = 0
WO = 3 * D
WF1 = 4 * D
BQ, BV, BO, BF1, BF2 = 0, D, 2 * D, 3 * D, 3 * D + FF
BW = 4 * D + FF
S_HEAD, S_BIAS, S_BPATCH, S_BHEAD, S_SSE, S_ROWS = 16, 32, 48, 49, 50, 56


class BiasRows:
    def __init__(self, ref):
        self.ref = ref

    def __getitem__(self, layer):
        return self.ref[layer][:, 6 * D :]


class BiasRows:
    def __init__(self, ref):
        self.ref = ref

    def __getitem__(self, layer):
        return self.ref[layer][:, 6 * D :]


class BiasRows:
    def __init__(self, ref):
        self.ref = ref

    def __getitem__(self, layer):
        return self.ref[layer][:, 6 * D :]


class BiasRows:
    def __init__(self, ref):
        self.ref = ref

    def __getitem__(self, layer):
        return self.ref[layer][:, 6 * D :]


def compute_kernel(images, group, direct, *refs):
    refs = list(refs)

    def take(count):
        got = refs[:count]
        del refs[:count]
        return got

    patches_ref, target_ref, pos_ref, mods_ref, first_in_ref, first_out_ref, w_patch_ref, w_head_ref = take(8)
    lbias_ref, tbias_ref = take(2)
    own_in_ref, own_out_ref = take(2) if direct else (None,) * 2
    g_in_ref, g_out_ref, sums_ref, g_mods_ref = take(4)
    out_t_ref, out_m_ref, out_d_ref = take(3) if direct else (None,) * 3
    w_in_ref, w_out_ref, tok, mid, qkv, att, branch, outb, normed, act, dinner, dsmall, stage, mod_sums, sems, w_sems = take(16)
    steps = images // group
    crow = group * TOK
    depth = lbias_ref.shape[0]
    lane = lax.broadcasted_iota(jnp.int32, (TOK, 128), 1)
    first_half = lane < HEAD_DIM

    def rows_of(i):
        return pl.ds(pl.multiple_of(i * TOK, TOK), TOK)

    def chunk_of(i):
        return pl.ds(pl.multiple_of(i * crow, crow), crow)

    def near(j):
        return slice(j * TOK, (j + 1) * TOK)

    def down_rows(layer, c):
        rows = FF // w_out_ref.shape[1]
        return w_out_ref[layer, c // rows : (c + FFC) // rows].reshape(FFC, D)

    def mod_row(b, k):
        return mods_ref[k, pl.ds(b, 1), :]

    loads = []
    for layer in range(1 if direct else depth):
        source = first_in_ref, first_out_ref
        if not direct:
            source = first_in_ref.at[layer], first_out_ref.at[layer]
        for n, (ours, theirs) in enumerate(zip((w_in_ref, w_out_ref), source)):
            loads.append(pltpu.make_async_copy(theirs, ours.at[layer], w_sems.at[2 * layer + n]))
            loads[-1].start()
    bias_ref = BiasRows(lbias_ref)

    sums_ref[...] = jnp.zeros_like(sums_ref)
    mod_sums[...] = jnp.zeros_like(mod_sums)

    def add_bias(layer, first, value):
        for at in range(0, value.shape[1], D):
            row = (first + at) // D
            sums_ref[S_BIAS // 8 + layer, row : row + 1, :] += value[:, at : at + D]

    def put_mod(b, k, value):
        mod_sums[k, pl.ds(b, 1), :] = value

    if direct:
        wide_m, wide_t = take(4), take(4)
        plane = take(2 * depth)
        s_got, r_sends, r_recvs, r_loads, g_sends, g_recvs, g_local, b_sends, b_recvs, w_sends, w_recvs, w_local = take(12)
        partners = Partners().all()
        greet(partners)
        m_pieces, t_pieces = [], []
        for layer in range(depth):
            for kind, (pieces, source, out, wide) in enumerate(
                ((m_pieces, g_out_ref, out_m_ref, wide_m), (t_pieces, g_in_ref, out_t_ref, wide_t))
            ):
                n = 2 * layer + kind
                pieces.append(
                    Reducer(source.at[layer], list(wide) + [plane[n]], out.at[layer], r_sends.at[n], r_recvs.at[n], r_loads.at[n])
                )
        w_pieces = []
        for layer in range(1, depth):
            own, ours = own_in_ref.at[layer], w_in_ref.at[layer]

            def sems_of(n, first=3 * (layer - 1)):
                return w_sends.at[first + n], w_recvs.at[first + n], w_local.at[first + n]

            w_pieces.append(by_columns(own, ours, *sems_of(0), 0, 4 * D))
            w_pieces.append(by_columns(own, ours, *sems_of(1), 4 * D, FF))
            w_pieces.append(by_rows(own_out_ref.at[layer], w_out_ref.at[layer], *sems_of(2)))
        s_piece = Butterfly(sums_ref, s_got, b_sends, b_recvs)
        d_pieces = []
        for n, (low, high) in enumerate(((0, 6 * (depth - 1)), (6 * (depth - 1), 6 * depth + 2))):
            d_pieces.append(
                Gatherer(
                    lambda q, a=low, b=high: g_mods_ref.at[a:b],
                    lambda f, q, a=low, b=high: out_d_ref.at[q, f, a:b],
                    lambda q, a=low, b=high: out_d_ref.at[q, :, a:b],
                    g_sends.at[n],
                    g_recvs.at[n],
                    g_local.at[n],
                )
            )

    def send_mods(low, high):
        g_mods_ref[low:high] = mod_sums[low:high].astype(BF16)

    def in_moves(layer, first):
        moves = []
        for q in range(4):
            source = stage.at[0, :, q * D : (q + 1) * D]
            if direct:
                target = (g_in_ref if first == QKV else g_out_ref).at[layer, q, :, 0:D]
            else:
                target = g_in_ref.at[layer, :, first + q * D : first + (q + 1) * D]
            moves.append(pltpu.make_async_copy(source, target, sems.at[0, q]))
        return moves

    def down_moves(layer):
        moves = []
        for c in range(4):
            if not direct:
                source = stage.at[1, :, c * D : (c + 1) * D]
                target = g_out_ref.at[layer, c * D : (c + 1) * D, :]
                moves.append(pltpu.make_async_copy(source, target, sems.at[1, c]))
                continue
            for owner in range(2):
                for q in range(4):
                    start = owner * (D // 2) + q * OWN
                    source = stage.at[1, start : start + OWN, c * D : (c + 1) * D]
                    begin = (2 * c + owner) * OWN
                    target = g_out_ref.at[layer, q, begin : begin + OWN, D : 2 * D]
                    moves.append(pltpu.make_async_copy(source, target, sems.at[1, len(moves)]))
        return moves

    def start(moves):
        for move in moves:
            move.start()

    def finish(moves):
        for move in moves:
            move.wait()

    def clear(slot):
        @pl.loop(0, FF // D)
        def _(c):
            stage[slot, :, pl.ds(pl.multiple_of(c * D, D), D)] = jnp.zeros((D, D), F32)

    def at(li, i, *actions):
        if not direct:
            return

        def place_at(turn_li, turn_i):
            for want_li, want_i, todo in actions:

                @pl.when(jnp.logical_and(turn_li == want_li, turn_i == want_i))
                def _():
                    for piece, k in todo:
                        piece.step(k)

        place_at(li, i)

    @pl.loop(0, images)
    def _(b):
        r = rows_of(b)
        tok[0, r, :] = dot(patches_ref[r, :], w_patch_ref[...], NT) + tbias_ref[:, 0:D] + pos_ref[...]

    def half(v, which):
        zero = jnp.zeros_like(v)
        return jnp.where(first_half, v, zero) if which == 0 else jnp.where(first_half, zero, v)

    def attention(layer, r):
        for pair in range(HEADS // 2):
            c = pair * 128
            q = qkv[layer, r, c : c + 128]
            k = qkv[layer, r, D + c : D + c + 128]
            v = qkv[layer, r, 2 * D + c : 2 * D + c + 128]
            got = []
            for which in range(2):
                s = dot(half(q, which), k, NT) * HEAD_DIM ** (-0.5)
                got.append(dot(soft_rows(s).astype(BF16), v))
            att[layer, r, c : c + 128] = jnp.where(first_half, got[0], got[1]).astype(BF16)

    def modulated(t, b, k):
        n, scale = norm_rows(t)
        return n, scale, (n * (1.0 + mod_row(b, k + 1)) + mod_row(b, k)).astype(BF16)

    for load in loads:
        load.wait()
    if direct:
        w_a, w_f, w_o = w_pieces

    @pl.loop(0, depth)
    def _(layer):
        mo = layer * 6

        @pl.loop(0, steps)
        def _(i):
            if direct:
                at(
                    layer,
                    i,
                    (0, 0, [(w_a, 0), (w_f, 0)]),
                    (0, 1, [(w_a, 2), (w_f, 1), (w_o, 1)]),
                    (1, 0, [(w_a, 4)]),
                )
            cr = chunk_of(i)
            bias = bias_ref[layer]
            for j in range(group):
                b = i * group + j
                normed[near(j), :] = modulated(tok[layer, rows_of(b), :], b, mo)[2]
            hc = normed[...]
            p = dot(hc, w_in_ref[layer, :, QKV : QKV + 2 * D])
            qkv[layer, cr, 0:D] = (p[:, 0:D] + bias[:, BQ : BQ + D]).astype(BF16)
            qkv[layer, cr, D : 2 * D] = p[:, D : 2 * D].astype(BF16)
            p = dot(hc, w_in_ref[layer, :, QKV + 2 * D : QKV + 3 * D])
            qkv[layer, cr, 2 * D : 3 * D] = (p + bias[:, BV : BV + D]).astype(BF16)
            for j in range(group):
                attention(layer, rows_of(i * group + j))
            if direct:
                at(
                    layer,
                    i,
                    (0, 0, [(w_a, 1), (w_o, 0)]),
                    (0, 1, [(w_a, 3), (w_f, 2), (w_o, 2)]),
                    (1, 0, [(w_f, 3), (w_o, 3), (w_f, 4), (w_o, 4)]),
                )
            br = dot(att[layer, cr, :], w_in_ref[layer, :, WO : WO + D]) + bias[:, BO : BO + D]
            branch[layer, cr, :] = br.astype(BF16)
            for j in range(group):
                b = i * group + j
                r = rows_of(b)
                t2 = tok[layer, r, :] + mod_row(b, mo + 2) * br[near(j)]
                mid[layer, r, :] = t2
                normed[near(j), :] = modulated(t2, b, mo + 3)[2]
            mc = normed[...]
            out = jnp.zeros((crow, D), F32) + bias[:, BF2 : BF2 + D]
            for c in range(0, FF, FFC):
                x = dot(mc, w_in_ref[layer, :, WF1 + c : WF1 + c + FFC]) + bias[:, BF1 + c : BF1 + c + FFC]
                a = (x * (0.5 * (1.0 + gelu_parts(x)))).astype(BF16)
                out = out + dot(a, down_rows(layer, c))
            outb[layer, cr, :] = out.astype(BF16)
            for j in range(group):
                b = i * group + j
                r = rows_of(b)
                tok[layer + 1, r, :] = mid[layer, r, :] + mod_row(b, mo + 5) * out[near(j)]

    dtok = tok.at[depth]

    @pl.loop(0, images)
    def _(b):
        r = rows_of(b)
        k = 6 * depth
        n, scale, n3 = modulated(dtok[r, :], b, k)
        miss = dot(n3, w_head_ref[...]) + tbias_ref[:, 5 * D : 5 * D + PATCH_IN] - target_ref[r, :]
        sums_ref[S_SSE // 8, S_SSE % 8 : S_SSE % 8 + 1, 0:PATCH_IN] += rows_sum(miss * miss)
        dp = (2.0 * miss).astype(BF16)
        sums_ref[S_HEAD // 8 : S_HEAD // 8 + 2] += dot(dp, n3, TN).reshape(2, 8, D)
        sums_ref[S_BHEAD // 8, S_BHEAD % 8 : S_BHEAD % 8 + 1, 0:PATCH_IN] += rows_sum(dp.astype(F32))
        dn3 = dot(dp, w_head_ref[...], NT)
        put_mod(b, k, rows_sum(dn3))
        put_mod(b, k + 1, rows_sum(dn3 * n))
        dtok[r, :] = norm_back(dn3 * (1.0 + mod_row(b, k + 1)), n, scale)

    if direct:
        t_last, m_last = t_pieces[depth - 1], m_pieces[depth - 1]
        t_first, m_first = t_pieces[0], m_pieces[0]
        d_first, d_last = d_pieces

    @pl.loop(0, depth)
    def _(li):
        layer = depth - 1 - li
        mo = layer * 6
        bias = bias_ref[layer]

        @pl.when(li > 0)
        def _():
            finish(in_moves(layer + 1, QKV))
            send_mods(6 * (depth - 1), 6 * depth + 2)

        clear(0)
        clear(1)

        @pl.loop(0, steps)
        def _(i):
            if direct:
                at(li, i, (1, 0, [(m_last, 2), (t_last, 0), (d_last, 0)]), (1, 1, [(t_last, 1)]))
            cr = chunk_of(i)
            for j in range(group):
                b = i * group + j
                r = rows_of(b)
                normed[near(j), :] = modulated(mid[layer, r, :], b, mo + 3)[2]
                d = dtok[r, :]
                put_mod(b, mo + 5, rows_sum(d * outb[layer, r, :].astype(F32)))
                do = (d * mod_row(b, mo + 5)).astype(BF16)
                dsmall[near(j), :] = do
                add_bias(layer, BF2, rows_sum(do.astype(F32)))
            mc = normed[...]
            do = dsmall[...]
            dm = jnp.zeros((crow, D), F32)
            for c in range(0, FF, FFC):
                x = dot(mc, w_in_ref[layer, :, WF1 + c : WF1 + c + FFC]) + bias[:, BF1 + c : BF1 + c + FFC]
                x2 = x * x
                t = jnp.tanh(GELU_A * (x + GELU_B * (x2 * x)))
                cdf = 0.5 * (1.0 + t)
                act[:, c : c + FFC] = (x * cdf).astype(BF16)
                slope = cdf + (0.5 * GELU_A) * x * (1.0 - t * t) * (1.0 + (3.0 * GELU_B) * x2)
                di = (dot(do, down_rows(layer, c), NT) * slope).astype(BF16)
                dinner[:, c : c + FFC] = di
                add_bias(layer, BF1 + c, rows_sum(di.astype(F32)))
                dm = dm + dot(di, w_in_ref[layer, :, WF1 + c : WF1 + c + FFC], NT)
            for j in range(group):
                b = i * group + j
                r = rows_of(b)
                n, scale = norm_rows(mid[layer, r, :])
                dmj = dm[near(j)]
                put_mod(b, mo + 3, rows_sum(dmj))
                put_mod(b, mo + 4, rows_sum(dmj * n))
                dtok[r, :] = dtok[r, :] + norm_back(dmj * (1.0 + mod_row(b, mo + 4)), n, scale)

            if direct:
                at(li, i, (1, 0, [(d_last, 1)]), (1, 1, [(m_last, 3), (d_last, 2)]))

            @pl.loop(0, FF // FFC)
            def _(c):
                cs = pl.ds(pl.multiple_of(c * FFC, FFC), FFC)
                stage[0, :, cs] += dot(normed[...], dinner[:, cs], TN)

            @pl.loop(0, FF // D)
            def _(c):
                cs = pl.ds(pl.multiple_of(c * D, D), D)
                stage[1, :, cs] += dot(dsmall[...], act[:, cs], TN)

        start(in_moves(layer, WF1))

        @pl.loop(0, FF // D)
        def _(c):
            cs = pl.ds(pl.multiple_of(c * D, D), D)
            stage[1, :, cs] = stage[1, :, cs].T

        start(down_moves(layer))

        @pl.loop(0, steps)
        def _(i):
            if direct:
                at(li, i, (1, 0, [(t_last, 2)]))
            cr = chunk_of(i)
            for j in range(group):
                b = i * group + j
                r = rows_of(b)
                d = dtok[r, :]
                put_mod(b, mo + 2, rows_sum(d * branch[layer, r, :].astype(F32)))
                db = (d * mod_row(b, mo + 2)).astype(BF16)
                dsmall[near(j), :] = db
                add_bias(layer, BO, rows_sum(db.astype(F32)))
            branch[layer, cr, :] = dot(dsmall[...], w_in_ref[layer, :, WO : WO + D], NT).astype(BF16)

            @pl.when(i == 0)
            def _():
                finish(in_moves(layer, WF1))
                finish(down_moves(layer))
                clear(0)

            if direct:
                at(li, i, (0, 0, [(m_last, 0)]), (1, 0, [(m_last, 4)]), (1, 1, [(m_first, 1), (t_last, 4)]))
            for j in range(group):
                r = rows_of(i * group + j)
                for pair in range(HEADS // 2):
                    c = pair * 128
                    q = qkv[layer, r, c : c + 128]
                    k = qkv[layer, r, D + c : D + c + 128]
                    v = qkv[layer, r, 2 * D + c : 2 * D + c + 128]
                    da = branch[layer, r, c : c + 128]
                    got = []
                    for which in range(2):
                        s = dot(half(q, which), k, NT) * HEAD_DIM ** (-0.5)
                        p = soft_rows(s)
                        dv = dot(p.astype(BF16), da, TN)
                        dpr = dot(half(da, which), v, NT)
                        ds = p * (dpr - jnp.sum(dpr * p, axis=-1, keepdims=True))
                        ds = ds.astype(BF16)
                        dq = dot(ds, k)
                        dk = dot(ds, q, TN)
                        got.append((dq, dk, dv))
                    dq = (jnp.where(first_half, got[0][0], got[1][0]) * HEAD_DIM ** (-0.5)).astype(BF16)
                    dk = (jnp.where(first_half, got[0][1], got[1][1]) * HEAD_DIM ** (-0.5)).astype(BF16)
                    dv = jnp.where(first_half, got[0][2], got[1][2]).astype(BF16)
                    qkv[layer, r, c : c + 128] = dq
                    qkv[layer, r, D + c : D + c + 128] = dk
                    qkv[layer, r, 2 * D + c : 2 * D + c + 128] = dv
                    sums_ref[S_BIAS // 8 + layer, 0:1, c : c + 128] += rows_sum(dq.astype(F32))
                    sums_ref[S_BIAS // 8 + layer, 1:2, c : c + 128] += rows_sum(dv.astype(F32))
            if direct:
                at(
                    li,
                    i,
                    (0, 0, [(m_last, 1)]),
                    (1, 0, [(m_last, 5), (m_first, 0), (t_last, 3), (d_last, 3)]),
                    (1, 1, [(t_last, 5), (d_last, 4)]),
                )
            dh = dot(qkv[layer, cr, :], w_in_ref[layer, :, QKV : QKV + 3 * D], NT)
            for j in range(group):
                b = i * group + j
                r = rows_of(b)
                n, scale, h = modulated(tok[layer, r, :], b, mo)
                normed[near(j), :] = h
                dhj = dh[near(j)]
                put_mod(b, mo, rows_sum(dhj))
                put_mod(b, mo + 1, rows_sum(dhj * n))
                dtok[r, :] = dtok[r, :] + norm_back(dhj * (1.0 + mod_row(b, mo + 1)), n, scale)

            @pl.loop(0, 3)
            def _(c):
                cs = pl.ds(pl.multiple_of(c * D, D), D)
                stage[0, :, cs] += dot(normed[...], qkv[layer, cr, cs], TN)

            stage[0, :, 3 * D : 4 * D] += dot(att[layer, cr, :], dsmall[...], TN)

        start(in_moves(layer, QKV))

    if direct:
        send_mods(0, 6 * (depth - 1))
        d_first.step(0)
        m_first.step(2)
    else:
        g_mods_ref[...] = mod_sums[...].astype(BF16)

    @pl.loop(0, images)
    def _(b):
        r = rows_of(b)
        d = dtok[r, :].astype(BF16)
        sums_ref[S_BPATCH // 8, S_BPATCH % 8 : S_BPATCH % 8 + 1, :] += rows_sum(d.astype(F32))
        sums_ref[0:2] += dot(patches_ref[r, :], d, TN).reshape(2, 8, D)

    finish(in_moves(0, QKV))
    if direct:
        for piece, k in (
            (t_first, 0),
            (s_piece, 0),
            (d_first, 1),
            (t_first, 1),
            (s_piece, 1),
            (d_first, 2),
            (s_piece, 2),
            (t_first, 2),
            (m_first, 3),
            (d_first, 3),
            (s_piece, 3),
            (s_piece, 4),
            (t_first, 3),
            (d_first, 4),
            (s_piece, 5),
            (m_first, 4),
            (t_first, 4),
            (m_first, 5),
            (t_first, 5),
        ):
            piece.step(k)


def run_steps(plans):
    last = max(first + count for first, count, _ in plans)
    for tick in range(last):
        for first, count, piece in plans:
            if 0 <= tick - first < count:
                piece.step(tick - first)


def compute(patches, target, pos, mods, w_in, w_out, w_patch, w_head, lbias, tbias, own=(), group=3):
    direct = len(own) > 0
    depth = lbias.shape[0]
    rows = patches.shape[0]
    images = rows // TOK
    crow = group * TOK
    kinds = mods.shape[0]
    vm = pl.BlockSpec(memory_space=pltpu.VMEM)
    anyspace = pl.BlockSpec(memory_space=pl.ANY)
    shape = jax.ShapeDtypeStruct
    dma = pltpu.SemaphoreType.DMA
    out_shape = [
        shape((depth, 4, D, D) if direct else (depth, D, 4 * D + FF), F32),
        shape((depth, 4, D, 2 * D) if direct else (depth, FF, D), F32),
        shape((S_ROWS // 8, 8, D), F32),
        shape((kinds, 8, D), BF16),
    ]
    out_specs = [anyspace, anyspace, vm, vm]
    scratch = [
        pltpu.VMEM((depth, D, 4 * D + FF), BF16),
        pltpu.VMEM((depth,) + (w_out.shape if direct else w_out.shape[1:]), BF16),
        pltpu.VMEM((depth + 1, rows, D), F32),
        pltpu.VMEM((depth, rows, D), F32),
        pltpu.VMEM((depth, rows, 3 * D), BF16),
        pltpu.VMEM((depth, rows, D), BF16),
        pltpu.VMEM((depth, rows, D), BF16),
        pltpu.VMEM((depth, rows, D), BF16),
        pltpu.VMEM((crow, D), BF16),
        pltpu.VMEM((crow, FF), BF16),
        pltpu.VMEM((crow, FF), BF16),
        pltpu.VMEM((crow, D), BF16),
        pltpu.VMEM((2, D, FF), F32),
        pltpu.VMEM((kinds, 8, D), F32),
        dma((2, 32)),
        dma((2 * depth,)),
    ]
    params = dict(vmem_limit_bytes=67_043_328)
    if direct:
        out_shape += [
            shape((depth, 4, OWN, D), F32),
            shape((depth, 4, OWN, 2 * D), F32),
            shape((4, 8, kinds, 8, D), BF16),
        ]
        out_specs += [vm, vm, anyspace]
        scratch += wide_scratch(2 * D) + wide_scratch(D)
        for _ in range(depth):
            scratch += [pltpu.VMEM((8, OWN, 2 * D), BF16), pltpu.VMEM((8, OWN, D), BF16)]
        count = 2 * depth
        gathers = 3 * (depth - 1)
        scratch += [pltpu.VMEM((5, S_ROWS // 8, 8, D), F32), dma((count, 13)), dma((count, 13)), dma((count, 2))]
        scratch += [dma((2, 10)), dma((2, 10)), dma((2,)), dma((5,)), dma((5,))]
        scratch += [dma((gathers, 10)), dma((gathers, 10)), dma((gathers,))]
        params.update(collective_id=1, has_side_effects=True)
    return pl.pallas_call(
        functools.partial(compute_kernel, images, group, direct),
        out_shape=tuple(out_shape),
        in_specs=[vm] * 4 + [anyspace] * 2 + [vm] * 4 + [anyspace] * len(own),
        out_specs=tuple(out_specs),
        scratch_shapes=scratch,
        compiler_params=pltpu.CompilerParams(**params),
        name="step_compute",
    )(patches, target, pos, mods, w_in, w_out, w_patch, w_head, lbias[:, None, :], tbias, *own)


def place():
    f = lax.axis_index("fsdp")
    r = lax.axis_index("rep")
    z = f // 2
    y = f - 2 * z
    x = r // 2
    c = r - 2 * x
    return z, y, x, c


def device(z, y, x, c):
    return {"fsdp": 2 * z + y, "rep": 2 * x + c}


def greet(peers):
    barrier = pltpu.get_barrier_semaphore()
    for peer in peers:
        pl.semaphore_signal(barrier, inc=1, device_id=peer, device_id_type=pl.DeviceIdType.MESH)
    pl.semaphore_wait(barrier, len(peers))


def remote(source, target, send, recv, peer):
    return pltpu.make_async_remote_copy(
        src_ref=source, dst_ref=target, send_sem=send, recv_sem=recv, device_id=peer, device_id_type=pl.DeviceIdType.MESH
    )


class Reducer:
    def __init__(self, source, bufs, out, sends, recvs, loads):
        self.source = source
        self.keep, self.got0, self.low, self.gotx, self.gotp = bufs
        self.out = out
        self.sends, self.recvs, self.loads = sends, recvs, loads

    def flat(self, ref, half):
        return ref.at[half].reshape(D, ref.shape[-1])

    def load(self, half):
        c = place()[3]
        return pltpu.make_async_copy(self.source.at[2 * half + c], self.flat(self.keep, half), self.loads.at[half])

    def move(self, slot):
        z, y, x, c = place()
        mine = 2 * x + c
        partners = Partners()
        if slot < 2:
            source, target, peer = self.source.at[2 * slot + 1 - c], self.flat(self.got0, slot), partners.c
        elif slot == 2:
            source, target, peer = self.low, self.gotx, partners.x
        elif slot < 10:
            f = lax.axis_index("fsdp")
            to = lax.rem(f + slot - 2, 8)
            source, target, peer = self.low.at[to], self.gotp.at[f], {"fsdp": to}
        else:
            peer = partners.x if slot == 10 else partners.c
            source = target = self.out.at[2 * (1 - x) + c if slot == 12 else mine]
        return remote(source, target, self.sends.at[slot], self.recvs.at[slot], peer)

    def step(self, k):
        z, y, x, c = place()
        f = 2 * z + y
        if k == 0:
            for half in range(2):
                self.load(half).start()
                self.move(half).start()
        if k == 1:
            for half in range(2):
                self.load(half).wait()
                self.move(half).wait()

            @pl.loop(0, 8)
            def _(i):
                self.low[i] = (self.keep[1 - x, i] + self.got0[1 - x, i]).astype(BF16)

            self.move(2).start()

            @pl.loop(0, 8)
            def _(i):
                self.keep[x, i] = self.keep[x, i] + self.got0[x, i]
        if k == 2:
            self.move(2).wait()

            @pl.loop(0, 8)
            def _(i):
                self.low[i] = (self.keep[x, i] + self.gotx[i].astype(F32)).astype(BF16)

            for slot in range(3, 10):
                self.move(slot).start()
            self.keep[x, f] = self.keep[x, f] + self.gotx[f].astype(F32)
        if k == 3:
            for slot in range(3, 10):
                self.move(slot).wait()
            total = self.keep[x, f]
            for d in range(1, 8):
                total = total + self.gotp[lax.rem(f + d, 8)].astype(F32)
            self.out[2 * x + c] = total
            for slot in range(10, 12):
                self.move(slot).start()
        if k == 4:
            self.move(10).wait()
            self.move(12).start()
        if k == 5:
            self.move(11).wait()
            self.move(12).wait()


class Partners:
    def __init__(self):
        z, y, x, c = place()
        self.c = device(z, y, x, 1 - c)
        self.x = device(z, y, 1 - x, c)
        self.y = device(z, 1 - y, x, c)
        self.z1 = device(z + 1 - 2 * lax.rem(z, 2), y, x, c)
        self.z2 = device(lax.rem(z + 2, 4), y, x, c)

    def pairs(self):
        return [self.c, self.x, self.y, self.z1, self.z2]

    def all(self):
        z, y, x, c = place()
        f = 2 * z + y
        return [self.c, self.x, device(z, y, 1 - x, 1 - c)] + [{"fsdp": lax.rem(f + k, 8)} for k in range(1, 8)]


REDUCER_STEPS = 6


def wide_scratch(width):
    return [
        pltpu.VMEM((2, 8, OWN, width), F32),
        pltpu.VMEM((2, 8, OWN, width), F32),
        pltpu.VMEM((8, OWN, width), BF16),
        pltpu.VMEM((8, OWN, width), BF16),
    ]


class Gatherer:
    def __init__(self, source, target, whole, sends, recvs, local):
        self.source, self.target, self.whole = source, target, whole
        self.sends, self.recvs, self.local = sends, recvs, local

    def own(self):
        z, y, x, c = place()
        return pltpu.make_async_copy(self.source(2 * x + c), self.target(2 * z + y, 2 * x + c), self.local)

    def move(self, slot):
        z, y, x, c = place()
        q = 2 * x + c
        if slot < 3:
            source, target, peer = self.source(q), self.target(2 * z + y, q), device(lax.rem(z + 1 + slot, 4), y, x, c)
        elif slot == 3:
            source, target, peer = self.source(q), self.target(2 * z + y, q), device(z, 1 - y, x, c)
        elif slot < 7:
            at = 2 * lax.rem(z + 7 - slot, 4) + y
            source = target = self.target(at, q)
            peer = device(z, 1 - y, x, c)
        else:
            part = 2 * (1 - x) + c if slot == 9 else q
            source = target = self.whole(part)
            peer = device(z, y, 1 - x, c) if slot == 7 else device(z, y, x, 1 - c)
        return remote(source, target, self.sends.at[slot], self.recvs.at[slot], peer)

    def step(self, k):
        if k == 0:
            for slot in range(4):
                self.move(slot).start()
            self.own().start()
        if k == 1:
            for slot in range(3):
                self.move(slot).wait()
                self.move(slot + 4).start()
        if k == 2:
            self.own().wait()
            for slot in range(3, 7):
                self.move(slot).wait()
            self.move(7).start()
            self.move(8).start()
        if k == 3:
            self.move(7).wait()
            self.move(9).start()
        if k == 4:
            self.move(8).wait()
            self.move(9).wait()


GATHER_STEPS = 5


def by_columns(source, target, sends, recvs, local, first=0, width=None):
    rows = source.shape[0]
    width = width or source.shape[1]
    part = width // 4

    def cols(q):
        return pl.ds(pl.multiple_of(first + q * part, 128), part)

    def rows_of(f):
        return pl.ds(pl.multiple_of(f * rows, 16), rows)

    return Gatherer(
        lambda q: source.at[:, cols(q)],
        lambda f, q: target.at[rows_of(f), cols(q)],
        lambda q: target.at[:, cols(q)],
        sends,
        recvs,
        local,
    )


def by_rows(source, target, sends, recvs, local):
    return Gatherer(
        lambda q: source.at[q],
        lambda f, q: target.at[f, q],
        lambda q: target.at[:, q],
        sends,
        recvs,
        local,
    )


def slab(source, target, sends, recvs, local):
    return Gatherer(lambda q: source, lambda f, q: target.at[q, f], lambda q: target.at[q], sends, recvs, local)


class Butterfly:
    def __init__(self, total, got, sends, recvs):
        self.total, self.got, self.sends, self.recvs = total, got, sends, recvs

    def move(self, k):
        partner = Partners().pairs()[k]
        return remote(self.total, self.got.at[k], self.sends.at[k], self.recvs.at[k], partner)

    def step(self, k):
        if k > 0:
            self.move(k - 1).wait()
            self.total[...] = self.total[...] + self.got[k - 1]
        if k < 5:
            self.move(k).start()


BUTTERFLY_STEPS = 6


C_T1, C_T2, C_PATCH, C_HEAD, C_ALL = 1024, 1280, 1664, 1792, 2048
SLOTS = 256


def silu_slope(x):
    gate = 1.0 / (1.0 + jnp.exp(-x))
    return gate * (1.0 + x * (1.0 - gate))


def silu(x):
    return x / (1.0 + jnp.exp(-x))


def prologue_kernel(
    kinds,
    images,
    small_ref,
    feat_ref,
    w_mods_ref,
    lbias_ref,
    tbias_ref,
    own_in_ref,
    own_out_ref,
    w_patch_ref,
    w_head_ref,
    time2_ref,
    w_in_ref,
    w_out_ref,
    mods_ref,
    time1_ref,
    s1_ref,
    before_ref,
    cond_ref,
    feats_ref,
    full,
    part,
    got,
    cond_rows,
    wide,
    sends,
    recvs,
    local,
    p_sends,
    p_recvs,
    p_local,
):
    z, y, x, c = place()
    f = 2 * z + y
    r = 2 * x + c

    def sems(n):
        return sends.at[n], recvs.at[n], local.at[n]

    feats = slab(feat_ref, feats_ref, *sems(0))
    small = by_columns(small_ref, full, *sems(1))
    own_in, own_out = own_in_ref.at[0], own_out_ref.at[0]
    attention = by_columns(own_in, w_in_ref, *sems(2), 0, 4 * D)
    inner = by_columns(own_in, w_in_ref, *sems(3), 4 * D, FF)
    outer = by_rows(own_out, w_out_ref, *sems(4))
    plans = [
        (0, GATHER_STEPS, feats),
        (0, GATHER_STEPS, small),
        (2, GATHER_STEPS, attention),
        (3, GATHER_STEPS, inner),
        (4, GATHER_STEPS, outer),
    ]
    partners = Partners()
    greet(partners.all())
    last = max(first + count for first, count, _ in plans)
    copies = []
    for tick in range(last):
        for first, count, piece in plans:
            if 0 <= tick - first < count:
                piece.step(tick - first)
        if tick != GATHER_STEPS - 1:
            continue
        rows = feats_ref[...].reshape(SLOTS, feats_ref.shape[-1])
        feat = rows[:, :FREQ].astype(BF16)
        label = rows[:, FREQ : FREQ + 1]
        place_of = lax.broadcasted_iota(jnp.int32, (SLOTS, C_T1), 1).astype(F32)
        picked = jnp.where(label == place_of, 1.0, 0.0).astype(BF16)
        time1 = dot(feat, full[:, C_T1:C_T2], NT) + tbias_ref[:, D : 2 * D]
        s1 = silu(time1).astype(BF16)
        before = dot(s1, full[:, C_T2 : C_T2 + D]) + tbias_ref[:, 2 * D : 3 * D] + dot(picked, full[:, :C_T1], NT)
        cond = silu(before)
        cond_rows[...] = cond
        pick = lax.broadcasted_iota(jnp.int32, (D, OWN), 0) == f * OWN + lax.broadcasted_iota(jnp.int32, (D, OWN), 1)
        group = cond_rows[pl.ds(pl.multiple_of(r * 64, 64), 64), :].astype(BF16)
        group = dot(group, jnp.where(pick, 1.0, 0.0).astype(BF16)).astype(BF16)
        for k in range(kinds):
            mods = dot(group, w_mods_ref[:, k * D : (k + 1) * D])
            for n in range(8):
                part[n, k * images : (k + 1) * images, :] = mods[8 * n : 8 * n + images]
        for k in range(1, 8):
            to = lax.rem(f + k, 8)
            copies.append(remote(part.at[to], got.at[f], p_sends.at[k - 1], p_recvs.at[k - 1], {"fsdp": to}))
            copies[-1].start()
        own = pltpu.make_async_copy(part.at[f], got.at[f], p_local)
        own.start()
        mine = pl.ds(pl.multiple_of(f * OWN, OWN), OWN)
        time1_ref[...] = time1.T
        wide[...] = s1.astype(F32).T
        s1_ref[...] = wide[mine, :].astype(BF16)
        wide[...] = before.T
        before_ref[...] = wide[mine, :]
        wide[...] = cond.T
        cond_ref[...] = wide[mine, :].astype(BF16)
        w_patch_ref[...] = full[:, C_PATCH : C_PATCH + PATCH_IN]
        w_head_ref[...] = full[:, C_HEAD : C_HEAD + PATCH_IN]
        time2_ref[...] = full[:, C_T2 : C_T2 + D]
        mods_ref[...] = jnp.zeros_like(mods_ref)
    own.wait()
    for copy in copies:
        copy.wait()
    depth = (kinds - 2) // 6
    for k in range(kinds):
        at = slice(k * images, (k + 1) * images)
        total = got[0, at]
        for n in range(1, 8):
            total = total + got[n, at]
        if k < 6 * depth:
            bias = lbias_ref[k // 6 : k // 6 + 1, k % 6 * D : k % 6 * D + D]
        else:
            first = 3 * D + (k - 6 * depth) * D
            bias = tbias_ref[:, first : first + D]
        mods_ref[k, 0:images] = total + bias


def prologue(small, feat, w_mods, lbias, tbias, own_in, own_out, images):
    kinds = w_mods.shape[1] // D
    shape = jax.ShapeDtypeStruct
    anyspace = pl.BlockSpec(memory_space=pl.ANY)
    vm = pl.BlockSpec(memory_space=pltpu.VMEM)
    dma = pltpu.SemaphoreType.DMA
    rows = -(-kinds * images // 8) * 8
    return pl.pallas_call(
        functools.partial(prologue_kernel, kinds, images),
        out_shape=(
            shape((D, PATCH_IN), BF16),
            shape((D, PATCH_IN), BF16),
            shape((D, D), BF16),
            shape((D, own_in.shape[2]), BF16),
            shape((8, 4, OWN, D), BF16),
            shape((16, 8, D), F32),
            shape((D, SLOTS), F32),
            shape((OWN, SLOTS), BF16),
            shape((OWN, SLOTS), F32),
            shape((OWN, SLOTS), BF16),
            shape((4, 8) + feat.shape, F32),
        ),
        in_specs=[anyspace, vm, vm, vm, vm, anyspace, anyspace],
        out_specs=(vm, vm, vm, anyspace, anyspace) + (vm,) * 6,
        scratch_shapes=[
            pltpu.VMEM((D, C_ALL), BF16),
            pltpu.VMEM((8, rows, D), F32),
            pltpu.VMEM((8, rows, D), F32),
            pltpu.VMEM((SLOTS, D), F32),
            pltpu.VMEM((D, SLOTS), F32),
            dma((5, 10)),
            dma((5, 10)),
            dma((5,)),
            dma((7,)),
            dma((7,)),
            dma,
        ],
        compiler_params=pltpu.CompilerParams(collective_id=2, has_side_effects=True, vmem_limit_bytes=60 * 1024 * 1024),
        name="step_prologue",
    )(small, feat, w_mods, lbias, tbias, own_in, own_out)


E_PATCH, E_T1, E_T2, E_FIN, E_HEAD, E_ALL = 1024, 1152, 1408, 1792, 2560, 2688
STAT = 1792


def column_of(row):
    n = row.shape[1]
    same = lax.broadcasted_iota(jnp.int32, (n, n), 0) == lax.broadcasted_iota(jnp.int32, (n, n), 1)
    return jnp.sum(jnp.where(same, row, 0.0), axis=1, keepdims=True)


def row_of(column):
    n = column.shape[0]
    same = lax.broadcasted_iota(jnp.int32, (n, n), 0) == lax.broadcasted_iota(jnp.int32, (n, n), 1)
    return jnp.sum(jnp.where(same, column, 0.0), axis=0, keepdims=True)


def total_of(v):
    return jnp.sum(rows_sum(v), axis=1, keepdims=True)


def update_kernel(
    sizes,
    out_t_ref,
    out_m_ref,
    sums_ref,
    d_mods_ref,
    cond_ref,
    before_ref,
    time1_ref,
    s1_ref,
    feats_ref,
    time2_ref,
    w_mods_ref,
    in_ref,
    down_ref,
    edge_ref,
    lbias_ref,
    tbias_ref,
    in_rows_ref,
    in_cols_ref,
    down_rows_ref,
    down_cols_ref,
    edge_rows_ref,
    edge_cols_ref,
    lbias_v_ref,
    tbias_v_ref,
    in_new,
    down_new,
    edge_new,
    lbias_new,
    tbias_new,
    in_rows_new,
    in_cols_new,
    down_rows_new,
    down_cols_new,
    edge_rows_new,
    edge_cols_new,
    lbias_v_new,
    tbias_v_new,
    tail_ref,
    g_in,
    g_down,
    g_edge,
    d_time2,
    d_time1,
    small_t,
    stats,
    squares,
    sends,
    recvs,
):
    classes, tokens = sizes
    depth = in_ref.shape[0]
    kinds = w_mods_ref.shape[1] // D
    fin = 6 * depth
    f = lax.axis_index("fsdp")
    others = [{"fsdp": lax.rem(f + k, 8)} for k in range(1, 8)]
    scale = 1.0 / (PATCH_IN * math.sqrt(tokens))
    mine = pl.ds(pl.multiple_of(f * OWN, OWN), OWN)
    greet(others)

    def share(n, buffer):
        copies = []
        for k in range(1, 8):
            copies.append(remote(buffer.at[f], buffer.at[f], sends.at[n, k - 1], recvs.at[n, k - 1], others[k - 1]))
            copies[-1].start()
        return copies

    d_cond = jnp.zeros((OWN, SLOTS), F32)
    ones = jnp.ones((8, SLOTS), BF16)
    for k in range(kinds):
        rows = d_mods_ref[:, :, k].astype(F32).reshape(SLOTS, D).astype(BF16)
        g = dot(cond_ref[...], rows) * scale
        b = dot(ones, rows)[0:1] * scale
        if k < fin:
            layer, at = k // 6, (k % 6) * D
            g_in[layer, :, at : at + D] = g
            lbias_new[layer : layer + 1, at : at + D] = b
        else:
            at = (k - fin) * D
            g_edge[:, E_FIN + at : E_FIN + at + D] = g
            tbias_new[:, 3 * D + at : 3 * D + at + D] = b
        d_cond = d_cond + dot(w_mods_ref[:, k * D : (k + 1) * D], rows, NT)
    d_before = d_cond * silu_slope(before_ref[...])
    d_time2[f] = d_before.astype(BF16)
    copies = share(0, d_time2)
    rows = feats_ref[...].reshape(SLOTS, feats_ref.shape[-1])
    feat = rows[:, :FREQ].astype(BF16)
    label = rows[:, FREQ : FREQ + 1]
    picked = jnp.where(label == lax.broadcasted_iota(jnp.int32, (SLOTS, E_PATCH), 1).astype(F32), 1.0, 0.0).astype(BF16)
    top = d_before.astype(BF16)
    left = d_before - top.astype(F32)
    middle = left.astype(BF16)
    low = (left - middle.astype(F32)).astype(BF16)
    g_edge[:, 0:E_PATCH] = (dot(top, picked) + dot(middle, picked) + dot(low, picked)) * scale
    small_t[:, 0 : 2 * PATCH_IN] = sums_ref[0 : 2 * PATCH_IN, :].T * scale
    own_small = small_t[mine, :]
    lane = lax.broadcasted_iota(jnp.int32, (OWN, 128), 1)
    g_edge[:, E_PATCH:E_T1] = jnp.where(lane < PATCH_IN, own_small, 0.0)
    g_edge[:, E_HEAD:E_ALL] = jnp.where(lane < PATCH_IN, pltpu.roll(own_small, 128 - PATCH_IN, 1), 0.0)
    for layer in range(depth):
        for q in range(4):
            g_in[layer, :, 6 * D + q * D : 7 * D + q * D] = out_t_ref[layer, q] * scale
            g_in[layer, :, 10 * D + q * D : 11 * D + q * D] = out_m_ref[layer, q, :, 0:D] * scale
            g_down[layer, q * OWN : (q + 1) * OWN, :] = out_m_ref[layer, q, :, D : 2 * D] * scale
    for copy in copies:
        copy.wait()
    d2 = d_time2[...].reshape(D, SLOTS)
    g_edge[:, E_T2:E_FIN] = dot(s1_ref[...], d2, NT) * scale
    d1 = (dot(time2_ref[...], d2) * silu_slope(time1_ref[...])).astype(BF16)
    d_time1[...] = d1
    g_edge[:, E_T1:E_T2] = dot(d_time1[mine, :], feat) * scale
    tbias_new[:, D : 2 * D] = dot(ones, d1, NT)[0:1] * scale
    tbias_new[:, 2 * D : 3 * D] = dot(ones, d2, NT)[0:1] * scale
    tbias_new[:, 0:D] = sums_ref[S_BPATCH : S_BPATCH + 1, :] * scale
    lane = lax.broadcasted_iota(jnp.int32, (1, 2 * PATCH_IN), 1)
    tbias_new[:, 5 * D :] = jnp.where(lane < PATCH_IN, sums_ref[S_BHEAD : S_BHEAD + 1, 0 : 2 * PATCH_IN], 0.0) * scale
    for layer in range(depth):
        for j in range(8):
            row = S_BIAS + 8 * layer + j
            lbias_new[layer : layer + 1, 6 * D + j * D : 7 * D + j * D] = sums_ref[row : row + 1, :] * scale

    wide = in_ref.shape[2]
    rows_in, rows_down = [], []
    for layer in range(depth):
        s = jnp.zeros((OWN, 1), F32)
        for t in range(wide // STAT):
            g = g_in[layer, :, t * STAT : (t + 1) * STAT]
            g2 = g * g
            s = s + jnp.sum(g2, axis=1, keepdims=True)
            stats[f, wide // STAT * layer + t : wide // STAT * layer + t + 1, :] = rows_sum(g2)
        new = decay * column_of(in_rows_ref[layer : layer + 1, :]) + (1.0 - decay) * (s / wide + eps_stat)
        rows_in.append(new)
        in_rows_new[layer : layer + 1, :] = row_of(new)
        g = g_down[layer]
        g2 = g * g
        new = decay * column_of(down_rows_ref[layer : layer + 1, :]) + (1.0 - decay) * (
            jnp.sum(g2, axis=1, keepdims=True) / D + eps_stat
        )
        rows_down.append(new)
        down_rows_new[layer : layer + 1, :] = row_of(new)
        stats[f, 7:8, E_ALL - STAT + layer * D : E_ALL - STAT + (layer + 1) * D] = rows_sum(g2)
    g = g_edge[...]
    g2 = g * g
    rows_edge = decay * column_of(edge_rows_ref[...]) + (1.0 - decay) * (
        jnp.sum(g2, axis=1, keepdims=True) / classes + eps_stat
    )
    edge_rows_new[...] = row_of(rows_edge)
    g2 = rows_sum(g2)
    stats[f, 6:7, :] = g2[:, 0:STAT]
    stats[f, 7:8, 0 : E_ALL - STAT] = g2[:, STAT:E_ALL]
    lane = lax.broadcasted_iota(jnp.int32, (1, 128), 1)
    totals = jnp.zeros((1, 128), F32)
    every = rows_in + rows_down + [rows_edge]
    for n, v in enumerate(every):
        totals = jnp.where(lane == n, rows_sum(v), totals)
    spot = E_ALL - STAT + depth * D
    stats[f, 7:8, spot : spot + 128] = totals
    copies = share(1, stats)

    def plain_rows(weight, new, old_v, new_v, columns):
        g = new[...]
        moment = decay * old_v[...] + (1.0 - decay) * (g * g + eps_stat)
        u = g * lax.rsqrt(moment)
        root = jnp.sqrt(jnp.sum(u * u, axis=1, keepdims=True) / columns)
        new_v[...] = moment
        new[...] = weight[...] - rate * u / jnp.maximum(1.0, root / clip_level)

    plain_rows(lbias_ref, lbias_new, lbias_v_ref, lbias_v_new, wide)
    plain_rows(tbias_ref, tbias_new, tbias_v_ref, tbias_v_new, 5 * D + 2 * PATCH_IN)
    loss = jnp.sum(sums_ref[S_SSE : S_SSE + 1, 0:PATCH_IN], axis=1, keepdims=True) / (tokens * PATCH_IN)

    for copy in copies:
        copy.wait()
    full = stats[0]
    for k in range(1, 8):
        full = full + stats[k]
    height = 8.0 * OWN
    tall = 4.0 * height

    def factors(rows_col, total, count, cols):
        return lax.rsqrt(rows_col / (total / count)), lax.rsqrt(cols)

    squared = jnp.zeros((1, 128), F32)
    used = []
    for layer in range(depth):
        total = full[7:8, spot + layer : spot + layer + 1]
        s = jnp.zeros((1, 1), F32)
        for t in range(wide // STAT):
            at = slice(t * STAT, (t + 1) * STAT)
            line = wide // STAT * layer + t
            cols = decay * in_cols_ref[layer : layer + 1, at] + (1.0 - decay) * (full[line : line + 1, :] / height + eps_stat)
            in_cols_new[layer : layer + 1, at] = cols
            a, b = factors(rows_in[layer], total, height, cols)
            u = g_in[layer, :, at] * a * b
            g_in[layer, :, at] = u
            s = s + total_of(u * u)
        squared = jnp.where(lane == layer, s, squared)
        at = E_ALL - STAT + layer * D
        cols = decay * down_cols_ref[layer : layer + 1, :] + (1.0 - decay) * (full[7:8, at : at + D] / tall + eps_stat)
        down_cols_new[layer : layer + 1, :] = cols
        total = full[7:8, spot + depth + layer : spot + depth + layer + 1]
        a, b = factors(rows_down[layer], total, tall, cols)
        u = g_down[layer] * a * b
        g_down[layer] = u
        squared = jnp.where(lane == depth + layer, total_of(u * u), squared)
    cols = jnp.concatenate([full[6:7, :], full[7:8, 0 : E_ALL - STAT]], axis=1)
    cols = decay * edge_cols_ref[...] + (1.0 - decay) * (cols / height + eps_stat)
    edge_cols_new[...] = cols
    a, b = factors(rows_edge, full[7:8, spot + 2 * depth : spot + 2 * depth + 1], height, cols)
    u = g_edge[...] * a * b
    g_edge[...] = u
    squared = jnp.where(lane == 2 * depth, total_of(u * u), squared)
    squares[f] = jnp.broadcast_to(squared, (8, 128))
    for copy in share(2, squares):
        copy.wait()
    full = squares[0]
    for k in range(1, 8):
        full = full + squares[k]
    full = full[0:1, :]
    counts = jnp.where(lane < depth, height * wide, jnp.where(lane < 2 * depth, tall * D, height * classes))
    roots = jnp.sqrt(full / counts)
    step = rate / jnp.maximum(1.0, roots / clip_level)
    tail_ref[...] = jnp.where(lane == 2 * depth + 1, loss, roots)
    for layer in range(depth):
        in_new[layer] = in_ref[layer] - step[:, layer : layer + 1] * g_in[layer]
        down_new[layer] = down_ref[layer] - step[:, depth + layer : depth + layer + 1] * g_down[layer]
    edge_new[...] = edge_ref[...] - step[:, 2 * depth : 2 * depth + 1] * g_edge[...]


def update(sizes, out_t, out_m, sums, d_mods, cond, before, time1, s1, feats, time2, w_mods, weights, stats):
    shape = jax.ShapeDtypeStruct
    vm = pl.BlockSpec(memory_space=pltpu.VMEM)
    dma = pltpu.SemaphoreType.DMA
    inputs = (out_t, out_m, sums, d_mods, cond, before, time1, s1, feats, time2, w_mods) + weights + stats
    outs = tuple(shape(v.shape, F32) for v in weights + stats) + (shape((1, 128), F32),)
    return pl.pallas_call(
        functools.partial(update_kernel, sizes),
        out_shape=outs,
        in_specs=[vm] * len(inputs),
        out_specs=(vm,) * len(outs),
        scratch_shapes=[
            pltpu.VMEM(weights[0].shape, F32),
            pltpu.VMEM(weights[1].shape, F32),
            pltpu.VMEM(weights[2].shape, F32),
            pltpu.VMEM((8, OWN, SLOTS), BF16),
            pltpu.VMEM((D, SLOTS), BF16),
            pltpu.VMEM((D, 128), F32),
            pltpu.VMEM((8, 8, STAT), F32),
            pltpu.VMEM((8, 8, 128), F32),
            dma((3, 7)),
            dma((3, 7)),
        ],
        compiler_params=pltpu.CompilerParams(collective_id=3, has_side_effects=True, vmem_limit_bytes=60 * 1024 * 1024),
        name="step_update",
    )(*inputs)


def mix_weights(tsteps):
    betas = 0.0001 + (0.02 - 0.0001) * jnp.arange(TSTEPS, dtype=jnp.float32) / (TSTEPS - 1)
    alpha_bar = jnp.exp(jnp.cumsum(jnp.log(1.0 - betas)))
    picked = jnp.arange(TSTEPS)[None, :] == tsteps[:, None]
    return jnp.sum(jnp.where(picked, alpha_bar[None, :], 0.0), axis=1)


def patchify(latent_rows):
    images = latent_rows.shape[0]
    grid_side = GRID // PATCH
    shaped = latent_rows.reshape(images, CHANNELS, grid_side, PATCH, grid_side, PATCH)
    shaped = jnp.transpose(shaped, (0, 2, 4, 1, 3, 5))
    return shaped.reshape(images, grid_side * grid_side, CHANNELS * PATCH * PATCH)


def position_table():
    side = GRID // PATCH
    quarter = D // 4
    omegas = 1.0 / 10000.0 ** (np.arange(quarter) / quarter)
    places = np.arange(side * side)

    def one_axis(coords):
        angles = coords[:, None] * omegas[None, :]
        return np.concatenate([np.sin(angles), np.cos(angles)], axis=1)

    return np.concatenate([one_axis(places % side), one_axis(places // side)], axis=1).astype(np.float32)


def time_features(tsteps):
    half_freq = FREQ // 2
    frequencies = jnp.exp(-math.log(10000.0) * jnp.arange(half_freq, dtype=jnp.float32) / half_freq)
    angles = tsteps.astype(jnp.float32)[:, None] * frequencies[None, :]
    return jnp.concatenate([jnp.cos(angles), jnp.sin(angles)], axis=1)


def fetch(layer_in, layer_out):
    own_in = layer_in[:, :, 6 * D :].astype(BF16)
    own_out = layer_out.astype(BF16)
    w_in = lax.all_gather(own_in, "fsdp", axis=1, tiled=True)
    w_out = lax.all_gather(own_out, "fsdp", axis=1, tiled=True)
    return w_in, w_out


def matmul(a, b, form):
    return jnp.einsum(form, a, b, preferred_element_type=F32)


def step_of(grad, rows_new, cols_new, rows_mean):
    second = rows_new[:, :, None] * cols_new[:, None, :] / rows_mean[:, None, None]
    return grad * lax.rsqrt(second)


def plain(weight, grad, moment):
    moment_new = decay * moment + (1.0 - decay) * (grad * grad + eps_stat)
    update = grad * lax.rsqrt(moment_new)
    root = jnp.sqrt(jnp.mean(update * update, axis=-1, keepdims=True))
    return (weight - rate * update / jnp.maximum(1.0, root / clip_level), moment_new)


def library_step(
    latents,
    tsteps,
    labels,
    noise,
    layer_in,
    layer_out,
    edge_mat,
    layer_bias,
    top_bias,
    in_rows,
    in_cols,
    out_rows,
    out_cols,
    edge_rows,
    edge_cols,
    layer_bias_v,
    top_bias_v,
):
    images = latents.shape[0]
    depth, own, wide = layer_in.shape
    fsdp = lax.axis_size("fsdp")
    rep = lax.axis_size("rep")
    at_f = lax.axis_index("fsdp")
    at_r = lax.axis_index("rep")
    every = images * fsdp * rep
    width = own * fsdp
    MOD = 6 * D
    start_freq = NCLS + PATCH_IN
    start_tail = start_freq + FREQ

    edge_low = edge_mat.astype(BF16)
    small = jnp.concatenate([edge_low[:, : start_tail + D], edge_low[:, start_tail + 3 * D :]], axis=1)
    full = lax.all_gather(small, "fsdp", axis=0, tiled=True)
    class_cols = full[:, :NCLS]
    patch_cols = full[:, NCLS:start_freq]
    freq_cols = full[:, start_freq:start_tail]
    time_second = full[:, start_tail : start_tail + D]
    head_cols = full[:, start_tail + D : start_tail + D + PATCH_IN]
    all_tsteps, all_labels = (
        lax.all_gather(tsteps, ("fsdp", "rep"), axis=0, tiled=True),
        lax.all_gather(labels, ("fsdp", "rep"), axis=0, tiled=True),
    )
    features = time_features(all_tsteps).astype(BF16)
    time1 = matmul(features, freq_cols, "bf,df->bd") + top_bias[D : 2 * D]
    s1 = jax.nn.silu(time1).astype(BF16)
    picked = (all_labels[:, None] == jnp.arange(NCLS)[None, :]).astype(BF16)
    before = matmul(s1, time_second, "bd,de->be") + top_bias[2 * D : 3 * D] + matmul(picked, class_cols, "bc,dc->bd")
    cond = jax.nn.silu(before).astype(BF16)

    def own_part(values):
        return lax.dynamic_slice_in_dim(values, at_f * own, own, axis=1)

    low_in = layer_in.astype(BF16)
    w_mods = jnp.concatenate(
        [low_in[layer, :, :MOD] for layer in range(depth)] + [edge_low[:, start_tail + D : start_tail + 3 * D]], axis=1
    )
    cond_own = own_part(cond)
    group_own = lax.dynamic_index_in_dim(cond_own.reshape(fsdp, rep, images, own), at_r, axis=1, keepdims=False)
    part = matmul(group_own.reshape(fsdp * images, own), w_mods, "bd,de->be")
    bias_mods = jnp.concatenate([layer_bias[layer, :MOD] for layer in range(depth)] + [top_bias[3 * D : 5 * D]])
    mods = lax.psum_scatter(part, "fsdp", scatter_dimension=0, tiled=True) + bias_mods
    kinds = 6 * depth + 2
    mods = mods.reshape(images, kinds, D)

    alphas = mix_weights(tsteps)
    noisy = jnp.sqrt(alphas)[:, None, None] * latents + jnp.sqrt(1.0 - alphas)[:, None, None] * noise
    patches = patchify(noisy).astype(BF16).reshape(images * TOK, PATCH_IN)
    target = patchify(noise).reshape(images * TOK, PATCH_IN)

    w_in, w_out = fetch(layer_in, layer_out)
    g_in, g_out, sums, d_mods = compute(
        patches,
        target,
        jnp.asarray(position_table()),
        jnp.transpose(jnp.pad(mods, ((0, 8 - images), (0, 16 - kinds), (0, 0))), (1, 0, 2)),
        w_in,
        w_out.reshape(depth, FF // FFC, FFC, D),
        patch_cols,
        head_cols,
        layer_bias,
        top_bias[None],
    )

    d_mods = jnp.transpose(d_mods, (1, 0, 2))[:images, :kinds].reshape(images, kinds * D)
    d_mods = lax.all_gather(d_mods, ("fsdp", "rep"), axis=0, tiled=True)
    g_rows = matmul(cond_own, d_mods, "bd,be->de")
    g_bmods = jnp.sum(d_mods.astype(F32), axis=0)
    d_before = matmul(d_mods, w_mods, "be,de->bd") * silu_slope(own_part(before))
    g_class = jnp.einsum("bd,bc->dc", d_before, picked.astype(F32), precision=lax.Precision.HIGHEST)
    d_time2 = lax.all_gather(d_before.astype(BF16), "fsdp", axis=1, tiled=True)
    g_time2 = matmul(own_part(s1), d_time2, "bd,be->de")
    d_time1 = (matmul(d_time2, time_second, "be,de->bd") * silu_slope(time1)).astype(BF16)
    g_time1 = matmul(own_part(d_time1), features, "bd,bf->df")

    shard_in = lax.psum(lax.psum_scatter(g_in, "fsdp", scatter_dimension=1, tiled=True), "rep")
    shard_out = lax.psum(lax.psum_scatter(g_out, "fsdp", scatter_dimension=1, tiled=True), "rep")
    sums = lax.psum(sums, ("fsdp", "rep")).reshape(S_ROWS, D)
    g_patch, g_head = sums[:S_HEAD], sums[S_HEAD:S_BIAS]
    g_bias = sums[S_BIAS:S_BPATCH].reshape(depth, BW)
    g_bpatch, g_bhead = sums[S_BPATCH : S_BPATCH + 1], sums[S_BHEAD : S_BHEAD + 1, :PATCH_IN]
    sse = jnp.sum(sums[S_SSE, :PATCH_IN])

    tok_total = every * TOK
    scale_grad = 1.0 / (PATCH_IN * math.sqrt(tok_total))
    loss = sse / (tok_total * PATCH_IN)
    fin = depth * MOD
    grad_edge = jnp.concatenate(
        [
            g_class,
            own_part(g_patch).T,
            g_time1,
            g_time2,
            g_rows[:, fin:],
            own_part(g_head).T,
            jnp.zeros((own, PATCH_IN), F32),
        ],
        axis=1,
    )[None] * scale_grad
    grad_in = jnp.concatenate([jnp.stack([g_rows[:, layer * MOD : (layer + 1) * MOD] for layer in range(depth)]), shard_in], axis=2) * scale_grad
    grad_out = shard_out * scale_grad
    grad_lbias = jnp.concatenate([g_bmods[:fin].reshape(depth, MOD), g_bias], axis=1) * scale_grad
    grad_tbias = jnp.concatenate(
        [
            g_bpatch[0],
            jnp.sum(d_time1.astype(F32), axis=0),
            jnp.sum(d_time2.astype(F32), axis=0),
            g_bmods[fin:],
            g_bhead[0],
            jnp.zeros((PATCH_IN,), F32),
        ]
    ) * scale_grad

    full_rows_in = width
    full_rows_out = layer_out.shape[1] * fsdp
    full_rows_edge = edge_mat.shape[0] * fsdp
    square_in = grad_in * grad_in + eps_stat
    square_out = grad_out * grad_out + eps_stat
    square_edge = grad_edge * grad_edge + eps_stat
    rows_in_new = decay * in_rows + (1.0 - decay) * jnp.mean(square_in, axis=2)
    rows_out_new = decay * out_rows + (1.0 - decay) * jnp.mean(square_out, axis=2)
    rows_edge_new = decay * edge_rows[None] + (1.0 - decay) * jnp.mean(square_edge, axis=2)
    col_in, total_in, col_out, total_out, col_edge, total_edge = lax.psum(
        (
            jnp.sum(square_in, axis=1),
            jnp.sum(rows_in_new, axis=1),
            jnp.sum(square_out, axis=1),
            jnp.sum(rows_out_new, axis=1),
            jnp.sum(square_edge, axis=1),
            jnp.sum(rows_edge_new, axis=1),
        ),
        "fsdp",
    )
    cols_in_new = decay * in_cols + (1.0 - decay) * col_in / full_rows_in
    cols_out_new = decay * out_cols + (1.0 - decay) * col_out / full_rows_out
    cols_edge_new = decay * edge_cols[None] + (1.0 - decay) * col_edge / full_rows_edge
    update_in = step_of(grad_in, rows_in_new, cols_in_new, total_in / full_rows_in)
    update_out = step_of(grad_out, rows_out_new, cols_out_new, total_out / full_rows_out)
    update_edge = step_of(grad_edge, rows_edge_new, cols_edge_new, total_edge / full_rows_edge)
    sum_in, sum_out, sum_edge = lax.psum(
        (
            jnp.sum(update_in * update_in, axis=(1, 2)),
            jnp.sum(update_out * update_out, axis=(1, 2)),
            jnp.sum(update_edge * update_edge, axis=(1, 2)),
        ),
        "fsdp",
    )
    roots_in = jnp.sqrt(sum_in / (full_rows_in * grad_in.shape[2]))
    roots_out = jnp.sqrt(sum_out / (full_rows_out * grad_out.shape[2]))
    roots_edge = jnp.sqrt(sum_edge / (full_rows_edge * grad_edge.shape[2]))
    factor_in = jnp.maximum(1.0, roots_in / clip_level)[:, None, None]
    factor_out = jnp.maximum(1.0, roots_out / clip_level)[:, None, None]
    factor_edge = jnp.maximum(1.0, roots_edge / clip_level)[:, None, None]
    in_new = layer_in - rate * update_in / factor_in
    out_new = layer_out - rate * update_out / factor_out
    edge_new = (edge_mat[None] - rate * update_edge / factor_edge)[0]
    clip_roots = jnp.concatenate([roots_in, roots_out, roots_edge])
    lbias_new, lbias_v_new = plain(layer_bias, grad_lbias, layer_bias_v)
    tbias_new, tbias_v_new = plain(top_bias, grad_tbias, top_bias_v)
    return (
        loss,
        in_new,
        out_new,
        edge_new,
        lbias_new,
        tbias_new,
        rows_in_new,
        cols_in_new,
        rows_out_new,
        cols_out_new,
        rows_edge_new[0],
        cols_edge_new[0],
        lbias_v_new,
        tbias_v_new,
        clip_roots,
    )


def direct_step(
    latents,
    tsteps,
    labels,
    noise,
    layer_in,
    layer_out,
    edge_mat,
    layer_bias,
    top_bias,
    in_rows,
    in_cols,
    out_rows,
    out_cols,
    edge_rows,
    edge_cols,
    layer_bias_v,
    top_bias_v,
):
    images = latents.shape[0]
    depth = layer_in.shape[0]
    MOD = 6 * D
    tokens = images * 32 * TOK
    classes = edge_mat.shape[1]
    start_freq = NCLS + PATCH_IN
    start_tail = start_freq + FREQ

    def wide_to(v, width, fill=0.0):
        return jnp.pad(v, ((0, 0), (0, width - v.shape[1])), constant_values=fill)

    def aligned(v, fill):
        return jnp.concatenate(
            [
                wide_to(v[:, :NCLS], E_PATCH, fill),
                wide_to(v[:, NCLS:start_freq], E_T1 - E_PATCH, fill),
                v[:, start_freq : start_tail + 3 * D],
                wide_to(v[:, start_tail + 3 * D :], E_ALL - E_HEAD, fill),
            ],
            axis=1,
        )

    edge_a = aligned(edge_mat, 0.0)
    edge_low = edge_a.astype(BF16)
    small = jnp.concatenate(
        [
            edge_low[:, :E_PATCH],
            edge_low[:, E_T1:E_FIN],
            edge_low[:, E_PATCH:E_T1],
            edge_low[:, E_HEAD:E_ALL],
            jnp.zeros((OWN, C_ALL - C_HEAD - (E_ALL - E_HEAD)), BF16),
        ],
        axis=1,
    )
    w_mods = jnp.concatenate([layer_in[layer, :, :MOD].astype(BF16) for layer in range(depth)] + [edge_low[:, E_FIN:E_HEAD]], axis=1)
    feat = jnp.concatenate(
        [time_features(tsteps), jnp.broadcast_to(labels.astype(F32)[:, None], (images, 128))], axis=1
    )
    feat = jnp.pad(feat, ((0, 8 - images), (0, 0)))
    tbias = top_bias[None]
    own = (layer_in[:, :, MOD:].astype(BF16), layer_out.astype(BF16).reshape(depth, 4, OWN, D))
    w_patch, w_head, time2, w_in, w_out, mods, time1, s1, before, cond, feats = prologue(
        small, feat, w_mods, layer_bias, tbias, *own, images
    )

    alphas = mix_weights(tsteps)
    noisy = jnp.sqrt(alphas)[:, None, None] * latents + jnp.sqrt(1.0 - alphas)[:, None, None] * noise
    patches = patchify(noisy).astype(BF16).reshape(images * TOK, PATCH_IN)
    target = patchify(noise).reshape(images * TOK, PATCH_IN)
    _, _, sums, _, out_t, out_m, d_mods = compute(
        patches, target, jnp.asarray(position_table()), mods, w_in, w_out, w_patch, w_head, layer_bias, tbias, own
    )
    weights = (layer_in, layer_out, edge_a, layer_bias, tbias)
    stats = (
        in_rows,
        in_cols,
        out_rows,
        out_cols,
        edge_rows[None],
        aligned(edge_cols[None], 1.0),
        layer_bias_v,
        top_bias_v[None],
    )
    (
        in_new,
        out_new,
        edge_new,
        lbias_new,
        tbias_new,
        in_rows_new,
        in_cols_new,
        out_rows_new,
        out_cols_new,
        edge_rows_new,
        edge_cols_new,
        lbias_v_new,
        tbias_v_new,
        tail,
    ) = update(
        (classes, tokens), out_t, out_m, sums.reshape(S_ROWS, D), d_mods, cond, before, time1, s1, feats, time2, w_mods, weights, stats
    )

    def natural(v):
        return jnp.concatenate(
            [v[:, :NCLS], v[:, E_PATCH : E_PATCH + PATCH_IN], v[:, E_T1 : E_HEAD + 2 * PATCH_IN]], axis=1
        )

    return (
        tail[0, 2 * depth + 1],
        in_new,
        out_new,
        natural(edge_new),
        lbias_new,
        tbias_new[0],
        in_rows_new,
        in_cols_new,
        out_rows_new,
        out_cols_new,
        edge_rows_new[0],
        natural(edge_cols_new)[0],
        lbias_v_new,
        tbias_v_new[0],
        tail[0, : 2 * depth + 1],
    )


def shards(*arrays):
    layer_in = arrays[4]
    mesh = (lax.axis_size("fsdp"), lax.axis_size("rep"), layer_in.shape[0], layer_in.shape[1])
    return (direct_step if mesh == (8, 4, 2, OWN) else library_step)(*arrays)


def solution(mesh):
    placed = (
        P(("fsdp", "rep"), None, None),
        P(("fsdp", "rep")),
        P(("fsdp", "rep")),
        P(("fsdp", "rep"), None, None),
        P(None, "fsdp", None),
        P(None, "fsdp", None),
        P("fsdp", None),
        P(),
        P(),
        P(None, "fsdp"),
        P(),
        P(None, "fsdp"),
        P(),
        P("fsdp"),
        P(),
        P(),
        P(),
    )
    return jax.shard_map(
        shards,
        mesh=mesh,
        in_specs=placed,
        out_specs=(
            P(),
            P(None, "fsdp", None),
            P(None, "fsdp", None),
            P("fsdp", None),
            P(),
            P(),
            P(None, "fsdp"),
            P(),
            P(None, "fsdp"),
            P(),
            P("fsdp"),
            P(),
            P(),
            P(),
            P(),
        ),
        check_vma=False,
    )
```

```python
import functools
import math

import jax
import jax.numpy as jnp
import numpy as np
from jax import lax
from jax.experimental import pallas as pl
from jax.experimental.pallas import tpu as pltpu
from jax.sharding import PartitionSpec as P

NCLS = 1001
FREQ = 256
CHANNELS = 4
PATCH = 2
GRID = 32
TSTEPS = 1000
eps_stat = 1e-30
decay = 0.5
rate = 0.01
clip_level = 1.0
D = 384
HEADS = 6
HEAD_DIM = 64
FF = 1536
TOK = 256
PATCH_IN = 16
eps_norm = 1e-06
F32 = jnp.float32
BF16 = jnp.bfloat16
GELU_A = 0.7978845608028654
GELU_B = 0.044715
NT = (((1,), (1,)), ((), ()))
TN = (((0,), (0,)), ((), ()))
FFC = 768
OWN = 48
ROWS = 32


def dot(a, b, dims=(((1,), (0,)), ((), ()))):
    return lax.dot_general(a, b, dims, preferred_element_type=F32)


def norm_rows(t):
    center = t - jnp.mean(t, axis=-1, keepdims=True)
    spread = jnp.mean(center * center, axis=-1, keepdims=True)
    scale = lax.rsqrt(spread + eps_norm)
    return center * scale, scale


def norm_back(dn, n, scale):
    mean_d = jnp.mean(dn, axis=-1, keepdims=True)
    mean_dn = jnp.mean(dn * n, axis=-1, keepdims=True)
    return scale * (dn - mean_d - n * mean_dn)


def rows_sum(v):
    return jnp.sum(v, axis=0, keepdims=True)


def column_of(row):
    n = row.shape[1]
    same = lax.broadcasted_iota(jnp.int32, (n, n), 0) == lax.broadcasted_iota(jnp.int32, (n, n), 1)
    return jnp.sum(jnp.where(same, row, 0.0), axis=1, keepdims=True)


def row_of(column):
    n = column.shape[0]
    same = lax.broadcasted_iota(jnp.int32, (n, n), 0) == lax.broadcasted_iota(jnp.int32, (n, n), 1)
    return jnp.sum(jnp.where(same, column, 0.0), axis=0, keepdims=True)


def soft_rows(s):
    e = jnp.exp(s - jnp.max(s, axis=-1, keepdims=True))
    return e * (1.0 / jnp.sum(e, axis=-1, keepdims=True))


def gelu_parts(x):
    x2 = x * x
    return x2, jnp.tanh(x * (GELU_A + (GELU_A * GELU_B) * x2))


QKV = 0
WO = 3 * D
WF1 = 4 * D
BQ, BV, BO, BF1, BF2 = 0, D, 2 * D, 3 * D, 3 * D + FF
BW = 4 * D + FF
S_HEAD, S_BIAS, S_BPATCH, S_BHEAD, S_SSE, S_ROWS = 16, 32, 48, 49, 50, 56


class BiasRows:
    def __init__(self, ref):
        self.ref = ref

    def __getitem__(self, layer):
        return self.ref[layer][:, 6 * D :]


def compute_kernel(images, group, direct, *refs):
    refs = list(refs)

    def take(count):
        got = refs[:count]
        del refs[:count]
        return got

    patches_ref, target_ref, pos_ref, mods_ref, first_in_ref, first_out_ref, w_patch_ref, w_head_ref = take(8)
    lbias_ref, tbias_ref = take(2)
    own_in_ref, own_out_ref = take(2) if direct else (None,) * 2
    g_in_ref, g_out_ref, sums_ref, g_mods_ref = take(4)
    out_t_ref, out_m_ref, out_d_ref = take(3) if direct else (None,) * 3
    w_in_ref, w_out_ref, tok, mid, qkv, att, branch, outb, normed, act, dinner, dsmall, dqkv, stage, mod_sums, scores, d_probs, probs, d_scores, sems, w_sems = take(21)
    steps = images // group
    crow = group * TOK
    depth = lbias_ref.shape[0]
    lane = lax.broadcasted_iota(jnp.int32, (TOK, 128), 1)
    first_half = lane < HEAD_DIM

    def rows_of(i):
        return pl.ds(pl.multiple_of(i * TOK, TOK), TOK)

    def chunk_of(i):
        return pl.ds(pl.multiple_of(i * crow, crow), crow)

    def near(j):
        return slice(j * TOK, (j + 1) * TOK)

    def down_rows(layer, c):
        rows = FF // w_out_ref.shape[1]
        return w_out_ref[layer, c // rows : (c + FFC) // rows].reshape(FFC, D)

    def mod_row(b, k):
        return mods_ref[k, pl.ds(b, 1), :]

    loads = []
    for layer in range(1 if direct else depth):
        source = first_in_ref, first_out_ref
        if not direct:
            source = first_in_ref.at[layer], first_out_ref.at[layer]
        for n, (ours, theirs) in enumerate(zip((w_in_ref, w_out_ref), source)):
            loads.append(pltpu.make_async_copy(theirs, ours.at[layer], w_sems.at[2 * layer + n]))
            loads[-1].start()
    bias_ref = BiasRows(lbias_ref)

    sums_ref[...] = jnp.zeros_like(sums_ref)
    mod_sums[...] = jnp.zeros_like(mod_sums)

    def add_bias(layer, first, value):
        for at in range(0, value.shape[1], D):
            row = (first + at) // D
            sums_ref[S_BIAS // 8 + layer, row : row + 1, :] += value[:, at : at + D]

    def put_mod(b, k, value):
        mod_sums[k, pl.ds(b, 1), :] = value

    if direct:
        wide_m, wide_t = take(4), take(4)
        plane = take(2 * depth)
        s_got, r_sends, r_recvs, r_loads, g_sends, g_recvs, g_local, b_sends, b_recvs, w_sends, w_recvs, w_local = take(12)
        partners = Partners().all()
        greet(partners)
        m_pieces, t_pieces = [], []
        for layer in range(depth):
            for kind, (pieces, source, out, wide) in enumerate(
                ((m_pieces, g_out_ref, out_m_ref, wide_m), (t_pieces, g_in_ref, out_t_ref, wide_t))
            ):
                n = 2 * layer + kind
                pieces.append(
                    Reducer(source.at[layer], list(wide) + [plane[n]], out.at[layer], r_sends.at[n], r_recvs.at[n], r_loads.at[n])
                )
        w_pieces = []
        for layer in range(1, depth):
            own, ours = own_in_ref.at[layer], w_in_ref.at[layer]

            def sems_of(n, first=3 * (layer - 1)):
                return w_sends.at[first + n], w_recvs.at[first + n], w_local.at[first + n]

            w_pieces.append(by_columns(own, ours, *sems_of(0), 0, 4 * D))
            w_pieces.append(by_columns(own, ours, *sems_of(1), 4 * D, FF))
            w_pieces.append(by_rows(own_out_ref.at[layer], w_out_ref.at[layer], *sems_of(2)))
        s_piece = Butterfly(sums_ref, s_got, b_sends, b_recvs)
        d_pieces = []
        for n, (low, high) in enumerate(((0, 6 * (depth - 1)), (6 * (depth - 1), 6 * depth + 2))):
            d_pieces.append(
                Gatherer(
                    lambda q, a=low, b=high: g_mods_ref.at[a:b],
                    lambda f, q, a=low, b=high: out_d_ref.at[q, f, a:b],
                    lambda q, a=low, b=high: out_d_ref.at[q, :, a:b],
                    g_sends.at[n],
                    g_recvs.at[n],
                    g_local.at[n],
                )
            )

    def send_mods(low, high):
        g_mods_ref[low:high] = mod_sums[low:high].astype(BF16)

    def in_moves(layer, first):
        moves = []
        for q in range(4):
            source = stage.at[0, :, q * D : (q + 1) * D]
            if direct:
                target = (g_in_ref if first == QKV else g_out_ref).at[layer, q, :, 0:D]
            else:
                target = g_in_ref.at[layer, :, first + q * D : first + (q + 1) * D]
            moves.append(pltpu.make_async_copy(source, target, sems.at[0, q]))
        return moves

    def down_moves(layer):
        moves = []
        for c in range(4):
            if not direct:
                source = stage.at[1, :, c * D : (c + 1) * D]
                target = g_out_ref.at[layer, c * D : (c + 1) * D, :]
                moves.append(pltpu.make_async_copy(source, target, sems.at[1, c]))
                continue
            for owner in range(2):
                for q in range(4):
                    start = owner * (D // 2) + q * OWN
                    source = stage.at[1, start : start + OWN, c * D : (c + 1) * D]
                    begin = (2 * c + owner) * OWN
                    target = g_out_ref.at[layer, q, begin : begin + OWN, D : 2 * D]
                    moves.append(pltpu.make_async_copy(source, target, sems.at[1, len(moves)]))
        return moves

    def start(moves):
        for move in moves:
            move.start()

    def finish(moves):
        for move in moves:
            move.wait()

    def clear(slot):
        @pl.loop(0, FF // D)
        def _(c):
            stage[slot, :, pl.ds(pl.multiple_of(c * D, D), D)] = jnp.zeros((D, D), F32)

    def at(li, i, *actions):
        if not direct:
            return

        def place_at(turn_li, turn_i):
            for want_li, want_i, todo in actions:

                @pl.when(jnp.logical_and(turn_li == want_li, turn_i == want_i))
                def _():
                    for piece, k in todo:
                        piece.step(k)

        place_at(li, i)

    @pl.loop(0, images)
    def _(b):
        r = rows_of(b)
        tok[0, r, :] = dot(patches_ref[:, r], w_patch_ref[...], (((0,), (1,)), ((), ()))) + tbias_ref[:, 0:D] + pos_ref[...]

    def half(v, which, factor=None):
        v = v if factor is None else v * jnp.asarray(factor, v.dtype)
        zero = jnp.zeros_like(v)
        return jnp.where(first_half, v, zero) if which == 0 else jnp.where(first_half, zero, v)

    def attention(layer, r, turn):
        for pair in range(HEADS // 2):
            c = pair * 128
            q = qkv[layer, r, c : c + 128]
            k = qkv[layer, r, D + c : D + c + 128]
            v = qkv[layer, r, 2 * D + c : 2 * D + c + 128]
            slot = turn % 2
            turn += 1
            for which in range(2):
                scores[slot, which] = dot(half(q, which, HEAD_DIM ** (-0.5)), k, NT)
            got = []
            for which in range(2):
                for at_row in range(0, TOK, ROWS):
                    block = slice(at_row, at_row + ROWS)
                    probs[slot, which, block, :] = soft_rows(scores[slot, which, block, :]).astype(BF16)
                got.append(dot(probs[slot, which], v))
            att[layer, r, c : c + 128] = jnp.where(first_half, got[0], got[1]).astype(BF16)

    def modulated(t, b, k):
        n, scale = norm_rows(t)
        return n, scale, (n * (1.0 + mod_row(b, k + 1)) + mod_row(b, k)).astype(BF16)

    for load in loads:
        load.wait()
    if direct:
        w_a, w_f, w_o = w_pieces

    @pl.loop(0, depth)
    def _(layer):
        mo = layer * 6

        @pl.loop(0, steps)
        def _(i):
            if direct:
                at(
                    layer,
                    i,
                    (0, 0, [(w_a, 0), (w_f, 0)]),
                    (0, 1, [(w_a, 2), (w_f, 1), (w_o, 1)]),
                    (1, 0, [(w_a, 4)]),
                )
            cr = chunk_of(i)
            bias = bias_ref[layer]
            for j in range(group):
                b = i * group + j
                normed[near(j), :] = modulated(tok[layer, rows_of(b), :], b, mo)[2]
            hc = normed[...]
            p = dot(hc, w_in_ref[layer, :, QKV : QKV + 2 * D])
            qkv[layer, cr, 0:D] = (p[:, 0:D] + bias[:, BQ : BQ + D]).astype(BF16)
            qkv[layer, cr, D : 2 * D] = p[:, D : 2 * D].astype(BF16)
            p = dot(hc, w_in_ref[layer, :, QKV + 2 * D : QKV + 3 * D])
            qkv[layer, cr, 2 * D : 3 * D] = (p + bias[:, BV : BV + D]).astype(BF16)
            for j in range(group):
                attention(layer, rows_of(i * group + j), 3 * j)
            if direct:
                at(
                    layer,
                    i,
                    (0, 0, [(w_a, 1), (w_o, 0)]),
                    (0, 1, [(w_a, 3), (w_f, 2), (w_o, 2)]),
                    (1, 0, [(w_f, 3), (w_o, 3), (w_f, 4), (w_o, 4)]),
                )
            br = dot(att[layer, cr, :], w_in_ref[layer, :, WO : WO + D]) + bias[:, BO : BO + D]
            branch[layer, cr, :] = br.astype(BF16)
            for j in range(group):
                b = i * group + j
                r = rows_of(b)
                t2 = tok[layer, r, :] + mod_row(b, mo + 2) * br[near(j)]
                mid[layer, r, :] = t2
                normed[near(j), :] = modulated(t2, b, mo + 3)[2]
            mc = normed[...]
            out = jnp.zeros((crow, D), F32) + bias[:, BF2 : BF2 + D]
            for c in range(0, FF, FFC):
                x = dot(mc, w_in_ref[layer, :, WF1 + c : WF1 + c + FFC]) + bias[:, BF1 + c : BF1 + c + FFC]
                side = 0.5 * x
                a = (side + side * gelu_parts(x)[1]).astype(BF16)
                out = out + dot(a, down_rows(layer, c))
            outb[layer, cr, :] = out.astype(BF16)
            for j in range(group):
                b = i * group + j
                r = rows_of(b)
                tok[layer + 1, r, :] = mid[layer, r, :] + mod_row(b, mo + 5) * out[near(j)]

    dtok = tok.at[depth]
    head_bias = column_of(tbias_ref[:, 5 * D : 5 * D + PATCH_IN])

    @pl.loop(0, images)
    def _(b):
        r = rows_of(b)
        k = 6 * depth
        n, scale, n3 = modulated(dtok[r, :], b, k)
        miss = dot(w_head_ref[...], n3, (((0,), (1,)), ((), ()))) + head_bias - target_ref[:, r]
        sums_ref[S_SSE // 8, S_SSE % 8 : S_SSE % 8 + 1, 0:TOK] += rows_sum(miss * miss)
        dp = (2.0 * miss).astype(BF16)
        sums_ref[S_HEAD // 8 : S_HEAD // 8 + 2] += dot(dp, n3).reshape(2, 8, D)
        sums_ref[S_BHEAD // 8, S_BHEAD % 8 : S_BHEAD % 8 + 1, 0:PATCH_IN] += row_of(
            jnp.sum(dp.astype(F32), axis=1, keepdims=True)
        )
        dn3 = dot(dp, w_head_ref[...], (((0,), (1,)), ((), ())))
        put_mod(b, k, rows_sum(dn3))
        put_mod(b, k + 1, rows_sum(dn3 * n))
        dtok[r, :] = norm_back(dn3 * (1.0 + mod_row(b, k + 1)), n, scale)

    if direct:
        t_last, m_last = t_pieces[depth - 1], m_pieces[depth - 1]
        t_first, m_first = t_pieces[0], m_pieces[0]
        d_first, d_last = d_pieces

    @pl.loop(0, depth)
    def _(li):
        layer = depth - 1 - li
        mo = layer * 6
        bias = bias_ref[layer]

        @pl.when(li > 0)
        def _():
            finish(in_moves(layer + 1, QKV))
            send_mods(6 * (depth - 1), 6 * depth + 2)

        clear(0)
        clear(1)

        @pl.loop(0, steps)
        def _(i):
            if direct:
                at(li, i, (1, 0, [(m_last, 2), (t_last, 0), (d_last, 0)]), (1, 1, [(t_last, 1)]))
            cr = chunk_of(i)
            for j in range(group):
                b = i * group + j
                r = rows_of(b)
                normed[near(j), :] = modulated(mid[layer, r, :], b, mo + 3)[2]
                d = dtok[r, :]
                put_mod(b, mo + 5, rows_sum(d * outb[layer, r, :].astype(F32)))
                do = (d * mod_row(b, mo + 5)).astype(BF16)
                dsmall[near(j), :] = do
                add_bias(layer, BF2, rows_sum(do.astype(F32)))
            mc = normed[...]
            do = dsmall[...]
            dm = jnp.zeros((crow, D), F32)
            for c in range(0, FF, FFC):
                x = dot(mc, w_in_ref[layer, :, WF1 + c : WF1 + c + FFC]) + bias[:, BF1 + c : BF1 + c + FFC]
                x2, t = gelu_parts(x)
                side = 0.5 * x
                act[:, c : c + FFC] = (side + side * t).astype(BF16)
                slope = (0.5 + 0.5 * t) + side * (1.0 - t * t) * (GELU_A + (3.0 * GELU_A * GELU_B) * x2)
                di = (dot(do, down_rows(layer, c), NT) * slope).astype(BF16)
                dinner[:, c : c + FFC] = di
                add_bias(layer, BF1 + c, rows_sum(di.astype(F32)))
                dm = dm + dot(di, w_in_ref[layer, :, WF1 + c : WF1 + c + FFC], NT)
            for j in range(group):
                b = i * group + j
                r = rows_of(b)
                n, scale = norm_rows(mid[layer, r, :])
                dmj = dm[near(j)]
                put_mod(b, mo + 3, rows_sum(dmj))
                put_mod(b, mo + 4, rows_sum(dmj * n))
                dtok[r, :] = dtok[r, :] + norm_back(dmj * (1.0 + mod_row(b, mo + 4)), n, scale)

            if direct:
                at(li, i, (1, 0, [(d_last, 1)]), (1, 1, [(m_last, 3), (d_last, 2)]))

            @pl.loop(0, FF // FFC)
            def _(c):
                cs = pl.ds(pl.multiple_of(c * FFC, FFC), FFC)
                stage[0, :, cs] += dot(normed[...], dinner[:, cs], TN)

            @pl.loop(0, FF // D)
            def _(c):
                cs = pl.ds(pl.multiple_of(c * D, D), D)
                stage[1, :, cs] += dot(dsmall[...], act[:, cs], TN)

        start(in_moves(layer, WF1))

        @pl.loop(0, FF // D)
        def _(c):
            cs = pl.ds(pl.multiple_of(c * D, D), D)
            stage[1, :, cs] = stage[1, :, cs].T

        start(down_moves(layer))

        @pl.loop(0, steps)
        def _(i):
            if direct:
                at(li, i, (1, 0, [(t_last, 2)]))
            cr = chunk_of(i)
            for j in range(group):
                b = i * group + j
                r = rows_of(b)
                d = dtok[r, :]
                put_mod(b, mo + 2, rows_sum(d * branch[layer, r, :].astype(F32)))
                db = (d * mod_row(b, mo + 2)).astype(BF16)
                dsmall[near(j), :] = db
                add_bias(layer, BO, rows_sum(db.astype(F32)))
            branch[layer, cr, :] = dot(dsmall[...], w_in_ref[layer, :, WO : WO + D], NT).astype(BF16)

            @pl.when(i == 0)
            def _():
                finish(in_moves(layer, WF1))
                finish(down_moves(layer))
                clear(0)

            if direct:
                at(li, i, (0, 0, [(m_last, 0)]), (1, 0, [(m_last, 4)]), (1, 1, [(m_first, 1), (t_last, 4)]))

            @pl.loop(0, group)
            def _(j):
                r = rows_of(i * group + j)
                here = rows_of(j)
                q_sums, v_sums = [], []
                for pair in range(HEADS // 2):
                    c = pair * 128
                    q = qkv[layer, r, c : c + 128]
                    k = qkv[layer, r, D + c : D + c + 128]
                    v = qkv[layer, r, 2 * D + c : 2 * D + c + 128]
                    da = branch[layer, r, c : c + 128]
                    slot = pair % 2
                    for which in range(2):
                        scores[slot, which] = dot(half(q, which, HEAD_DIM ** (-0.5)), k, NT)
                        d_probs[slot, which] = dot(half(da, which), v, NT)
                    got = []
                    for which in range(2):
                        for at_row in range(0, TOK, ROWS):
                            block = slice(at_row, at_row + ROWS)
                            p = soft_rows(scores[slot, which, block, :])
                            probs[slot, which, block, :] = p.astype(BF16)
                            dpr = d_probs[slot, which, block, :]
                            ds = p * (dpr - jnp.sum(dpr * p, axis=-1, keepdims=True))
                            d_scores[slot, which, block, :] = ds.astype(BF16)
                        dv = dot(probs[slot, which], da, TN)
                        dq = dot(d_scores[slot, which], k)
                        dk = dot(d_scores[slot, which], q, TN)
                        got.append((dq, dk, dv))
                    dq = (jnp.where(first_half, got[0][0], got[1][0]) * HEAD_DIM ** (-0.5)).astype(BF16)
                    dk = (jnp.where(first_half, got[0][1], got[1][1]) * HEAD_DIM ** (-0.5)).astype(BF16)
                    dv = jnp.where(first_half, got[0][2], got[1][2]).astype(BF16)
                    dqkv[here, c : c + 128] = dq
                    dqkv[here, D + c : D + c + 128] = dk
                    dqkv[here, 2 * D + c : 2 * D + c + 128] = dv
                    q_sums.append(rows_sum(dq.astype(F32)))
                    v_sums.append(rows_sum(dv.astype(F32)))
                sums_ref[S_BIAS // 8 + layer, 0:1, :] += jnp.concatenate(q_sums, axis=1)
                sums_ref[S_BIAS // 8 + layer, 1:2, :] += jnp.concatenate(v_sums, axis=1)

            if direct:
                at(
                    li,
                    i,
                    (0, 0, [(m_last, 1)]),
                    (1, 0, [(m_last, 5), (m_first, 0), (t_last, 3), (d_last, 3)]),
                    (1, 1, [(t_last, 5), (d_last, 4)]),
                )
            dh = dot(dqkv[...], w_in_ref[layer, :, QKV : QKV + 3 * D], NT)
            for j in range(group):
                b = i * group + j
                r = rows_of(b)
                n, scale, h = modulated(tok[layer, r, :], b, mo)
                normed[near(j), :] = h
                dhj = dh[near(j)]
                put_mod(b, mo, rows_sum(dhj))
                put_mod(b, mo + 1, rows_sum(dhj * n))
                dtok[r, :] = dtok[r, :] + norm_back(dhj * (1.0 + mod_row(b, mo + 1)), n, scale)

            @pl.loop(0, 3)
            def _(c):
                cs = pl.ds(pl.multiple_of(c * D, D), D)
                stage[0, :, cs] += dot(normed[...], dqkv[:, cs], TN)

            stage[0, :, 3 * D : 4 * D] += dot(att[layer, cr, :], dsmall[...], TN)

        start(in_moves(layer, QKV))

    if direct:
        send_mods(0, 6 * (depth - 1))
        d_first.step(0)
        m_first.step(2)
    else:
        g_mods_ref[...] = mod_sums[...].astype(BF16)

    @pl.loop(0, images)
    def _(b):
        r = rows_of(b)
        d = dtok[r, :].astype(BF16)
        sums_ref[S_BPATCH // 8, S_BPATCH % 8 : S_BPATCH % 8 + 1, :] += rows_sum(d.astype(F32))
        sums_ref[0:2] += dot(patches_ref[:, r], d).reshape(2, 8, D)

    finish(in_moves(0, QKV))
    if direct:
        for piece, k in (
            (t_first, 0),
            (s_piece, 0),
            (d_first, 1),
            (t_first, 1),
            (s_piece, 1),
            (s_piece, 2),
            (t_first, 2),
            (d_first, 2),
            (s_piece, 3),
            (m_first, 3),
            (s_piece, 4),
            (d_first, 3),
            (t_first, 3),
            (d_first, 4),
            (s_piece, 5),
            (m_first, 4),
            (t_first, 4),
            (m_first, 5),
            (t_first, 5),
        ):
            piece.step(k)


def run_steps(plans):
    last = max(first + count for first, count, _ in plans)
    for tick in range(last):
        for first, count, piece in plans:
            if 0 <= tick - first < count:
                piece.step(tick - first)


def compute(patches, target, pos, mods, w_in, w_out, w_patch, w_head, lbias, tbias, own=(), group=3):
    direct = len(own) > 0
    depth = lbias.shape[0]
    rows = patches.shape[1]
    images = rows // TOK
    crow = group * TOK
    kinds = mods.shape[0]
    vm = pl.BlockSpec(memory_space=pltpu.VMEM)
    anyspace = pl.BlockSpec(memory_space=pl.ANY)
    shape = jax.ShapeDtypeStruct
    dma = pltpu.SemaphoreType.DMA
    out_shape = [
        shape((depth, 4, D, D) if direct else (depth, D, 4 * D + FF), F32),
        shape((depth, 4, D, 2 * D) if direct else (depth, FF, D), F32),
        shape((S_ROWS // 8, 8, D), F32),
        shape((kinds, 8, D), BF16),
    ]
    out_specs = [anyspace, anyspace, vm, vm]
    scratch = [
        pltpu.VMEM((depth, D, 4 * D + FF), BF16),
        pltpu.VMEM((depth,) + (w_out.shape if direct else w_out.shape[1:]), BF16),
        pltpu.VMEM((depth + 1, rows, D), F32),
        pltpu.VMEM((depth, rows, D), F32),
        pltpu.VMEM((depth, rows, 3 * D), BF16),
        pltpu.VMEM((depth, rows, D), BF16),
        pltpu.VMEM((depth, rows, D), BF16),
        pltpu.VMEM((depth, rows, D), BF16),
        pltpu.VMEM((crow, D), BF16),
        pltpu.VMEM((crow, FF), BF16),
        pltpu.VMEM((crow, FF), BF16),
        pltpu.VMEM((crow, D), BF16),
        pltpu.VMEM((crow, 3 * D), BF16),
        pltpu.VMEM((2, D, FF), F32),
        pltpu.VMEM((kinds, 8, D), F32),
        pltpu.VMEM((2, 2, TOK, TOK), F32),
        pltpu.VMEM((2, 2, TOK, TOK), F32),
        pltpu.VMEM((2, 2, TOK, TOK), BF16),
        pltpu.VMEM((2, 2, TOK, TOK), BF16),
        dma((2, 32)),
        dma((2 * depth,)),
    ]
    params = dict(vmem_limit_bytes=67_043_328)
    if direct:
        out_shape += [
            shape((depth, 4, OWN, D), F32),
            shape((depth, 4, OWN, 2 * D), F32),
            shape((4, 8, kinds, 8, D), BF16),
        ]
        out_specs += [anyspace, anyspace, anyspace]
        scratch += wide_scratch(2 * D) + wide_scratch(D)
        for _ in range(depth):
            scratch += [pltpu.VMEM((8, OWN, 2 * D), BF16), pltpu.VMEM((8, OWN, D), BF16)]
        count = 2 * depth
        gathers = 3 * (depth - 1)
        scratch += [pltpu.VMEM((5, S_ROWS // 8, 8, D), F32), dma((count, 13)), dma((count, 13)), dma((count, 3))]
        scratch += [dma((2, 10)), dma((2, 10)), dma((2,)), dma((5,)), dma((5,))]
        scratch += [dma((gathers, 10)), dma((gathers, 10)), dma((gathers,))]
        params.update(collective_id=1, has_side_effects=True)
    return pl.pallas_call(
        functools.partial(compute_kernel, images, group, direct),
        out_shape=tuple(out_shape),
        in_specs=[vm] * 4 + [anyspace] * 2 + [vm] * 4 + [anyspace] * len(own),
        out_specs=tuple(out_specs),
        scratch_shapes=scratch,
        compiler_params=pltpu.CompilerParams(**params),
        name="step_compute",
    )(patches, target, pos, mods, w_in, w_out, w_patch, w_head, lbias[:, None, :], tbias, *own)


def place():
    f = lax.axis_index("fsdp")
    r = lax.axis_index("rep")
    z = f // 2
    y = f - 2 * z
    x = r // 2
    c = r - 2 * x
    return z, y, x, c


def device(z, y, x, c):
    return {"fsdp": 2 * z + y, "rep": 2 * x + c}


def greet(peers):
    barrier = pltpu.get_barrier_semaphore()
    for peer in peers:
        pl.semaphore_signal(barrier, inc=1, device_id=peer, device_id_type=pl.DeviceIdType.MESH)
    pl.semaphore_wait(barrier, len(peers))


def remote(source, target, send, recv, peer):
    return pltpu.make_async_remote_copy(
        src_ref=source, dst_ref=target, send_sem=send, recv_sem=recv, device_id=peer, device_id_type=pl.DeviceIdType.MESH
    )


class Reducer:
    def __init__(self, source, bufs, out, sends, recvs, loads):
        self.source = source
        self.keep, self.got0, self.low, self.gotx, self.gotp = bufs
        self.out = out
        self.sends, self.recvs, self.loads = sends, recvs, loads

    def flat(self, ref, half):
        return ref.at[half].reshape(D, ref.shape[-1])

    def load(self, half):
        c = place()[3]
        return pltpu.make_async_copy(self.source.at[2 * half + c], self.flat(self.keep, half), self.loads.at[half])

    def store(self):
        z, y, x, c = place()
        return pltpu.make_async_copy(self.keep.at[x, 2 * z + y], self.out.at[2 * x + c], self.loads.at[2])

    def move(self, slot):
        z, y, x, c = place()
        mine = 2 * x + c
        partners = Partners()
        if slot < 2:
            source, target, peer = self.source.at[2 * slot + 1 - c], self.flat(self.got0, slot), partners.c
        elif slot == 2:
            source, target, peer = self.low, self.gotx, partners.x
        elif slot < 10:
            f = lax.axis_index("fsdp")
            to = lax.rem(f + slot - 2, 8)
            source, target, peer = self.low.at[to], self.gotp.at[f], {"fsdp": to}
        else:
            peer = partners.x if slot == 10 else partners.c
            target = self.out.at[2 * (1 - x) + c if slot == 12 else mine]
            source = target if slot == 12 else self.keep.at[x, 2 * z + y]
        return remote(source, target, self.sends.at[slot], self.recvs.at[slot], peer)

    def step(self, k):
        z, y, x, c = place()
        f = 2 * z + y
        if k == 0:
            for half in range(2):
                self.load(half).start()
                self.move(half).start()
        if k == 1:
            for half in range(2):
                self.load(half).wait()
                self.move(half).wait()

            @pl.loop(0, 8)
            def _(i):
                self.low[i] = (self.keep[1 - x, i] + self.got0[1 - x, i]).astype(BF16)

            self.move(2).start()

            @pl.loop(0, 8)
            def _(i):
                self.keep[x, i] = self.keep[x, i] + self.got0[x, i]
        if k == 2:
            self.move(2).wait()

            @pl.loop(0, 8)
            def _(i):
                self.low[i] = (self.keep[x, i] + self.gotx[i].astype(F32)).astype(BF16)

            for slot in range(3, 10):
                self.move(slot).start()
            self.keep[x, f] = self.keep[x, f] + self.gotx[f].astype(F32)
        if k == 3:
            for slot in range(3, 10):
                self.move(slot).wait()
            total = self.keep[x, f]
            for d in range(1, 8):
                total = total + self.gotp[lax.rem(f + d, 8)].astype(F32)
            self.keep[x, f] = total
            self.store().start()
            for slot in range(10, 12):
                self.move(slot).start()
        if k == 4:
            self.move(10).wait()
            self.move(12).start()
        if k == 5:
            self.store().wait()
            self.move(11).wait()
            self.move(12).wait()


class Partners:
    def __init__(self):
        z, y, x, c = place()
        self.c = device(z, y, x, 1 - c)
        self.x = device(z, y, 1 - x, c)
        self.y = device(z, 1 - y, x, c)
        self.z1 = device(z + 1 - 2 * lax.rem(z, 2), y, x, c)
        self.z2 = device(lax.rem(z + 2, 4), y, x, c)

    def pairs(self):
        return [self.c, self.x, self.y, self.z1, self.z2]

    def all(self):
        z, y, x, c = place()
        f = 2 * z + y
        return [self.c, self.x, device(z, y, 1 - x, 1 - c)] + [{"fsdp": lax.rem(f + k, 8)} for k in range(1, 8)]


REDUCER_STEPS = 6


def wide_scratch(width):
    return [
        pltpu.VMEM((2, 8, OWN, width), F32),
        pltpu.VMEM((2, 8, OWN, width), F32),
        pltpu.VMEM((8, OWN, width), BF16),
        pltpu.VMEM((8, OWN, width), BF16),
    ]


class Gatherer:
    def __init__(self, source, target, whole, sends, recvs, local):
        self.source, self.target, self.whole = source, target, whole
        self.sends, self.recvs, self.local = sends, recvs, local

    def own(self):
        z, y, x, c = place()
        return pltpu.make_async_copy(self.source(2 * x + c), self.target(2 * z + y, 2 * x + c), self.local)

    def move(self, slot):
        z, y, x, c = place()
        q = 2 * x + c
        if slot < 3:
            source, target, peer = self.source(q), self.target(2 * z + y, q), device(lax.rem(z + 1 + slot, 4), y, x, c)
        elif slot == 3:
            source, target, peer = self.source(q), self.target(2 * z + y, q), device(z, 1 - y, x, c)
        elif slot < 7:
            at = 2 * lax.rem(z + 7 - slot, 4) + y
            source = target = self.target(at, q)
            peer = device(z, 1 - y, x, c)
        else:
            part = 2 * (1 - x) + c if slot == 9 else q
            source = target = self.whole(part)
            peer = device(z, y, 1 - x, c) if slot == 7 else device(z, y, x, 1 - c)
        return remote(source, target, self.sends.at[slot], self.recvs.at[slot], peer)

    def step(self, k):
        if k == 0:
            for slot in range(4):
                self.move(slot).start()
            self.own().start()
        if k == 1:
            for slot in range(3):
                self.move(slot).wait()
                self.move(slot + 4).start()
        if k == 2:
            self.own().wait()
            for slot in range(3, 7):
                self.move(slot).wait()
            self.move(7).start()
            self.move(8).start()
        if k == 3:
            self.move(7).wait()
            self.move(9).start()
        if k == 4:
            self.move(8).wait()
            self.move(9).wait()


GATHER_STEPS = 5


def by_columns(source, target, sends, recvs, local, first=0, width=None):
    rows = source.shape[0]
    width = width or source.shape[1]
    part = width // 4

    def cols(q):
        return pl.ds(pl.multiple_of(first + q * part, 128), part)

    def rows_of(f):
        return pl.ds(pl.multiple_of(f * rows, 16), rows)

    return Gatherer(
        lambda q: source.at[:, cols(q)],
        lambda f, q: target.at[rows_of(f), cols(q)],
        lambda q: target.at[:, cols(q)],
        sends,
        recvs,
        local,
    )


def by_rows(source, target, sends, recvs, local):
    return Gatherer(
        lambda q: source.at[q],
        lambda f, q: target.at[f, q],
        lambda q: target.at[:, q],
        sends,
        recvs,
        local,
    )


def slab(source, target, sends, recvs, local):
    return Gatherer(lambda q: source, lambda f, q: target.at[q, f], lambda q: target.at[q], sends, recvs, local)


class Butterfly:
    def __init__(self, total, got, sends, recvs):
        self.total, self.got, self.sends, self.recvs = total, got, sends, recvs

    def move(self, k):
        partner = Partners().pairs()[k]
        return remote(self.total, self.got.at[k], self.sends.at[k], self.recvs.at[k], partner)

    def step(self, k):
        if k > 0:
            self.move(k - 1).wait()
            self.total[...] = self.total[...] + self.got[k - 1]
        if k < 5:
            self.move(k).start()


BUTTERFLY_STEPS = 6


C_T1, C_T2, C_PATCH, C_HEAD, C_ALL = 1024, 1280, 1664, 1792, 2048
SLOTS = 256


def silu_slope(x):
    gate = 1.0 / (1.0 + jnp.exp(-x))
    return gate * (1.0 + x * (1.0 - gate))


def silu(x):
    return x / (1.0 + jnp.exp(-x))


def prologue_kernel(
    kinds,
    images,
    small_ref,
    feat_ref,
    w_mods_ref,
    lbias_ref,
    tbias_ref,
    own_in_ref,
    own_out_ref,
    w_patch_ref,
    w_head_ref,
    time2_ref,
    w_in_ref,
    w_out_ref,
    mods_ref,
    time1_ref,
    s1_ref,
    before_ref,
    cond_ref,
    feats_ref,
    full,
    part,
    got,
    cond_rows,
    wide,
    sends,
    recvs,
    local,
    p_sends,
    p_recvs,
    p_local,
):
    z, y, x, c = place()
    f = 2 * z + y
    r = 2 * x + c

    def sems(n):
        return sends.at[n], recvs.at[n], local.at[n]

    feats = slab(feat_ref, feats_ref, *sems(0))
    small = by_columns(small_ref, full, *sems(1))
    own_in, own_out = own_in_ref.at[0], own_out_ref.at[0]
    attention = by_columns(own_in, w_in_ref, *sems(2), 0, 4 * D)
    inner = by_columns(own_in, w_in_ref, *sems(3), 4 * D, FF)
    outer = by_rows(own_out, w_out_ref, *sems(4))
    plans = [
        (0, GATHER_STEPS, feats),
        (0, GATHER_STEPS, small),
        (2, GATHER_STEPS, attention),
        (3, GATHER_STEPS, inner),
        (4, GATHER_STEPS, outer),
    ]
    partners = Partners()
    greet(partners.all())
    last = max(first + count for first, count, _ in plans)
    copies = []
    for tick in range(last):
        for first, count, piece in plans:
            if 0 <= tick - first < count:
                piece.step(tick - first)
        if tick != GATHER_STEPS - 1:
            continue
        rows = feats_ref[...].reshape(SLOTS, feats_ref.shape[-1])
        feat = rows[:, :FREQ].astype(BF16)
        label = rows[:, FREQ : FREQ + 1]
        place_of = lax.broadcasted_iota(jnp.int32, (SLOTS, C_T1), 1).astype(F32)
        picked = jnp.where(label == place_of, 1.0, 0.0).astype(BF16)
        time1 = dot(feat, full[:, C_T1:C_T2], NT) + tbias_ref[:, D : 2 * D]
        s1 = silu(time1).astype(BF16)
        before = dot(s1, full[:, C_T2 : C_T2 + D]) + tbias_ref[:, 2 * D : 3 * D] + dot(picked, full[:, :C_T1], NT)
        cond = silu(before)
        cond_rows[...] = cond
        pick = lax.broadcasted_iota(jnp.int32, (D, OWN), 0) == f * OWN + lax.broadcasted_iota(jnp.int32, (D, OWN), 1)
        group = cond_rows[pl.ds(pl.multiple_of(r * 64, 64), 64), :].astype(BF16)
        group = dot(group, jnp.where(pick, 1.0, 0.0).astype(BF16)).astype(BF16)
        for k in range(kinds):
            mods = dot(group, w_mods_ref[:, k * D : (k + 1) * D])
            for n in range(8):
                part[n, k * images : (k + 1) * images, :] = mods[8 * n : 8 * n + images]
        for k in range(1, 8):
            to = lax.rem(f + k, 8)
            copies.append(remote(part.at[to], got.at[f], p_sends.at[k - 1], p_recvs.at[k - 1], {"fsdp": to}))
            copies[-1].start()
        own = pltpu.make_async_copy(part.at[f], got.at[f], p_local)
        own.start()
        mine = pl.ds(pl.multiple_of(f * OWN, OWN), OWN)
        time1_ref[...] = time1.T
        wide[...] = s1.astype(F32).T
        s1_ref[...] = wide[mine, :].astype(BF16)
        wide[...] = before.T
        before_ref[...] = wide[mine, :]
        wide[...] = cond.T
        cond_ref[...] = wide[mine, :].astype(BF16)
        w_patch_ref[...] = full[:, C_PATCH : C_PATCH + PATCH_IN]
        w_head_ref[...] = full[:, C_HEAD : C_HEAD + PATCH_IN]
        time2_ref[...] = full[:, C_T2 : C_T2 + D]
        mods_ref[...] = jnp.zeros_like(mods_ref)
    own.wait()
    for copy in copies:
        copy.wait()
    depth = (kinds - 2) // 6
    for k in range(kinds):
        at = slice(k * images, (k + 1) * images)
        total = got[0, at]
        for n in range(1, 8):
            total = total + got[n, at]
        if k < 6 * depth:
            bias = lbias_ref[k // 6 : k // 6 + 1, k % 6 * D : k % 6 * D + D]
        else:
            first = 3 * D + (k - 6 * depth) * D
            bias = tbias_ref[:, first : first + D]
        mods_ref[k, 0:images] = total + bias


def prologue(small, feat, w_mods, lbias, tbias, own_in, own_out, images):
    kinds = w_mods.shape[1] // D
    shape = jax.ShapeDtypeStruct
    anyspace = pl.BlockSpec(memory_space=pl.ANY)
    vm = pl.BlockSpec(memory_space=pltpu.VMEM)
    dma = pltpu.SemaphoreType.DMA
    rows = -(-kinds * images // 8) * 8
    return pl.pallas_call(
        functools.partial(prologue_kernel, kinds, images),
        out_shape=(
            shape((D, PATCH_IN), BF16),
            shape((D, PATCH_IN), BF16),
            shape((D, D), BF16),
            shape((D, own_in.shape[2]), BF16),
            shape((8, 4, OWN, D), BF16),
            shape((16, 8, D), F32),
            shape((D, SLOTS), F32),
            shape((OWN, SLOTS), BF16),
            shape((OWN, SLOTS), F32),
            shape((OWN, SLOTS), BF16),
            shape((4, 8) + feat.shape, F32),
        ),
        in_specs=[anyspace, vm, vm, vm, vm, anyspace, anyspace],
        out_specs=(vm, vm, vm, anyspace, anyspace) + (vm,) * 6,
        scratch_shapes=[
            pltpu.VMEM((D, C_ALL), BF16),
            pltpu.VMEM((8, rows, D), F32),
            pltpu.VMEM((8, rows, D), F32),
            pltpu.VMEM((SLOTS, D), F32),
            pltpu.VMEM((D, SLOTS), F32),
            dma((5, 10)),
            dma((5, 10)),
            dma((5,)),
            dma((7,)),
            dma((7,)),
            dma,
        ],
        compiler_params=pltpu.CompilerParams(collective_id=2, has_side_effects=True, vmem_limit_bytes=60 * 1024 * 1024),
        name="step_prologue",
    )(small, feat, w_mods, lbias, tbias, own_in, own_out)


E_PATCH, E_T1, E_T2, E_FIN, E_HEAD, E_ALL = 1024, 1152, 1408, 1792, 2560, 2688
STAT = 1792


def total_of(v):
    return jnp.sum(rows_sum(v), axis=1, keepdims=True)


def update_kernel(
    sizes,
    out_t_ref,
    out_m_ref,
    sums_ref,
    d_mods_ref,
    cond_ref,
    before_ref,
    time1_ref,
    s1_ref,
    feats_ref,
    time2_ref,
    w_mods_ref,
    in_ref,
    down_ref,
    edge_ref,
    lbias_ref,
    tbias_ref,
    in_rows_ref,
    in_cols_ref,
    down_rows_ref,
    down_cols_ref,
    edge_rows_ref,
    edge_cols_ref,
    lbias_v_ref,
    tbias_v_ref,
    in_new,
    down_new,
    edge_new,
    lbias_new,
    tbias_new,
    in_rows_new,
    in_cols_new,
    down_rows_new,
    down_cols_new,
    edge_rows_new,
    edge_cols_new,
    lbias_v_new,
    tbias_v_new,
    tail_ref,
    g_in,
    g_down,
    g_edge,
    d_time2,
    d_time1,
    small_t,
    stats,
    squares,
    sends,
    recvs,
):
    classes, tokens = sizes
    depth = in_ref.shape[0]
    kinds = w_mods_ref.shape[1] // D
    fin = 6 * depth
    f = lax.axis_index("fsdp")
    others = [{"fsdp": lax.rem(f + k, 8)} for k in range(1, 8)]
    scale = 1.0 / (PATCH_IN * math.sqrt(tokens))
    mine = pl.ds(pl.multiple_of(f * OWN, OWN), OWN)
    greet(others)

    def share(n, buffer):
        copies = []
        for k in range(1, 8):
            copies.append(remote(buffer.at[f], buffer.at[f], sends.at[n, k - 1], recvs.at[n, k - 1], others[k - 1]))
            copies[-1].start()
        return copies

    d_cond = jnp.zeros((OWN, SLOTS), F32)
    ones = jnp.ones((8, SLOTS), BF16)
    for k in range(kinds):
        rows = d_mods_ref[:, :, k].astype(F32).reshape(SLOTS, D).astype(BF16)
        g = dot(cond_ref[...], rows) * scale
        b = dot(ones, rows)[0:1] * scale
        if k < fin:
            layer, at = k // 6, (k % 6) * D
            g_in[layer, :, at : at + D] = g
            lbias_new[layer : layer + 1, at : at + D] = b
        else:
            at = (k - fin) * D
            g_edge[:, E_FIN + at : E_FIN + at + D] = g
            tbias_new[:, 3 * D + at : 3 * D + at + D] = b
        d_cond = d_cond + dot(w_mods_ref[:, k * D : (k + 1) * D], rows, NT)
    d_before = d_cond * silu_slope(before_ref[...])
    d_time2[f] = d_before.astype(BF16)
    copies = share(0, d_time2)
    rows = feats_ref[...].reshape(SLOTS, feats_ref.shape[-1])
    feat = rows[:, :FREQ].astype(BF16)
    label = rows[:, FREQ : FREQ + 1]
    picked = jnp.where(label == lax.broadcasted_iota(jnp.int32, (SLOTS, E_PATCH), 1).astype(F32), 1.0, 0.0).astype(BF16)
    top = d_before.astype(BF16)
    left = d_before - top.astype(F32)
    middle = left.astype(BF16)
    low = (left - middle.astype(F32)).astype(BF16)
    g_edge[:, 0:E_PATCH] = (dot(top, picked) + dot(middle, picked) + dot(low, picked)) * scale
    small_t[:, 0 : 2 * PATCH_IN] = sums_ref[0 : 2 * PATCH_IN, :].T * scale
    own_small = small_t[mine, :]
    lane = lax.broadcasted_iota(jnp.int32, (OWN, 128), 1)
    g_edge[:, E_PATCH:E_T1] = jnp.where(lane < PATCH_IN, own_small, 0.0)
    g_edge[:, E_HEAD:E_ALL] = jnp.where(lane < PATCH_IN, pltpu.roll(own_small, 128 - PATCH_IN, 1), 0.0)
    for layer in range(depth):
        for q in range(4):
            g_in[layer, :, 6 * D + q * D : 7 * D + q * D] = out_t_ref[layer, q] * scale
            g_in[layer, :, 10 * D + q * D : 11 * D + q * D] = out_m_ref[layer, q, :, 0:D] * scale
            g_down[layer, q * OWN : (q + 1) * OWN, :] = out_m_ref[layer, q, :, D : 2 * D] * scale
    for copy in copies:
        copy.wait()
    d2 = d_time2[...].reshape(D, SLOTS)
    g_edge[:, E_T2:E_FIN] = dot(s1_ref[...], d2, NT) * scale
    d1 = (dot(time2_ref[...], d2) * silu_slope(time1_ref[...])).astype(BF16)
    d_time1[...] = d1
    g_edge[:, E_T1:E_T2] = dot(d_time1[mine, :], feat) * scale
    tbias_new[:, D : 2 * D] = dot(ones, d1, NT)[0:1] * scale
    tbias_new[:, 2 * D : 3 * D] = dot(ones, d2, NT)[0:1] * scale
    tbias_new[:, 0:D] = sums_ref[S_BPATCH : S_BPATCH + 1, :] * scale
    lane = lax.broadcasted_iota(jnp.int32, (1, 2 * PATCH_IN), 1)
    tbias_new[:, 5 * D :] = jnp.where(lane < PATCH_IN, sums_ref[S_BHEAD : S_BHEAD + 1, 0 : 2 * PATCH_IN], 0.0) * scale
    for layer in range(depth):
        for j in range(8):
            row = S_BIAS + 8 * layer + j
            lbias_new[layer : layer + 1, 6 * D + j * D : 7 * D + j * D] = sums_ref[row : row + 1, :] * scale

    wide = in_ref.shape[2]
    rows_in, rows_down = [], []
    for layer in range(depth):
        s = jnp.zeros((OWN, 1), F32)
        for t in range(wide // STAT):
            g = g_in[layer, :, t * STAT : (t + 1) * STAT]
            g2 = g * g
            s = s + jnp.sum(g2, axis=1, keepdims=True)
            stats[f, wide // STAT * layer + t : wide // STAT * layer + t + 1, :] = rows_sum(g2)
        new = decay * column_of(in_rows_ref[layer : layer + 1, :]) + (1.0 - decay) * (s / wide + eps_stat)
        rows_in.append(new)
        in_rows_new[layer : layer + 1, :] = row_of(new)
        g = g_down[layer]
        g2 = g * g
        new = decay * column_of(down_rows_ref[layer : layer + 1, :]) + (1.0 - decay) * (
            jnp.sum(g2, axis=1, keepdims=True) / D + eps_stat
        )
        rows_down.append(new)
        down_rows_new[layer : layer + 1, :] = row_of(new)
        stats[f, 7:8, E_ALL - STAT + layer * D : E_ALL - STAT + (layer + 1) * D] = rows_sum(g2)
    g = g_edge[...]
    g2 = g * g
    rows_edge = decay * column_of(edge_rows_ref[...]) + (1.0 - decay) * (
        jnp.sum(g2, axis=1, keepdims=True) / classes + eps_stat
    )
    edge_rows_new[...] = row_of(rows_edge)
    g2 = rows_sum(g2)
    stats[f, 6:7, :] = g2[:, 0:STAT]
    stats[f, 7:8, 0 : E_ALL - STAT] = g2[:, STAT:E_ALL]
    lane = lax.broadcasted_iota(jnp.int32, (1, 128), 1)
    totals = jnp.zeros((1, 128), F32)
    every = rows_in + rows_down + [rows_edge]
    for n, v in enumerate(every):
        totals = jnp.where(lane == n, rows_sum(v), totals)
    spot = E_ALL - STAT + depth * D
    stats[f, 7:8, spot : spot + 128] = totals
    copies = share(1, stats)

    def plain_rows(weight, new, old_v, new_v, columns):
        g = new[...]
        moment = decay * old_v[...] + (1.0 - decay) * (g * g + eps_stat)
        u = g * lax.rsqrt(moment)
        root = jnp.sqrt(jnp.sum(u * u, axis=1, keepdims=True) / columns)
        new_v[...] = moment
        new[...] = weight[...] - rate * u / jnp.maximum(1.0, root / clip_level)

    plain_rows(lbias_ref, lbias_new, lbias_v_ref, lbias_v_new, wide)
    plain_rows(tbias_ref, tbias_new, tbias_v_ref, tbias_v_new, 5 * D + 2 * PATCH_IN)
    loss = jnp.sum(sums_ref[S_SSE : S_SSE + 1, 0:TOK], axis=1, keepdims=True) / (tokens * PATCH_IN)

    for copy in copies:
        copy.wait()
    full = stats[0]
    for k in range(1, 8):
        full = full + stats[k]
    height = 8.0 * OWN
    tall = 4.0 * height

    def factors(rows_col, total, count, cols):
        return lax.rsqrt(rows_col / (total / count)), lax.rsqrt(cols)

    squared = jnp.zeros((1, 128), F32)
    used = []
    for layer in range(depth):
        total = full[7:8, spot + layer : spot + layer + 1]
        s = jnp.zeros((1, 1), F32)
        for t in range(wide // STAT):
            at = slice(t * STAT, (t + 1) * STAT)
            line = wide // STAT * layer + t
            cols = decay * in_cols_ref[layer : layer + 1, at] + (1.0 - decay) * (full[line : line + 1, :] / height + eps_stat)
            in_cols_new[layer : layer + 1, at] = cols
            a, b = factors(rows_in[layer], total, height, cols)
            u = g_in[layer, :, at] * a * b
            g_in[layer, :, at] = u
            s = s + total_of(u * u)
        squared = jnp.where(lane == layer, s, squared)
        at = E_ALL - STAT + layer * D
        cols = decay * down_cols_ref[layer : layer + 1, :] + (1.0 - decay) * (full[7:8, at : at + D] / tall + eps_stat)
        down_cols_new[layer : layer + 1, :] = cols
        total = full[7:8, spot + depth + layer : spot + depth + layer + 1]
        a, b = factors(rows_down[layer], total, tall, cols)
        u = g_down[layer] * a * b
        g_down[layer] = u
        squared = jnp.where(lane == depth + layer, total_of(u * u), squared)
    cols = jnp.concatenate([full[6:7, :], full[7:8, 0 : E_ALL - STAT]], axis=1)
    cols = decay * edge_cols_ref[...] + (1.0 - decay) * (cols / height + eps_stat)
    edge_cols_new[...] = cols
    a, b = factors(rows_edge, full[7:8, spot + 2 * depth : spot + 2 * depth + 1], height, cols)
    u = g_edge[...] * a * b
    g_edge[...] = u
    squared = jnp.where(lane == 2 * depth, total_of(u * u), squared)
    squares[f] = jnp.broadcast_to(squared, (8, 128))
    for copy in share(2, squares):
        copy.wait()
    full = squares[0]
    for k in range(1, 8):
        full = full + squares[k]
    full = full[0:1, :]
    counts = jnp.where(lane < depth, height * wide, jnp.where(lane < 2 * depth, tall * D, height * classes))
    roots = jnp.sqrt(full / counts)
    step = rate / jnp.maximum(1.0, roots / clip_level)
    tail_ref[...] = jnp.where(lane == 2 * depth + 1, loss, roots)
    for layer in range(depth):
        in_new[layer] = in_ref[layer] - step[:, layer : layer + 1] * g_in[layer]
        down_new[layer] = down_ref[layer] - step[:, depth + layer : depth + layer + 1] * g_down[layer]
    edge_new[...] = edge_ref[...] - step[:, 2 * depth : 2 * depth + 1] * g_edge[...]


def update(sizes, out_t, out_m, sums, d_mods, cond, before, time1, s1, feats, time2, w_mods, weights, stats):
    shape = jax.ShapeDtypeStruct
    vm = pl.BlockSpec(memory_space=pltpu.VMEM)
    dma = pltpu.SemaphoreType.DMA
    inputs = (out_t, out_m, sums, d_mods, cond, before, time1, s1, feats, time2, w_mods) + weights + stats
    outs = tuple(shape(v.shape, F32) for v in weights + stats) + (shape((1, 128), F32),)
    return pl.pallas_call(
        functools.partial(update_kernel, sizes),
        out_shape=outs,
        in_specs=[vm] * len(inputs),
        out_specs=(vm,) * len(outs),
        scratch_shapes=[
            pltpu.VMEM(weights[0].shape, F32),
            pltpu.VMEM(weights[1].shape, F32),
            pltpu.VMEM(weights[2].shape, F32),
            pltpu.VMEM((8, OWN, SLOTS), BF16),
            pltpu.VMEM((D, SLOTS), BF16),
            pltpu.VMEM((D, 128), F32),
            pltpu.VMEM((8, 8, STAT), F32),
            pltpu.VMEM((8, 8, 128), F32),
            dma((3, 7)),
            dma((3, 7)),
        ],
        compiler_params=pltpu.CompilerParams(collective_id=3, has_side_effects=True, vmem_limit_bytes=60 * 1024 * 1024),
        name="step_update",
    )(*inputs)


def mix_weights(tsteps):
    betas = 0.0001 + (0.02 - 0.0001) * jnp.arange(TSTEPS, dtype=jnp.float32) / (TSTEPS - 1)
    alpha_bar = jnp.exp(jnp.cumsum(jnp.log(1.0 - betas)))
    picked = jnp.arange(TSTEPS)[None, :] == tsteps[:, None]
    return jnp.sum(jnp.where(picked, alpha_bar[None, :], 0.0), axis=1)


def patch_rows(latent_rows):
    images = latent_rows.shape[0]
    side = GRID // PATCH
    shaped = latent_rows.reshape(images, CHANNELS, side, PATCH, side, PATCH)
    return jnp.transpose(shaped, (1, 3, 5, 0, 2, 4)).reshape(PATCH_IN, images * TOK)


def position_table():
    side = GRID // PATCH
    quarter = D // 4
    omegas = 1.0 / 10000.0 ** (np.arange(quarter) / quarter)
    angles = np.arange(side)[:, None] * omegas[None, :]
    axis = jnp.asarray(np.concatenate([np.sin(angles), np.cos(angles)], axis=1), F32)
    across = jnp.broadcast_to(axis[None, :, :], (side, side, 2 * quarter))
    down = jnp.broadcast_to(axis[:, None, :], (side, side, 2 * quarter))
    return jnp.concatenate([across, down], axis=2).reshape(side * side, D)


def time_features(tsteps):
    half_freq = FREQ // 2
    frequencies = jnp.exp(-math.log(10000.0) * jnp.arange(half_freq, dtype=jnp.float32) / half_freq)
    angles = tsteps.astype(jnp.float32)[:, None] * frequencies[None, :]
    return jnp.concatenate([jnp.cos(angles), jnp.sin(angles)], axis=1)


def fetch(layer_in, layer_out):
    own_in = layer_in[:, :, 6 * D :].astype(BF16)
    own_out = layer_out.astype(BF16)
    w_in = lax.all_gather(own_in, "fsdp", axis=1, tiled=True)
    w_out = lax.all_gather(own_out, "fsdp", axis=1, tiled=True)
    return w_in, w_out


def matmul(a, b, form):
    return jnp.einsum(form, a, b, preferred_element_type=F32)


def step_of(grad, rows_new, cols_new, rows_mean):
    second = rows_new[:, :, None] * cols_new[:, None, :] / rows_mean[:, None, None]
    return grad * lax.rsqrt(second)


def plain(weight, grad, moment):
    moment_new = decay * moment + (1.0 - decay) * (grad * grad + eps_stat)
    update = grad * lax.rsqrt(moment_new)
    root = jnp.sqrt(jnp.mean(update * update, axis=-1, keepdims=True))
    return (weight - rate * update / jnp.maximum(1.0, root / clip_level), moment_new)


def library_step(
    latents,
    tsteps,
    labels,
    noise,
    layer_in,
    layer_out,
    edge_mat,
    layer_bias,
    top_bias,
    in_rows,
    in_cols,
    out_rows,
    out_cols,
    edge_rows,
    edge_cols,
    layer_bias_v,
    top_bias_v,
):
    images = latents.shape[0]
    depth, own, wide = layer_in.shape
    fsdp = lax.axis_size("fsdp")
    rep = lax.axis_size("rep")
    at_f = lax.axis_index("fsdp")
    at_r = lax.axis_index("rep")
    every = images * fsdp * rep
    width = own * fsdp
    MOD = 6 * D
    start_freq = NCLS + PATCH_IN
    start_tail = start_freq + FREQ

    edge_low = edge_mat.astype(BF16)
    small = jnp.concatenate([edge_low[:, : start_tail + D], edge_low[:, start_tail + 3 * D :]], axis=1)
    full = lax.all_gather(small, "fsdp", axis=0, tiled=True)
    class_cols = full[:, :NCLS]
    patch_cols = full[:, NCLS:start_freq]
    freq_cols = full[:, start_freq:start_tail]
    time_second = full[:, start_tail : start_tail + D]
    head_cols = full[:, start_tail + D : start_tail + D + PATCH_IN]
    all_tsteps, all_labels = (
        lax.all_gather(tsteps, ("fsdp", "rep"), axis=0, tiled=True),
        lax.all_gather(labels, ("fsdp", "rep"), axis=0, tiled=True),
    )
    features = time_features(all_tsteps).astype(BF16)
    time1 = matmul(features, freq_cols, "bf,df->bd") + top_bias[D : 2 * D]
    s1 = jax.nn.silu(time1).astype(BF16)
    picked = (all_labels[:, None] == jnp.arange(NCLS)[None, :]).astype(BF16)
    before = matmul(s1, time_second, "bd,de->be") + top_bias[2 * D : 3 * D] + matmul(picked, class_cols, "bc,dc->bd")
    cond = jax.nn.silu(before).astype(BF16)

    def own_part(values):
        return lax.dynamic_slice_in_dim(values, at_f * own, own, axis=1)

    low_in = layer_in.astype(BF16)
    w_mods = jnp.concatenate(
        [low_in[layer, :, :MOD] for layer in range(depth)] + [edge_low[:, start_tail + D : start_tail + 3 * D]], axis=1
    )
    cond_own = own_part(cond)
    group_own = lax.dynamic_index_in_dim(cond_own.reshape(fsdp, rep, images, own), at_r, axis=1, keepdims=False)
    part = matmul(group_own.reshape(fsdp * images, own), w_mods, "bd,de->be")
    bias_mods = jnp.concatenate([layer_bias[layer, :MOD] for layer in range(depth)] + [top_bias[3 * D : 5 * D]])
    mods = lax.psum_scatter(part, "fsdp", scatter_dimension=0, tiled=True) + bias_mods
    kinds = 6 * depth + 2
    mods = mods.reshape(images, kinds, D)

    alphas = mix_weights(tsteps)
    noisy = jnp.sqrt(alphas)[:, None, None] * latents + jnp.sqrt(1.0 - alphas)[:, None, None] * noise
    patches = patch_rows(noisy.astype(BF16))
    target = patch_rows(noise)

    w_in, w_out = fetch(layer_in, layer_out)
    g_in, g_out, sums, d_mods = compute(
        patches,
        target,
        position_table(),
        jnp.transpose(jnp.pad(mods, ((0, 8 - images), (0, 16 - kinds), (0, 0))), (1, 0, 2)),
        w_in,
        w_out.reshape(depth, FF // FFC, FFC, D),
        patch_cols,
        head_cols,
        layer_bias,
        top_bias[None],
    )

    d_mods = jnp.transpose(d_mods, (1, 0, 2))[:images, :kinds].reshape(images, kinds * D)
    d_mods = lax.all_gather(d_mods, ("fsdp", "rep"), axis=0, tiled=True)
    g_rows = matmul(cond_own, d_mods, "bd,be->de")
    g_bmods = jnp.sum(d_mods.astype(F32), axis=0)
    d_before = matmul(d_mods, w_mods, "be,de->bd") * silu_slope(own_part(before))
    g_class = jnp.einsum("bd,bc->dc", d_before, picked.astype(F32), precision=lax.Precision.HIGHEST)
    d_time2 = lax.all_gather(d_before.astype(BF16), "fsdp", axis=1, tiled=True)
    g_time2 = matmul(own_part(s1), d_time2, "bd,be->de")
    d_time1 = (matmul(d_time2, time_second, "be,de->bd") * silu_slope(time1)).astype(BF16)
    g_time1 = matmul(own_part(d_time1), features, "bd,bf->df")

    shard_in = lax.psum(lax.psum_scatter(g_in, "fsdp", scatter_dimension=1, tiled=True), "rep")
    shard_out = lax.psum(lax.psum_scatter(g_out, "fsdp", scatter_dimension=1, tiled=True), "rep")
    sums = lax.psum(sums, ("fsdp", "rep")).reshape(S_ROWS, D)
    g_patch, g_head = sums[:S_HEAD], sums[S_HEAD:S_BIAS]
    g_bias = sums[S_BIAS:S_BPATCH].reshape(depth, BW)
    g_bpatch, g_bhead = sums[S_BPATCH : S_BPATCH + 1], sums[S_BHEAD : S_BHEAD + 1, :PATCH_IN]
    sse = jnp.sum(sums[S_SSE, :TOK])

    tok_total = every * TOK
    scale_grad = 1.0 / (PATCH_IN * math.sqrt(tok_total))
    loss = sse / (tok_total * PATCH_IN)
    fin = depth * MOD
    grad_edge = jnp.concatenate(
        [
            g_class,
            own_part(g_patch).T,
            g_time1,
            g_time2,
            g_rows[:, fin:],
            own_part(g_head).T,
            jnp.zeros((own, PATCH_IN), F32),
        ],
        axis=1,
    )[None] * scale_grad
    grad_in = jnp.concatenate([jnp.stack([g_rows[:, layer * MOD : (layer + 1) * MOD] for layer in range(depth)]), shard_in], axis=2) * scale_grad
    grad_out = shard_out * scale_grad
    grad_lbias = jnp.concatenate([g_bmods[:fin].reshape(depth, MOD), g_bias], axis=1) * scale_grad
    grad_tbias = jnp.concatenate(
        [
            g_bpatch[0],
            jnp.sum(d_time1.astype(F32), axis=0),
            jnp.sum(d_time2.astype(F32), axis=0),
            g_bmods[fin:],
            g_bhead[0],
            jnp.zeros((PATCH_IN,), F32),
        ]
    ) * scale_grad

    full_rows_in = width
    full_rows_out = layer_out.shape[1] * fsdp
    full_rows_edge = edge_mat.shape[0] * fsdp
    square_in = grad_in * grad_in + eps_stat
    square_out = grad_out * grad_out + eps_stat
    square_edge = grad_edge * grad_edge + eps_stat
    rows_in_new = decay * in_rows + (1.0 - decay) * jnp.mean(square_in, axis=2)
    rows_out_new = decay * out_rows + (1.0 - decay) * jnp.mean(square_out, axis=2)
    rows_edge_new = decay * edge_rows[None] + (1.0 - decay) * jnp.mean(square_edge, axis=2)
    col_in, total_in, col_out, total_out, col_edge, total_edge = lax.psum(
        (
            jnp.sum(square_in, axis=1),
            jnp.sum(rows_in_new, axis=1),
            jnp.sum(square_out, axis=1),
            jnp.sum(rows_out_new, axis=1),
            jnp.sum(square_edge, axis=1),
            jnp.sum(rows_edge_new, axis=1),
        ),
        "fsdp",
    )
    cols_in_new = decay * in_cols + (1.0 - decay) * col_in / full_rows_in
    cols_out_new = decay * out_cols + (1.0 - decay) * col_out / full_rows_out
    cols_edge_new = decay * edge_cols[None] + (1.0 - decay) * col_edge / full_rows_edge
    update_in = step_of(grad_in, rows_in_new, cols_in_new, total_in / full_rows_in)
    update_out = step_of(grad_out, rows_out_new, cols_out_new, total_out / full_rows_out)
    update_edge = step_of(grad_edge, rows_edge_new, cols_edge_new, total_edge / full_rows_edge)
    sum_in, sum_out, sum_edge = lax.psum(
        (
            jnp.sum(update_in * update_in, axis=(1, 2)),
            jnp.sum(update_out * update_out, axis=(1, 2)),
            jnp.sum(update_edge * update_edge, axis=(1, 2)),
        ),
        "fsdp",
    )
    roots_in = jnp.sqrt(sum_in / (full_rows_in * grad_in.shape[2]))
    roots_out = jnp.sqrt(sum_out / (full_rows_out * grad_out.shape[2]))
    roots_edge = jnp.sqrt(sum_edge / (full_rows_edge * grad_edge.shape[2]))
    factor_in = jnp.maximum(1.0, roots_in / clip_level)[:, None, None]
    factor_out = jnp.maximum(1.0, roots_out / clip_level)[:, None, None]
    factor_edge = jnp.maximum(1.0, roots_edge / clip_level)[:, None, None]
    in_new = layer_in - rate * update_in / factor_in
    out_new = layer_out - rate * update_out / factor_out
    edge_new = (edge_mat[None] - rate * update_edge / factor_edge)[0]
    clip_roots = jnp.concatenate([roots_in, roots_out, roots_edge])
    lbias_new, lbias_v_new = plain(layer_bias, grad_lbias, layer_bias_v)
    tbias_new, tbias_v_new = plain(top_bias, grad_tbias, top_bias_v)
    return (
        loss,
        in_new,
        out_new,
        edge_new,
        lbias_new,
        tbias_new,
        rows_in_new,
        cols_in_new,
        rows_out_new,
        cols_out_new,
        rows_edge_new[0],
        cols_edge_new[0],
        lbias_v_new,
        tbias_v_new,
        clip_roots,
    )


def direct_step(
    latents,
    tsteps,
    labels,
    noise,
    layer_in,
    layer_out,
    edge_mat,
    layer_bias,
    top_bias,
    in_rows,
    in_cols,
    out_rows,
    out_cols,
    edge_rows,
    edge_cols,
    layer_bias_v,
    top_bias_v,
):
    images = latents.shape[0]
    depth = layer_in.shape[0]
    MOD = 6 * D
    tokens = images * 32 * TOK
    classes = edge_mat.shape[1]
    start_freq = NCLS + PATCH_IN
    start_tail = start_freq + FREQ

    def wide_to(v, width, fill=0.0):
        return jnp.pad(v, ((0, 0), (0, width - v.shape[1])), constant_values=fill)

    def aligned(v, fill):
        return jnp.concatenate(
            [
                wide_to(v[:, :NCLS], E_PATCH, fill),
                wide_to(v[:, NCLS:start_freq], E_T1 - E_PATCH, fill),
                v[:, start_freq : start_tail + 3 * D],
                wide_to(v[:, start_tail + 3 * D :], E_ALL - E_HEAD, fill),
            ],
            axis=1,
        )

    edge_a = aligned(edge_mat, 0.0)
    edge_low = edge_a.astype(BF16)
    small = jnp.concatenate(
        [
            edge_low[:, :E_PATCH],
            edge_low[:, E_T1:E_FIN],
            edge_low[:, E_PATCH:E_T1],
            edge_low[:, E_HEAD:E_ALL],
            jnp.zeros((OWN, C_ALL - C_HEAD - (E_ALL - E_HEAD)), BF16),
        ],
        axis=1,
    )
    w_mods = jnp.concatenate([layer_in[layer, :, :MOD].astype(BF16) for layer in range(depth)] + [edge_low[:, E_FIN:E_HEAD]], axis=1)
    feat = jnp.concatenate(
        [time_features(tsteps), jnp.broadcast_to(labels.astype(F32)[:, None], (images, 128))], axis=1
    )
    feat = jnp.pad(feat, ((0, 8 - images), (0, 0)))
    tbias = top_bias[None]
    own = (layer_in[:, :, MOD:].astype(BF16), layer_out.astype(BF16).reshape(depth, 4, OWN, D))
    w_patch, w_head, time2, w_in, w_out, mods, time1, s1, before, cond, feats = prologue(
        small, feat, w_mods, layer_bias, tbias, *own, images
    )

    alphas = mix_weights(tsteps)
    noisy = jnp.sqrt(alphas)[:, None, None] * latents + jnp.sqrt(1.0 - alphas)[:, None, None] * noise
    patches = patch_rows(noisy.astype(BF16))
    target = patch_rows(noise)
    _, _, sums, _, out_t, out_m, d_mods = compute(
        patches, target, position_table(), mods, w_in, w_out, w_patch, w_head, layer_bias, tbias, own
    )
    weights = (layer_in, layer_out, edge_a, layer_bias, tbias)
    stats = (
        in_rows,
        in_cols,
        out_rows,
        out_cols,
        edge_rows[None],
        aligned(edge_cols[None], 1.0),
        layer_bias_v,
        top_bias_v[None],
    )
    (
        in_new,
        out_new,
        edge_new,
        lbias_new,
        tbias_new,
        in_rows_new,
        in_cols_new,
        out_rows_new,
        out_cols_new,
        edge_rows_new,
        edge_cols_new,
        lbias_v_new,
        tbias_v_new,
        tail,
    ) = update(
        (classes, tokens), out_t, out_m, sums.reshape(S_ROWS, D), d_mods, cond, before, time1, s1, feats, time2, w_mods, weights, stats
    )

    def natural(v):
        return jnp.concatenate(
            [v[:, :NCLS], v[:, E_PATCH : E_PATCH + PATCH_IN], v[:, E_T1 : E_HEAD + 2 * PATCH_IN]], axis=1
        )

    return (
        tail[0, 2 * depth + 1],
        in_new,
        out_new,
        natural(edge_new),
        lbias_new,
        tbias_new[0],
        in_rows_new,
        in_cols_new,
        out_rows_new,
        out_cols_new,
        edge_rows_new[0],
        natural(edge_cols_new)[0],
        lbias_v_new,
        tbias_v_new[0],
        tail[0, : 2 * depth + 1],
    )


def shards(*arrays):
    layer_in = arrays[4]
    mesh = (lax.axis_size("fsdp"), lax.axis_size("rep"), layer_in.shape[0], layer_in.shape[1])
    return (direct_step if mesh == (8, 4, 2, OWN) else library_step)(*arrays)


def solution(mesh):
    placed = (
        P(("fsdp", "rep"), None, None),
        P(("fsdp", "rep")),
        P(("fsdp", "rep")),
        P(("fsdp", "rep"), None, None),
        P(None, "fsdp", None),
        P(None, "fsdp", None),
        P("fsdp", None),
        P(),
        P(),
        P(None, "fsdp"),
        P(),
        P(None, "fsdp"),
        P(),
        P("fsdp"),
        P(),
        P(),
        P(),
    )
    return jax.shard_map(
        shards,
        mesh=mesh,
        in_specs=placed,
        out_specs=(
            P(),
            P(None, "fsdp", None),
            P(None, "fsdp", None),
            P("fsdp", None),
            P(),
            P(),
            P(None, "fsdp"),
            P(),
            P(None, "fsdp"),
            P(),
            P("fsdp"),
            P(),
            P(),
            P(),
            P(),
        ),
        check_vma=False,
    )
```
